32 devices in a mesh: fsdp: 8 (over z, y), tensor: 4 (over x, core).
Axes of the slice: x: 2, y: 2, z: 4, core: 2. Of those that a mesh axis runs over, the one named last changes fastest.
Arguments:
- tokens: bfloat16 [12288, 768], P(('fsdp', 'tensor')), may hold values from -6 to 6
- attn_weight: bfloat16 [3, 768, 768], P(None, 'fsdp', 'tensor'), may hold values from -0.21875 to 0.21875
- query_value_bias: bfloat16 [2, 12, 64], P(None, 'tensor', 'fsdp'), may hold values from -3 to 3
- out_weight: bfloat16 [768, 768], P('tensor', 'fsdp'), may hold values from -1.25 to 1.25
- hidden_weight: bfloat16 [768, 3072], P('fsdp', 'tensor'), may hold values from -0.21875 to 0.21875
- hidden_bias: bfloat16 [48, 64], P('tensor', 'fsdp'), may hold values from -3 to 3
- down_weight: bfloat16 [3072, 768], P('tensor', 'fsdp'), may hold values from -0.109375 to 0.109375
- norm_gains: bfloat16 [2, 768], P(None, 'fsdp'), may hold values from 0.5 to 1.5
- norm_biases: bfloat16 [2, 768], P(None, 'fsdp'), may hold values from -2 to 2
- output_biases: bfloat16 [2, 768], P(None, 'fsdp'), may hold values from -2 to 2
- segment_ids: int32 [12288], P('fsdp'), may hold values from 0 to 15, as said below
- padding: int32 [12288], P('fsdp'), may hold values from 0 to 1, as said below
- cotangent: bfloat16 [12288, 768], P(('fsdp', 'tensor')), may hold values from -6 to 6
Outputs:
- layer_out: bfloat16 [12288, 768], P(('fsdp', 'tensor'))
- tokens_grad: float32 [12288, 768], P(('fsdp', 'tensor'))
- attn_weight_grad: float32 [3, 768, 768], P(None, 'fsdp', 'tensor')
- query_value_bias_grad: float32 [2, 12, 64], P(None, 'tensor', 'fsdp')
- out_weight_grad: float32 [768, 768], P('tensor', 'fsdp')
- hidden_weight_grad: float32 [768, 3072], P('fsdp', 'tensor')
- hidden_bias_grad: float32 [48, 64], P('tensor', 'fsdp')
- down_weight_grad: float32 [3072, 768], P('tensor', 'fsdp')
- norm_gains_grad: float32 [2, 768], P(None, 'fsdp')
- norm_biases_grad: float32 [2, 768], P(None, 'fsdp')
- output_biases_grad: float32 [2, 768], P(None, 'fsdp')
- root_squares: float32 [3], replicated
The draws below stay inside these ranges and needn't reach their ends.
Inputs may be any that keep to these rules, and one draw needn't show every extreme that they name: `segment_ids`: within each sequence of 1536 positions, segment ids start at 0 and rise by one at each new document; every document has 96 to 768 tokens except the last of a sequence, which its end may cut; some document has exactly 768 tokens. Within each sequence, the padding positions (value 0) form a tail of at most 192 positions.
All inputs are finite; a program needn't handle non-finite values.
Results may differ from the reference program's by a relative error of at most 0.013.
The reference program's roundings to bfloat16 on the way count: a program that leaves them out, or rounds other values in their place, can miss the bound.
Values may be sent and summed in bfloat16 or wider, within the bound.
A program may use at most 192 MiB of HBM per device.

```python
import jax
import jax.numpy as jnp
from jax import lax

D = 768
H = 12
DH = 64
FF = 3072
TOK_DEV = 1536
TOKENS = 12288
DOC_MOST = 768
DOC_LEAST = 96


def packed_layout(key):
    seq_count = TOKENS // TOK_DEV
    doc_slots = TOK_DEV // DOC_LEAST + 1
    base_key = jax.random.fold_in(key, 4711)
    key_lengths, key_pick, key_pad = jax.random.split(base_key, 3)
    doc_lengths = jax.random.randint(key_lengths, (seq_count, doc_slots), DOC_LEAST, DOC_MOST + 1, dtype=jnp.int32)
    chosen = jax.random.randint(key_pick, (), 0, seq_count, dtype=jnp.int32)
    seq_numbers = jnp.arange(seq_count, dtype=jnp.int32)
    shortest_seq = (chosen + 1) % seq_count
    doc_lengths = jnp.where((seq_numbers == shortest_seq)[:, None], DOC_LEAST, doc_lengths)
    first_docs = jnp.where(seq_numbers == chosen, DOC_MOST, doc_lengths[:, 0])
    doc_lengths = doc_lengths.at[:, 0].set(first_docs)
    doc_ends = jnp.cumsum(doc_lengths, axis=1)
    positions = jnp.arange(TOK_DEV, dtype=jnp.int32)
    seg_table = jnp.sum((positions[None, :, None] >= doc_ends[:, None, :]).astype(jnp.int32), axis=2)
    pad_lengths = jax.random.randint(key_pad, (seq_count,), 0, TOK_DEV // 8 + 1, dtype=jnp.int32)
    pad_table = (positions[None, :] < TOK_DEV - pad_lengths[:, None]).astype(jnp.int32)
    return (seg_table.reshape(TOKENS).astype(jnp.int32), pad_table.reshape(TOKENS).astype(jnp.int32))


def draw_segment_ids(key, part):
    return packed_layout(key)[0]


def draw_padding(key, part):
    return packed_layout(key)[1]


def levels(stream_key, extent, cuts, low, largest):
    loudness = 1.0
    for position, blocks in cuts:
        heights = jax.random.uniform(jax.random.fold_in(jax.random.fold_in(stream_key, 6), position), (blocks,), jnp.float32, low / len(cuts), largest / len(cuts))
        loudness = loudness * jnp.repeat(jnp.exp(heights), extent[position] // blocks).reshape((-1,) + (1,) * (len(extent) - 1 - position))
    return loudness


def bell_draw(rng, extent, width, limit, cuts=(), kind=jnp.bfloat16):
    level = levels(rng, extent, cuts, -0.22, 0.18) if cuts else 1.0
    values = jax.random.normal(rng, extent, jnp.float32) * width * level
    return jnp.minimum(jnp.maximum(values, -limit), limit).astype(kind)


def setup_inputs(seed: int = 0) -> dict:
    key_list = jax.random.split(jax.random.key(seed), 14)
    tokens = bell_draw(key_list[0], (TOKENS, D), 1.0, 6.0, ((0, 32),))
    attn_weight = bell_draw(key_list[1], (3, D, D), D ** -0.5, 0.21875, ((1, 8), (2, 4)))
    query_value_bias = bell_draw(key_list[2], (2, H, DH), 0.5, 3.0, ((1, 4), (2, 8)))
    out_weight = bell_draw(key_list[3], (D, D), (D // 32) ** -0.5, 1.25, ((0, 4), (1, 8)))
    hidden_weight = bell_draw(key_list[4], (D, FF), D ** -0.5, 0.21875, ((0, 8), (1, 4)))
    hidden_bias = bell_draw(key_list[5], (FF // DH, DH), 0.5, 3.0, ((0, 4), (1, 8)))
    down_weight = bell_draw(key_list[6], (FF, D), FF ** -0.5, 0.109375, ((0, 4), (1, 8)))
    norm_gains = jnp.clip(1.0 + 0.1 * jax.random.normal(key_list[7], (2, D), jnp.float32), 0.5, 1.5).astype(jnp.bfloat16)
    norm_biases = bell_draw(key_list[8], (2, D), 0.3, 2.0, ((1, 8),))
    output_biases = bell_draw(key_list[9], (2, D), 0.3, 2.0, ((1, 8),))
    segment_ids = draw_segment_ids(jax.random.fold_in(key_list[13], 71), 0)
    padding = draw_padding(jax.random.fold_in(key_list[13], 71), 0)
    cotangent = bell_draw(key_list[12], (TOKENS, D), 1.0, 6.0, ((0, 32),))
    return {"tokens": tokens, "attn_weight": attn_weight, "query_value_bias": query_value_bias, "out_weight": out_weight, "hidden_weight": hidden_weight, "hidden_bias": hidden_bias, "down_weight": down_weight, "norm_gains": norm_gains, "norm_biases": norm_biases, "output_biases": output_biases, "segment_ids": segment_ids, "padding": padding, "cotangent": cotangent}


EPSILON = 1e-12
HIGHEST_PRECISION = lax.Precision.HIGHEST

@jax.custom_vjp
def low(v):
    return lax.optimization_barrier(v.astype(jnp.bfloat16)).astype(jnp.float32)

@jax.custom_vjp
def low_back(v):
    return v

def low_keep(v):
    return (low(v), None)

def low_pass(kept, grad):
    return (grad,)

def back_keep(v):
    return (v, None)

def back_low(kept, grad):
    return (low(grad),)
low.defvjp(low_keep, low_pass)
low_back.defvjp(back_keep, back_low)

def layer_norm(hidden, gain_row, shift_row):
    row_mean = lax.optimization_barrier(jnp.mean(hidden, axis=-1, keepdims=True))
    centered = hidden - row_mean
    variance = lax.optimization_barrier(jnp.mean(centered * centered, axis=-1, keepdims=True))
    return centered * lax.rsqrt(variance + EPSILON) * gain_row + shift_row

def matmul_high(left, right):
    return jnp.dot(left, right, precision=HIGHEST_PRECISION)

def attend(queries, all_keys, all_values, seg_ids, pad_flags):
    seq_len = queries.shape[0]
    block_rows = min(512, seq_len)
    positions = jnp.arange(seq_len, dtype=jnp.int32)
    key_live = pad_flags == 1

    def one_block(block_index):
        row_start = block_index * block_rows
        q_rows = lax.dynamic_slice_in_dim(queries, row_start, block_rows, 0)
        seg_rows = lax.dynamic_slice_in_dim(seg_ids, row_start, block_rows, 0)
        pad_rows = lax.dynamic_slice_in_dim(pad_flags, row_start, block_rows, 0)
        pos_rows = row_start + jnp.arange(block_rows, dtype=jnp.int32)
        raw_scores = low_back(jnp.einsum('qhd,khd->hqk', q_rows, all_keys, precision=HIGHEST_PRECISION) * 0.125)
        allowed = (seg_rows[:, None] == seg_ids[None, :]) & key_live[None, :] | (pos_rows[:, None] == positions[None, :])
        masked = jnp.where(allowed[None], raw_scores, -1e+30)
        row_top = lax.optimization_barrier(jnp.max(masked, axis=-1, keepdims=True))
        exp_terms = jnp.exp(masked - row_top)
        attn_probs = exp_terms / lax.optimization_barrier(jnp.sum(exp_terms, axis=-1, keepdims=True))
        context = jnp.einsum('hqk,khd->qhd', low(attn_probs), all_values, precision=HIGHEST_PRECISION)
        return context * pad_rows.astype(context.dtype)[:, None, None]
    blocks = lax.map(jax.checkpoint(one_block), jnp.arange(seq_len // block_rows, dtype=jnp.int32))
    return blocks.reshape(seq_len, -1)

def forward(inputs, attn_w, qv_b, out_w, hidden_w, hidden_b, down_w, gain_rows, shift_rows, bias_rows, seg_ids, pad_flags):
    seq_len = inputs.shape[0]
    projected = jnp.einsum('sd,jde->jse', inputs, attn_w, precision=HIGHEST_PRECISION)
    queries = low(low_back(projected[0] + qv_b[0].reshape(D)))
    all_keys = low(low_back(projected[1]))
    all_values = low(low_back(projected[2] + qv_b[1].reshape(D)))
    context = attend(queries.reshape(seq_len, H, DH), all_keys.reshape(seq_len, H, DH), all_values.reshape(seq_len, H, DH), seg_ids, pad_flags)
    context = low(low_back(context))
    attn_branch = low_back(matmul_high(context, out_w) + bias_rows[0])
    first_norm = layer_norm(inputs + attn_branch, gain_rows[0], shift_rows[0])
    pre_act = low_back(matmul_high(low(first_norm), hidden_w) + hidden_b.reshape(FF))
    acted = jax.nn.gelu(pre_act, approximate=False)
    ff_branch = low_back(matmul_high(low(acted), down_w) + bias_rows[1])
    layer_value = layer_norm(first_norm + ff_branch, gain_rows[1], shift_rows[1])
    return (layer_value, (attn_branch, ff_branch))

def reference(tokens, attn_weight, query_value_bias, out_weight, hidden_weight, hidden_bias, down_weight, norm_gains, norm_biases, output_biases, segment_ids, padding, cotangent):
    weights = tuple((w.astype(jnp.float32) for w in (attn_weight, query_value_bias, out_weight, hidden_weight, hidden_bias, down_weight, norm_gains, norm_biases, output_biases)))
    seq_count = TOKENS // TOK_DEV
    token_seqs = tokens.astype(jnp.float32).reshape(seq_count, TOK_DEV, D)
    cot_seqs = cotangent.astype(jnp.float32).reshape(seq_count, TOK_DEV, D)
    seg_seqs = segment_ids.reshape(seq_count, TOK_DEV)
    pad_seqs = padding.reshape(seq_count, TOK_DEV)

    def per_sequence(carried, item):
        grad_totals, square_totals = carried
        inputs, cot_rows, seg_ids, pad_flags = item

        def local_forward(inputs_in, *weight_list):
            return forward(inputs_in, *weight_list, seg_ids, pad_flags)
        layer_value, pull_back, branches = jax.vjp(local_forward, inputs, *weights, has_aux=True)
        grads = pull_back(cot_rows)
        attn_branch, ff_branch = branches
        live_rows = pad_flags.astype(jnp.float32)[:, None]
        squares = jnp.stack([jnp.sum(live_rows * inputs * inputs), jnp.sum(live_rows * attn_branch * attn_branch), jnp.sum(live_rows * ff_branch * ff_branch)])
        grad_totals = tuple((total + grad for total, grad in zip(grad_totals, grads[1:])))
        return ((grad_totals, square_totals + squares), (layer_value.astype(jnp.bfloat16), grads[0]))
    start_totals = (tuple((jnp.zeros_like(w) for w in weights)), jnp.zeros((3,), jnp.float32))
    (grad_totals, square_totals), (layer_seqs, dtoken_seqs) = lax.scan(per_sequence, start_totals, (token_seqs, cot_seqs, seg_seqs, pad_seqs))
    live_count = jnp.sum(padding.astype(jnp.float32))
    root_values = jnp.sqrt(square_totals / (live_count * D))
    return (layer_seqs.reshape(TOKENS, D), dtoken_seqs.reshape(TOKENS, D), grad_totals[0], grad_totals[1], grad_totals[2], grad_totals[3], grad_totals[4], grad_totals[5], grad_totals[6], grad_totals[7], grad_totals[8], root_values)
```

```python
import functools

import jax
import jax.numpy as jnp
from jax import lax
from jax.experimental import pallas as pl
from jax.experimental.pallas import tpu as pltpu
from jax.sharding import PartitionSpec as P

D = 768
DH = 64


EPSILON = 1e-12
F32=jnp.float32; BF=jnp.bfloat16
BQ=256; BK=256

def dot(a,b,dn=((1,),(0,))):
    return lax.dot_general(a,b,(dn,((),())),preferred_element_type=F32)

def head_rows(x_t, h):
    r = lax.broadcasted_iota(jnp.int32, x_t.shape, 0)//DH
    return jnp.where(r==h, x_t, jnp.zeros_like(x_t))
def head_cols(x, h):
    r = lax.broadcasted_iota(jnp.int32, x.shape, 1)//DH
    return jnp.where(r==h, x, jnp.zeros_like(x))

def fold_max(s): return jnp.max(s.reshape(s.shape[0]//8,8,s.shape[1]),axis=0)
def fold_sum(s): return jnp.sum(s.reshape(s.shape[0]//8,8,s.shape[1]),axis=0)

def fwd_kernel(heads, bounds, q_ref,k_ref,v_ref,sq_ref,sk_ref,pad_ref, ctx_ref, octx_ref, lse_ref, qt, kh, vt, sc):
    S=q_ref.shape[0]; W=heads*DH
    qt[...]=(q_ref[...].astype(F32)*0.125).T.astype(BF)
    kk=k_ref[...]
    for h in range(heads): kh[h]=kk[:,h*DH:(h+1)*DH]
    vt[...]=v_ref[...].astype(F32).T.astype(BF)
    def qblock(i,_):
        q0=pl.multiple_of(i*BQ,BQ)
        lo=bounds[2*i]; hi=bounds[2*i+1]
        sq=sq_ref[0:1,pl.ds(q0,BQ)]
        qpos=q0+lax.broadcasted_iota(jnp.int32,(BK,BQ),1)
        def first(j,c):
            k0=pl.multiple_of(j*BK,BK)
            sk=jnp.concatenate([sk_ref[pl.ds(k0,BK),:]]*(BQ//128),axis=1)
            kpos=k0+lax.broadcasted_iota(jnp.int32,(BK,BQ),0)
            ok=(sk==sq)|(kpos==qpos)
            out=[]
            for h in range(heads):
                s=jnp.where(ok,dot(kh[h,pl.ds(k0,BK),:],qt[h*DH:(h+1)*DH,pl.ds(q0,BQ)]),-1e30)
                sc[h,pl.ds(k0,BK),:]=s
                out.append(jnp.maximum(c[h],fold_max(s)))
            return tuple(out)
        m=lax.fori_loop(lo,hi,first,(jnp.full((8,BQ),-3e38,F32),)*heads)
        m=[jnp.max(x,axis=0,keepdims=True) for x in m]
        def second(j,c):
            k0=pl.multiple_of(j*BK,BK)
            out=[]
            for h in range(heads):
                l,acc=c[2*h:2*h+2]
                p=jnp.exp(sc[h,pl.ds(k0,BK),:]-m[h])
                out+=[l+fold_sum(p),acc+dot(vt[h*DH:(h+1)*DH,pl.ds(k0,BK)],p.astype(BF))]
            return tuple(out)
        c=lax.fori_loop(lo,hi,second,(jnp.zeros((8,BQ),F32),jnp.zeros((DH,BQ),F32))*heads)
        o=[]
        for h in range(heads):
            l,acc=c[2*h:2*h+2]
            l=jnp.sum(l,axis=0,keepdims=True)
            lse_ref[h:h+1,pl.ds(q0,BQ)]=m[h]+jnp.log(l)
            o.append(acc/l)
        ot=jnp.concatenate(o,axis=0)*pad_ref[0:1,pl.ds(q0,BQ)]
        octx_ref[:,pl.ds(q0,BQ)]=ot
        ctx_ref[pl.ds(q0,BQ),:]=ot.T.astype(BF)
        return 0
    lax.fori_loop(0,S//BQ,qblock,0)

def attn_fwd(bounds,q,k,v,sq,sk,pad):
    S,W=q.shape; heads=W//DH
    vm=pl.BlockSpec(memory_space=pltpu.VMEM)
    return pl.pallas_call(functools.partial(fwd_kernel,heads),
        in_specs=[pl.BlockSpec(memory_space=pltpu.SMEM)]+[vm]*6,
        out_specs=[vm]*3,
        out_shape=[jax.ShapeDtypeStruct((S,W),BF),jax.ShapeDtypeStruct((W,S),F32),jax.ShapeDtypeStruct((heads,S),F32)],
        scratch_shapes=[pltpu.VMEM((W,S),BF),pltpu.VMEM((heads,S,DH),BF),pltpu.VMEM((W,S),BF),pltpu.VMEM((heads,S,BQ),F32)],
        compiler_params=pltpu.CompilerParams(vmem_limit_bytes=56<<20),
        name="attend_forward")(bounds,q,k,v,sq,sk,pad)

def bwd_kernel(heads, bounds, q_ref,k_ref,v_ref,dc_ref,oct_ref,lse_ref,sq_ref,sk_ref,pad_ref, dqkv_ref, qt, dt, kt, kh, vh, qh, dh, dqt, dsum, dka, dva):
    S=q_ref.shape[0]; W=heads*DH
    qs=(q_ref[...].astype(F32)*0.125)
    qsb=qs.astype(BF); qt[...]=qs.T.astype(BF)
    kk=k_ref[...]; vv=v_ref[...]
    kt[...]=kk.astype(F32).T.astype(BF)
    dct=dc_ref[...].astype(F32).T*pad_ref[0:1,:]
    dt[...]=dct.astype(BF)
    dcn=dct.T.astype(BF)
    prod=dct*oct_ref[...]
    for h in range(heads):
        c=slice(h*DH,(h+1)*DH)
        kh[h]=kk[:,c]; vh[h]=vv[:,c]; qh[h]=qsb[:,c]; dh[h]=dcn[:,c]
        dsum[h:h+1,:]=jnp.sum(prod[h*DH:(h+1)*DH],axis=0,keepdims=True)
    dqt[...]=jnp.zeros_like(dqt)
    def kblock(j,_):
        k0=pl.multiple_of(j*BK,BK)
        lo=bounds[2*j]; hi=bounds[2*j+1]
        sk=jnp.concatenate([sk_ref[pl.ds(k0,BK),:]]*(BQ//128),axis=1)
        kpos=k0+lax.broadcasted_iota(jnp.int32,(BK,BQ),0)
        dka[...]=jnp.zeros_like(dka); dva[...]=jnp.zeros_like(dva)
        def body(i,_):
            q0=pl.multiple_of(i*BQ,BQ)
            sq=sq_ref[0:1,pl.ds(q0,BQ)]
            qpos=q0+lax.broadcasted_iota(jnp.int32,(BK,BQ),1)
            ok=(sk==sq)|(kpos==qpos)
            for h in range(heads):
                r=slice(h*DH,(h+1)*DH)
                s=jnp.where(ok,dot(kh[h,pl.ds(k0,BK),:],qt[r,pl.ds(q0,BQ)]),-1e30)
                p=jnp.exp(s-lse_ref[h:h+1,pl.ds(q0,BQ)])
                dp=dot(vh[h,pl.ds(k0,BK),:],dt[r,pl.ds(q0,BQ)])
                ds=(p*(dp-dsum[h:h+1,pl.ds(q0,BQ)])).astype(BF)
                dva[h]+=dot(p.astype(BF),dh[h,pl.ds(q0,BQ),:])
                dka[h]+=dot(ds,qh[h,pl.ds(q0,BQ),:])
                dqt[r,pl.ds(q0,BQ)]+=dot(kt[r,pl.ds(k0,BK)],ds)
            return 0
        lax.fori_loop(lo,hi,body,0)
        dqkv_ref[1,pl.ds(k0,BK),:]=jnp.concatenate([dka[h] for h in range(heads)],axis=1).astype(BF)
        dqkv_ref[2,pl.ds(k0,BK),:]=jnp.concatenate([dva[h] for h in range(heads)],axis=1).astype(BF)
        return 0
    lax.fori_loop(0,S//BK,kblock,0)
    dqkv_ref[0]=(dqt[...]*0.125).T.astype(BF)

def attn_bwd(bounds,q,k,v,dc,oct,lse,sq,sk,pad):
    S,W=q.shape; heads=W//DH
    vm=pl.BlockSpec(memory_space=pltpu.VMEM)
    return pl.pallas_call(functools.partial(bwd_kernel,heads),
        in_specs=[pl.BlockSpec(memory_space=pltpu.SMEM)]+[vm]*9,
        out_specs=vm,
        out_shape=jax.ShapeDtypeStruct((3,S,W),BF),
        scratch_shapes=[pltpu.VMEM((W,S),BF)]*3+[pltpu.VMEM((heads,S,DH),BF)]*4+[pltpu.VMEM((W,S),F32),pltpu.VMEM((heads,S),F32)]+[pltpu.VMEM((heads,BK,DH),F32)]*2,
        compiler_params=pltpu.CompilerParams(vmem_limit_bytes=60<<20),
        name="attend_backward")(bounds,q,k,v,dc,oct,lse,sq,sk,pad)

def side_tables(seg,pad):
    S=seg.shape[0]; nb=S//BQ
    skl=jnp.where(pad==1,seg,-1)
    sk=jnp.broadcast_to(skl[:,None],(S,128))
    sb=seg.reshape(nb,BQ)
    lo=jnp.sum((seg[None,:]<sb[:,:1]).astype(jnp.int32),axis=1)//BK
    hi=(jnp.sum((seg[None,:]<=sb[:,-1:]).astype(jnp.int32),axis=1)+BK-1)//BK
    return jnp.stack([lo,hi],axis=1).reshape(-1), seg[None,:], sk, pad.astype(F32)[None,:]


def split_up(value, dim, devices):
    before, after = (value.shape[:dim], value.shape[dim + 1 :])
    return jnp.moveaxis(value.reshape(*before, devices, -1, *after), dim, 0)


def summed_on_arrival(value, axis, dim):
    blocks = split_up(value, dim, lax.axis_size(axis))
    arrived = lax.all_to_all(blocks, axis, split_axis=0, concat_axis=0, tiled=True)
    return arrived.astype(jnp.float32).sum(axis=0)


def sent_together(arrays, axis, dim, along):
    ends, at = ([], 0)
    for a in arrays[:-1]:
        at += a.shape[along]
        ends.append(at)
    both = jnp.concatenate(arrays, axis=along)
    return tuple(jnp.split(summed_on_arrival(both, axis, dim), ends, axis=along))


def layer_norm(hidden, gain_row, shift_row):
    row_mean = jnp.mean(hidden, axis=-1, keepdims=True)
    centered = hidden - row_mean
    variance = jnp.mean(centered * centered, axis=-1, keepdims=True)
    return centered * lax.rsqrt(variance + EPSILON) * gain_row + shift_row


def gelu_exact(value):
    return jax.nn.gelu(value, approximate=False)


def shards(
    tokens,
    attn_weight,
    query_value_bias,
    out_weight,
    hidden_weight,
    hidden_bias,
    down_weight,
    norm_gains,
    norm_biases,
    output_biases,
    segment_ids,
    padding,
    cotangent,
):
    wide = jnp.float32
    narrow = jnp.bfloat16
    gathered = (
        lax.all_gather(attn_weight, "fsdp", axis=1, tiled=True),
        lax.all_gather(query_value_bias, "fsdp", axis=2, tiled=True),
        lax.all_gather(out_weight, "fsdp", axis=1, tiled=True),
        lax.all_gather(hidden_weight, "fsdp", axis=0, tiled=True),
        lax.all_gather(hidden_bias, "fsdp", axis=1, tiled=True),
        lax.all_gather(down_weight, "fsdp", axis=1, tiled=True),
        lax.all_gather(norm_gains, "fsdp", axis=1, tiled=True),
        lax.all_gather(norm_biases, "fsdp", axis=1, tiled=True),
        lax.all_gather(output_biases, "fsdp", axis=1, tiled=True),
    )
    w_qkv, qv_full, w_proj, w_up, up_bias, w_down, gain_rows, shift_rows, bias_rows = gathered
    row_count = tokens.shape[0]
    seq_len = segment_ids.shape[0]
    tensor_place = lax.axis_index("tensor")
    local_pad = lax.dynamic_slice_in_dim(padding, tensor_place * row_count, row_count, 0).astype(
        wide
    )
    whole_rows = lax.all_gather(tokens, "tensor", axis=0, tiled=True)
    width = w_qkv.shape[2]
    heads = width // DH
    projected = jnp.einsum("sd,jde->jse", whole_rows, w_qkv, preferred_element_type=wide)
    qv_flat = qv_full.astype(wide).reshape(2, width)
    queries = (projected[0] + qv_flat[0]).astype(narrow)
    all_keys = projected[1].astype(narrow)
    all_values = (projected[2] + qv_flat[1]).astype(narrow)
    bounds, seg_row, seg_keys, pad_row = side_tables(segment_ids, padding)
    context_low, context_t, log_totals = attn_fwd(
        bounds, queries, all_keys, all_values, seg_row, seg_keys, pad_row
    )
    attn_part = jnp.dot(context_low, w_proj, preferred_element_type=wide)
    attn_branch = lax.psum_scatter(
        attn_part, "tensor", scatter_dimension=0, tiled=True
    ) + bias_rows[0].astype(wide)
    input_rows = tokens.astype(wide)
    first_norm, first_pull = jax.vjp(
        layer_norm, input_rows + attn_branch, gain_rows[0].astype(wide), shift_rows[0].astype(wide)
    )
    up_use, down_use, up_bias_use = (w_up, w_down, up_bias)
    normed_all = lax.all_gather(first_norm.astype(narrow), "tensor", axis=0, tiled=True)
    pre_act = jnp.dot(normed_all, up_use, preferred_element_type=wide) + up_bias_use.astype(
        wide
    ).reshape(-1)
    acted, gelu_pull = jax.vjp(gelu_exact, pre_act)
    acted_low = acted.astype(narrow)
    ff_part = jnp.dot(acted_low, down_use, preferred_element_type=wide)
    ff_sum = lax.psum_scatter(
        ff_part.astype(jnp.bfloat16), "tensor", scatter_dimension=0, tiled=True
    ).astype(jnp.float32)
    ff_branch = ff_sum + bias_rows[1].astype(wide)
    layer_value, second_pull = jax.vjp(
        layer_norm, first_norm + ff_branch, gain_rows[1].astype(wide), shift_rows[1].astype(wide)
    )
    layer_out = layer_value.astype(narrow)
    live_col = local_pad[:, None]
    squares = jnp.stack(
        [
            jnp.sum(live_col * input_rows * input_rows),
            jnp.sum(live_col * attn_branch * attn_branch),
            jnp.sum(live_col * ff_branch * ff_branch),
        ]
    )
    square_sums, live_count = lax.psum((squares, jnp.sum(local_pad)), ("fsdp", "tensor"))
    root_values = jnp.sqrt(square_sums / (live_count * D))
    d_second, d_gain_two, d_shift_two = second_pull(cotangent.astype(wide))
    d_ff_low = d_second.astype(narrow)
    d_ff_bias = jnp.sum(d_ff_low.astype(wide), axis=0)
    d_ff_all = lax.all_gather(d_ff_low, "tensor", axis=0, tiled=True)
    d_down = jnp.einsum("sf,sd->fd", acted_low, d_ff_all, preferred_element_type=wide)
    d_acted = jnp.einsum("sd,fd->sf", d_ff_all, down_use, preferred_element_type=wide)
    d_pre_low = gelu_pull(d_acted)[0].astype(narrow)
    d_up_bias = jnp.sum(d_pre_low.astype(wide), axis=0).reshape(up_bias_use.shape)
    d_up = jnp.einsum("sd,sf->df", normed_all, d_pre_low, preferred_element_type=wide)
    d_norm_part = jnp.einsum("sf,df->sd", d_pre_low, up_use, preferred_element_type=wide)
    d_first_in = d_second + lax.psum_scatter(d_norm_part, "tensor", scatter_dimension=0, tiled=True)
    d_first, d_gain_one, d_shift_one = first_pull(d_first_in)
    d_attn_low = d_first.astype(narrow)
    d_attn_bias = jnp.sum(d_attn_low.astype(wide), axis=0)
    d_attn_all = lax.all_gather(d_attn_low, "tensor", axis=0, tiled=True)
    d_proj = jnp.einsum("se,sd->ed", context_low, d_attn_all, preferred_element_type=wide)
    d_context = jnp.einsum("sd,ed->se", d_attn_all, w_proj, preferred_element_type=wide).astype(
        narrow
    )
    d_qkv = attn_bwd(
        bounds, queries, all_keys, all_values, d_context, context_t, log_totals,
        seg_row, seg_keys, pad_row,
    )
    d_qkv_wide = d_qkv.astype(wide)
    d_qv_bias = jnp.stack([jnp.sum(d_qkv_wide[0], axis=0), jnp.sum(d_qkv_wide[2], axis=0)]).reshape(
        2, heads, DH
    )
    d_attn_weight = jnp.einsum("sd,jse->jde", whole_rows, d_qkv, preferred_element_type=wide)
    d_tokens_part = jnp.einsum("jse,jde->sd", d_qkv, w_qkv, preferred_element_type=wide)
    d_tokens = d_first + lax.psum_scatter(
        d_tokens_part.astype(jnp.bfloat16), "tensor", scatter_dimension=0, tiled=True
    ).astype(jnp.float32)
    gain_terms, shift_terms, bias_terms = lax.psum(
        (
            jnp.stack([d_gain_one, d_gain_two]),
            jnp.stack([d_shift_one, d_shift_two]),
            jnp.stack([d_attn_bias, d_ff_bias]),
        ),
        "tensor",
    )
    grads = (
        summed_on_arrival(d_attn_weight.astype(jnp.bfloat16), "fsdp", 1),
        summed_on_arrival(d_qv_bias.astype(jnp.bfloat16), "fsdp", 2),
        summed_on_arrival(d_proj.astype(jnp.bfloat16), "fsdp", 1),
        summed_on_arrival(d_up.astype(jnp.bfloat16), "fsdp", 0),
        summed_on_arrival(d_up_bias.astype(jnp.bfloat16), "fsdp", 1),
        *sent_together(
            (
                d_down.astype(jnp.bfloat16),
                gain_terms.astype(jnp.bfloat16),
                shift_terms.astype(jnp.bfloat16),
                bias_terms.astype(jnp.bfloat16),
            ),
            "fsdp",
            1,
            0,
        ),
    )
    return (
        layer_out,
        d_tokens,
        grads[0],
        grads[1],
        grads[2],
        grads[3],
        grads[4],
        grads[5],
        grads[6],
        grads[7],
        grads[8],
        root_values,
    )


def solution(mesh):
    placed = (
        P(("fsdp", "tensor"), None),
        P(None, "fsdp", "tensor"),
        P(None, "tensor", "fsdp"),
        P("tensor", "fsdp"),
        P("fsdp", "tensor"),
        P("tensor", "fsdp"),
        P("tensor", "fsdp"),
        P(None, "fsdp"),
        P(None, "fsdp"),
        P(None, "fsdp"),
        P("fsdp"),
        P("fsdp"),
        P(("fsdp", "tensor"), None),
    )
    return jax.shard_map(
        shards,
        mesh=mesh,
        in_specs=placed,
        out_specs=(
            P(("fsdp", "tensor"), None),
            P(("fsdp", "tensor"), None),
            P(None, "fsdp", "tensor"),
            P(None, "tensor", "fsdp"),
            P("tensor", "fsdp"),
            P("fsdp", "tensor"),
            P("tensor", "fsdp"),
            P("tensor", "fsdp"),
            P(None, "fsdp"),
            P(None, "fsdp"),
            P(None, "fsdp"),
            P(),
        ),
        check_vma=False,
    )
```

```python
import functools

import jax
import jax.numpy as jnp
from jax import lax
from jax.experimental import pallas as pl
from jax.experimental.pallas import tpu as pltpu
from jax.sharding import PartitionSpec as P

DH = 64
EPSILON = 1e-12
BQ = 256
BK = 256
F32 = jnp.float32
BF = jnp.bfloat16
MESH = pl.DeviceIdType.MESH
DMA = pltpu.SemaphoreType.DMA
ROWS = 128
MISC = 16
MOST = 768


def places(n):
    t = lax.axis_index("tensor")
    f = lax.axis_index("fsdp")
    c, x = t % 2, t // 2
    core, cross, diag = 2 * x + 1 - c, 2 * (1 - x) + c, 2 * (1 - x) + 1 - c
    y, z = f % 2, f // 2
    place = z + y * (n - 1 - 2 * z)

    def at(p):
        y = p // max(n // 2, 1)
        return 2 * (p + y * (n - 1 - 2 * p)) + y

    return t, f, core, cross, diag, place, at


def send(src, dst, ss, rs, **axes):
    return pltpu.make_async_remote_copy(
        src_ref=src, dst_ref=dst, send_sem=ss, recv_sem=rs, device_id=axes, device_id_type=MESH
    )


def meet(core, cross, ring, *more):
    gate = pltpu.get_barrier_semaphore()
    for where in (core, cross) + more:
        pl.semaphore_signal(gate, inc=1, device_id={"tensor": where}, device_id_type=MESH)
    for where in ring:
        pl.semaphore_signal(gate, inc=1, device_id={"fsdp": where}, device_id_type=MESH)
    pl.semaphore_wait(gate, 2 + len(ring) + len(more))


def both_ways(n, place, at, local, held, sems):
    rs, rr, ls, lr = sems
    nxt, prv = at((place + 1) % n), at((place + n - 1) % n)
    far = n // 2
    half = local.shape[0] // 2
    steps = []
    for s in range(far):
        a, b = at((place - s + n) % n), at((place + s) % n)
        up = local if s == 0 else held.at[a]
        down = local if s == 0 else held.at[b]
        row = []
        for k in (0, 1):
            part = pl.ds(k * half, half)
            if s < far - 1 or k == 0:
                row.append(send(up.at[part], held.at[a, part], rs.at[s, k], rr.at[s, k], fsdp=nxt))
            if s < far - 1 or k == 1:
                row.append(send(down.at[part], held.at[b, part], ls.at[s, k], lr.at[s, k], fsdp=prv))
        steps.append(row)
    return steps


def ring_on(steps, s):
    for i, c in enumerate(steps[s]):
        if s < len(steps) - 1:
            steps[s - 1][i].wait_recv()
            c.start()
    if s == len(steps) - 1:
        steps[s - 1][0].wait_recv()
        steps[s][0].start()
        steps[s - 1][1].wait_recv()
        steps[s - 1][2].wait_recv()
        steps[s - 1][3].wait_recv()
        steps[s][1].start()


def ring_end(steps):
    for c in steps[-1]:
        c.wait_recv()
    for row in steps:
        for c in row:
            c.wait_send()


def mm(a, b, ca=1, cb=0):
    return lax.dot_general(a, b, (((ca,), (cb,)), ((), ())), preferred_element_type=F32)


def some(ref, rows, c0, c1, j, count):
    g = ref.shape[0]
    if g % count:
        size = rows // count
        return ref[0, j * size : (j + 1) * size, c0:c1]
    g //= count
    return ref[j * g : (j + 1) * g, :rows, c0:c1].reshape(g * rows, c1 - c0)


def whole(ref, rows, c0, c1):
    g = ref.shape[0]
    return ref[:, :rows, c0:c1].reshape(g * rows, c1 - c0)


def fold_max(s):
    return jnp.max(s.reshape(s.shape[0] // 8, 8, s.shape[1]), axis=0)


def fold_sum(s):
    return jnp.sum(s.reshape(s.shape[0] // 8, 8, s.shape[1]), axis=0)


def col_sum(s):
    return jnp.sum(fold_sum(s), axis=0, keepdims=True)


def project_kernel(n, ring, *refs):
    refs = list(refs)
    pop = lambda m: [refs.pop(0) for _ in range(m)]
    tok, seg, alive = pop(3)
    if ring:
        far = [seg, alive] + pop(7)
    else:
        (wg,) = pop(1)
    full, qkv, misc, sq, sk, live, lives, bounds = pop(8)
    if ring:
        wg, mine = pop(2)
        near = pop(len(far))
        nsem = pop(1)[0]
        for j in range(len(far)):
            pltpu.make_async_copy(far[j], near[j], nsem.at[j]).start()
    lsem, xs, xr, cs, cr, fs, fr = pop(7)
    gsems = refs
    t, f, core, cross, diag, place, at = places(n)
    rows, d = tok.shape
    part = wg.shape[1] - MISC
    head = qkv.shape[2]
    if ring:
        for j in range(len(far)):
            pltpu.make_async_copy(far[j], near[j], nsem.at[j]).wait()
        seg, alive, aw, ow, gains, shifts, biases, hb, qvb = near
        mine[:part] = jnp.concatenate([aw[0], aw[1], aw[2], ow[...].astype(F32).T.astype(BF)], axis=1)
        col = lax.broadcasted_iota(jnp.int32, (part, d), 1)
        row = lax.broadcasted_iota(jnp.int32, (part, d), 0)
        spread = (col == f * part + row).astype(BF)
        wide = [mm(r[...], spread) for r in (gains, shifts, biases)]
        k = hb.shape[0]
        col = lax.broadcasted_iota(jnp.int32, (k, d), 1)
        row = lax.broadcasted_iota(jnp.int32, (k, d), 0)
        spread = (col % DH == f * k + row).astype(BF)
        h = mm(hb[...].astype(F32).T.astype(BF), spread)
        col = lax.broadcasted_iota(jnp.int32, h.shape, 1) // DH
        row = lax.broadcasted_iota(jnp.int32, h.shape, 0)
        h = jnp.sum(jnp.where(col == row, h, 0.0), axis=0, keepdims=True)
        b = jnp.zeros((1, d), F32)
        col = lax.broadcasted_iota(jnp.int32, (1, d), 1) // DH
        heads = qvb.shape[0]
        for j in range(heads):
            x = mm(qvb[j], spread)
            b = jnp.where(col == j, x[0:1], jnp.where(col == 2 * heads + j, x[1:2], b))
        mine[part:] = jnp.concatenate(wide + [h, b, jnp.zeros((8, d), F32)], axis=0).astype(BF)
        steps = both_ways(n, place, at, mine, wg, gsems)
        meet(core, cross, (at((place + 1) % n), at((place + n - 1) % n)))
    else:
        meet(core, cross, ())
    R = range(rows // ROWS)
    cut = lambda i: pl.ds(i * ROWS, ROWS)
    xc = [send(tok.at[cut(i)], full.at[t, cut(i)], xs.at[i], xr.at[i], tensor=cross) for i in R]
    cc = [send(tok.at[cut(i)], full.at[t, cut(i)], cs.at[i], cr.at[i], tensor=core) for i in R]
    fc = [send(full.at[cross, cut(i)], full.at[cross, cut(i)], fs.at[i], fr.at[i], tensor=core) for i in R]
    own = [pltpu.make_async_copy(tok, full.at[t], lsem.at[0])]
    if ring:
        own.append(pltpu.make_async_copy(mine, wg.at[f], lsem.at[1]))
        for c in steps[0]:
            c.start()
    for c in xc + cc + own:
        c.start()

    groups = seg.shape[0]
    ids = seg[...].astype(F32)
    on = alive[...]
    keys = jnp.where(on == 1, ids, -1.0)
    onf = on.astype(F32)
    for g in range(groups):
        c = slice(g * 128, (g + 1) * 128)
        sq[:, c] = ids[g : g + 1]
        live[:, c] = onf[g : g + 1]
        sk[c, :] = jnp.broadcast_to(keys[g : g + 1], (128, 128)).T
        lives[c, :] = jnp.broadcast_to(onf[g : g + 1], (128, 128)).T
    per = BQ // 128
    for i in range(groups // per):
        under = jnp.sum((ids < ids[i * per : i * per + 1, 0:1]).astype(F32))
        upto = jnp.sum((ids <= ids[(i + 1) * per - 1 : (i + 1) * per, 127:128]).astype(F32))
        bounds[2 * i] = under.astype(jnp.int32) // BK
        bounds[2 * i + 1] = (upto.astype(jnp.int32) + BK - 1) // BK

    if ring:
        for s in range(1, len(steps)):
            ring_on(steps, s)
    for i in R:
        xc[i].wait_recv()
        fc[i].start()
    for c in own:
        c.wait()
    for c in cc:
        c.wait_recv()
    if ring:
        ring_end(steps)
    misc[...] = jnp.sum(wg[:, part:, :].astype(F32), axis=0)
    w = 3 * head

    def block(i):
        p = mm(full[i], whole(wg, part, 0, w)) + misc[7:8, :w]
        for j in range(3):
            qkv[j, pl.ds(i * rows, rows), :] = p[:, j * head : (j + 1) * head].astype(BF)

    def three(j, _):
        block(lax.select(j == 0, t, lax.select(j == 1, core, cross)))
        return 0

    lax.fori_loop(0, 3, three, 0)
    for c in fc:
        c.wait_recv()
    block(diag)
    for c in xc + cc + fc:
        c.wait_send()


def project(n, tok, head, seg, alive, raw=None, wg=None):
    ring = wg is None
    vm = pl.BlockSpec(memory_space=pltpu.VMEM)
    rows, d = tok.shape
    nch = rows // ROWS
    s = jax.ShapeDtypeStruct
    total = 4 * rows
    outs = [
        s((4, rows, d), BF),
        s((3, total, head), BF),
        s((MISC, d), F32),
        s((1, total), F32),
        s((total, 128), F32),
        s((1, total), F32),
        s((total, 128), F32),
        s((2 * total // BQ,), jnp.int32),
    ]
    specs = [vm] * 7 + [pl.BlockSpec(memory_space=pltpu.SMEM)]
    scratch = [DMA((2,))] + [DMA((nch,))] * 6
    ops = (tok, seg.reshape(-1, 128), alive.reshape(-1, 128))
    if ring:
        ops = tuple(pltpu.with_memory_space_constraint(x, pltpu.HBM) for x in ops + raw)
        outs.append(s((n, d // n + MISC, d), BF))
        specs.append(vm)
        held = [pltpu.VMEM(x.shape, x.dtype) for x in ops[1:]]
        scratch = [pltpu.VMEM((d // n + MISC, d), BF)] + held + [DMA((len(held),))] + scratch + [DMA((n // 2, 2))] * 4
    else:
        ops += (wg,)
    got = pl.pallas_call(
        functools.partial(project_kernel, n, ring),
        in_specs=[pl.BlockSpec(memory_space=pltpu.HBM) if ring else vm] * len(ops),
        out_specs=specs,
        out_shape=outs,
        scratch_shapes=scratch,
        compiler_params=pltpu.CompilerParams(
            collective_id=1, has_side_effects=True, vmem_limit_bytes=2 << 20
        ),
        name="project",
    )(*ops)
    return tuple(got) if ring else tuple(got) + (wg,)


def moments(h):
    mean = jnp.mean(h, axis=-1, keepdims=True)
    c = h - mean
    r = lax.rsqrt(jnp.mean(c * c, axis=-1, keepdims=True) + EPSILON)
    return c * r, r


def norm_back(dy, g, xhat, r):
    dx = dy * g
    return r * (
        dx
        - jnp.mean(dx, axis=-1, keepdims=True)
        - xhat * jnp.mean(dx * xhat, axis=-1, keepdims=True)
    )


def scatter_tools(core, cross, part, cs, cr, xs, xr, sems):
    ccs, ccr, xxs, xxr = sems
    a = lambda i, k: send(cs.at[k], cr.at[k], ccs.at[i, k], ccr.at[i, k], tensor=core)
    b = lambda i, k: send(xs.at[k], xr.at[k], xxs.at[i, k], xxr.at[i, k], tensor=cross)

    def put(i, k, tile, count):
        if i > 0:
            a(i - 1, k).wait_send()
        width = part.shape[-1] // count
        for j in range(count):
            p = tile(j)
            m = p.shape[0] // 4
            c = slice(j * width, (j + 1) * width)
            cs[k, 0, :, c] = p[m : 2 * m].astype(BF)
            cs[k, 1, :, c] = p[3 * m :].astype(BF)
            part[k, 0, :, c] = p[:m]
            part[k, 1, :, c] = p[2 * m : 3 * m]
        a(i, k).start()

    def across(i, k):
        a(i, k).wait_recv()
        if i > 0:
            b(i - 1, k).wait_send()
        xs[k] = (part[k, 1] + cr[k, 1].astype(F32)).astype(BF)
        b(i, k).start()
        part[k, 0] = part[k, 0] + cr[k, 0].astype(F32)

    def take(i, k):
        b(i, k).wait_recv()
        return part[k, 0] + xr[k].astype(F32)

    def end(i, k):
        a(i, k).wait_send()
        b(i, k).wait_send()

    return put, across, take, end


def block_rows(ref, device, c0, c1, n):
    size = ref.shape[0] // n
    return ref.at[pl.ds(pl.multiple_of(device * size, size), size), pl.ds(c0, c1 - c0)]


class RingSum:
    def __init__(self, n, place, at, local, c0, c1, rbuf, ss, rs, right):
        self.n, self.rbuf = n, rbuf
        target = at((place + 1) % n) if right else at((place + n - 1) % n)
        step = -1 if right else 1
        self.own = lambda s: block_rows(local, at((place + step * (1 + s) + 2 * n) % n), c0, c1, n)

        def copy(s):
            src = self.own(0) if s == 0 else rbuf.at[s - 1]
            return send(src, rbuf.at[s], ss.at[s], rs.at[s], fsdp=target)

        self.copy = copy

    def go(self, s):
        if s > 0:
            self.copy(s - 1).wait_recv()
            self.rbuf[s - 1] = (self.rbuf[s - 1].astype(F32) + self.own(s)[...].astype(F32)).astype(BF)
        self.copy(s).start()

    def close(self):
        s = self.n - 2
        self.copy(s).wait_recv()
        return self.rbuf[s].astype(F32) + self.own(s + 1)[...].astype(F32)

    def sent(self):
        for s in range(self.n - 1):
            self.copy(s).wait_send()


def ring_group(n, place, at, local, tracks):
    m = len(tracks)
    q = [RingSum(n, place, at, local, j * 128, j * 128 + 128, *tracks[j], j < m // 2) for j in range(m)]
    left = list(range(n - 1))

    def go():
        if left:
            s = left.pop(0)
            for j in range(m // 2):
                q[j].go(s)
                q[j + m // 2].go(s)

    def close():
        while left:
            go()
        x = jnp.concatenate([r.close() for r in q], axis=1)
        for r in q:
            r.sent()
        return x

    return go, close


def ring_scratch(n, rows, widths):
    out = []
    for w in widths:
        out += [pltpu.VMEM((n - 1, rows, w), BF)]
        out += [DMA((n - 1,)), DMA((n - 1,))]
    return out


def attend_block(i, lo, hi, heads, sq_ref, sk_ref, pad_ref, qt, kh, vt, sc, ctx_ref, octx_ref, lse_ref):
    q0 = pl.multiple_of(i * BQ, BQ)
    sq = sq_ref[0:1, pl.ds(q0, BQ)]
    qpos = q0 + lax.broadcasted_iota(jnp.int32, (BK, BQ), 1)
    part = sc.shape[1] // BK
    spot = lambda h, j: (sc.shape[0] // heads * h + j // part, pl.ds(pl.multiple_of(j % part * BK, BK), BK), slice(None))

    def first(j, c):
        k0 = pl.multiple_of(j * BK, BK)
        sk = jnp.concatenate([sk_ref[pl.ds(k0, BK), :]] * (BQ // 128), axis=1)
        kpos = k0 + lax.broadcasted_iota(jnp.int32, (BK, BQ), 0)
        ok = (sk == sq) | (kpos == qpos)
        out = []
        for h in range(heads):
            s = jnp.where(ok, mm(kh(h, j)[...], qt(h, i)[...]), -1e30)
            sc[spot(h, j)] = s
            out.append(jnp.maximum(c[h], fold_max(s)))
        return tuple(out)

    m = lax.fori_loop(lo, hi, first, (jnp.full((8, BQ), -3e38, F32),) * heads)
    m = [jnp.max(x, axis=0, keepdims=True) for x in m]

    def second(j, c):
        out = []
        for h in range(heads):
            l, acc = c[2 * h : 2 * h + 2]
            p = jnp.exp(sc[spot(h, j)] - m[h])
            out += [l + fold_sum(p), acc + mm(vt(h, j)[...], p.astype(BF))]
        return tuple(out)

    c = lax.fori_loop(lo, hi, second, (jnp.zeros((8, BQ), F32), jnp.zeros((DH, BQ), F32)) * heads)
    o = []
    for h in range(heads):
        l, acc = c[2 * h : 2 * h + 2]
        l = jnp.sum(l, axis=0, keepdims=True)
        lse_ref[h : h + 1, pl.ds(q0, BQ)] = m[h] + jnp.log(l)
        o.append(acc / l)
    ot = jnp.concatenate(o, axis=0) * pad_ref[0:1, pl.ds(q0, BQ)]
    octx_ref[:, pl.ds(q0, BQ)] = ot
    ctx_ref[pl.ds(q0, BQ), :] = ot.T.astype(BF)


def middle_kernel(n, ring, *refs):
    refs = list(refs)
    pop = lambda m: [refs.pop(0) for _ in range(m)]
    qkv, sq, sk, live_row, wg, misc, full, cot_hbm, pad = pop(9)
    if ring:
        wh, wd = pop(2)
    else:
        (wf,) = pop(1)
    out, dfirst, dctx, octx, lse, gout, gup, odown, sums = pop(9)
    gdown = odown
    if ring:
        (wf, gdown) = pop(2)
    ctx, call, slab, wo, dsend = pop(5)
    (norm, dff, acted, dgelu, pre, dpre, first, xhat, r1, part, csem, lsem) = pop(12)
    cs, cr, xs, xr = pop(4)
    ocs, ocr, oxs, oxr = pop(4)
    rsem = pop(4)
    gsem = pop(6)
    osem = pop(4)
    ssem = pop(6)
    asem = pop(6)
    dsem = pop(6)
    ff = wf.shape[2] // 2
    if ring:
        wsem = pop(4)
        tracks = [pop(3) for _ in range(ff // 128)]
    t, f, core, cross, diag, place, at = places(n)
    rows, d = out.shape
    fetch = pltpu.make_async_copy(cot_hbm, out, csem.at[0])
    fetch.start()
    nch = rows // ROWS
    wpart = wg.shape[1] - MISC
    fpart = wf.shape[1]
    width = ctx.shape[1]
    heads = width // DH
    where = (t, core, cross, diag)
    put, across, take, end = scatter_tools(core, cross, part, cs, cr, xs, xr, rsem)
    gs = {}
    for i, buf in enumerate((norm, dff)):
        gs[i] = (
            lambda k, buf=buf, i=i: send(buf.at[k, 0], buf.at[k, 2], gsem[0].at[i, k], gsem[1].at[i, k], tensor=cross),
            lambda k, buf=buf, i=i: send(buf.at[k, 0], buf.at[k, 1], gsem[2].at[i, k], gsem[3].at[i, k], tensor=core),
            lambda k, buf=buf, i=i: send(buf.at[k, 2], buf.at[k, 3], gsem[4].at[i, k], gsem[5].at[i, k], tensor=core),
        )

    def share(i, k):
        gs[i][0](k).start()
        gs[i][1](k).start()

    def shared(i, k):
        gs[i][0](k).wait_recv()
        gs[i][2](k).start()
        gs[i][1](k).wait_recv()
        gs[i][2](k).wait_recv()

    lane0 = d - slab.shape[-1]
    mine = wg.at[:, pl.ds(0, wpart), pl.ds(lane0, slab.shape[-1])]
    slabs = (
        send(mine, slab.at[1], ssem[0].at[0], ssem[1].at[0], tensor=cross),
        send(mine, slab.at[0], ssem[2].at[0], ssem[3].at[0], tensor=core),
        send(slab.at[1], slab.at[2], ssem[4].at[0], ssem[5].at[0], tensor=core),
    )

    def rows_at(w, k):
        return pl.ds(pl.multiple_of(w * rows + k * ROWS, ROWS), ROWS)

    def give(j, k):
        return send(ctx.at[rows_at(where[j], k), :], call.at[k, j], asem[2 * j - 2].at[k], asem[2 * j - 1].at[k], tensor=where[j])

    def back(j, k):
        return send(dsend.at[k, j - 1], dctx.at[rows_at(t, k), :], dsem[2 * j - 2].at[k], dsem[2 * j - 1].at[k], tensor=where[j])

    if ring:
        load = [
            pltpu.make_async_copy(wh, wf.at[f, :, pl.ds(0, ff)], lsem.at[0]),
            pltpu.make_async_copy(wd, wf.at[f, :, pl.ds(ff, ff)], lsem.at[1]),
        ]
        for c in load:
            c.start()
        for c in load:
            c.wait()
        steps = both_ways(n, place, at, wf.at[f], wf, wsem)
        meet(core, cross, (at((place + 1) % n), at((place + n - 1) % n)), diag)
        for c in steps[0]:
            c.start()
    else:
        meet(core, cross, (), diag)
    slabs[0].start()
    slabs[1].start()
    sums[...] = jnp.zeros_like(sums)

    blocks = 4 * rows // BQ
    across_lanes = d // BQ

    def turned(top):
        def tile(h, i):
            lanes = pl.ds(pl.multiple_of(i % across_lanes * BQ, BQ), BQ)
            return dff.at[h, i // across_lanes, pl.ds(top, DH), lanes]

        return tile

    qt, vt = turned(0), turned(DH)
    stack = 4 * ROWS // BK

    def kh(h, j):
        lanes = pl.ds(pl.multiple_of(j // stack * 128, 128), DH)
        return acted.at[h, pl.ds(pl.multiple_of(j % stack * BK, BK), BK), lanes]

    def prepare(i, _):
        r = pl.ds(pl.multiple_of(i * BQ, BQ), BQ)
        qs = (qkv[0, r, :].astype(F32) * 0.125).T.astype(BF)
        vs = qkv[2, r, :].astype(F32).T.astype(BF)
        ks = qkv[1, r, :]
        for h in range(heads):
            c = slice(h * DH, (h + 1) * DH)
            qt(h, i)[...] = qs[c]
            vt(h, i)[...] = vs[c]
            kh(h, i)[...] = ks[:, c]
        return 0

    lax.fori_loop(0, blocks, prepare, 0)
    reach = (MOST - 2 + BK) // BK

    def attend(base, stride, count):
        def body(i, _):
            b = base + i * stride
            lo = jnp.maximum(b - reach, 0)
            hi = jnp.minimum(b + reach + 1, blocks)
            attend_block(b, lo, hi, heads, sq, sk, live_row, qt, kh, vt, dgelu, ctx, octx, lse)
            return 0

        lax.fori_loop(0, count, body, 0)

    def give_when(sent):
        for w in range(4):
            ks = [k for k in range(nch) if k in sent[w]]
            for j in (3, 2, 1):

                @pl.when(where[j] == w)
                def _(j=j, ks=ks):
                    for k in ks:
                        give(j, k).start()

    def rows_of(k):
        return pl.ds(pl.multiple_of(k * ROWS, ROWS), ROWS)

    def pad_rows(k):
        return pad[rows_at(t, k), 0:1]

    def live(k, x):
        s = jnp.sum(x * x, axis=-1, keepdims=True) * pad_rows(k)
        return jnp.sum(s, axis=0, keepdims=True)

    lane = lax.broadcasted_iota(jnp.int32, (1, d), 1)

    def note(j, v):
        sums[7:8, :] += jnp.where(lane == d // 2 + j, v, 0.0)

    def norm_one(k):
        for j in (1, 2, 3):
            give(j, k).wait_recv()
        call[k, 0] = ctx[rows_at(t, k), :]
        x = full[t, rows_of(k), :].astype(F32)
        branch = misc[4:5, :]
        for j in range(4):
            branch = branch + mm(call[k, j], wo[j], 1, 1)
        xh, r = moments(x + branch)
        y = xh * misc[0:1, :] + misc[2:3, :]
        first[k] = y
        xhat[k] = xh
        r1[k] = r
        norm[k, 0] = y.astype(BF)
        share(0, k)
        note(0, live(k, x))
        note(1, live(k, branch))
        note(3, jnp.sum(pad_rows(k), axis=0, keepdims=True))

    def loop(fn):
        def body(k, _):
            fn(k)
            return 0

        lax.fori_loop(0, nch, body, 0)

    done, whole_rows = set(), [set() for _ in range(4)]

    def ran(ids):
        done.update(r for b in ids for r in range(b * BQ // ROWS, (b + 1) * BQ // ROWS))
        fresh = [
            {k for k in range(nch) if w * nch + k in done and k not in whole_rows[w]} for w in range(4)
        ]
        for w in range(4):
            whole_rows[w] |= fresh[w]
        give_when(fresh)

    attend(0, 1, 2)
    ran((0, 1))
    if ring:
        ring_on(steps, 1)
    attend(3, 1, 2)
    ran((3, 4))
    slabs[0].wait_recv()
    slabs[2].start()
    if ring:
        ring_on(steps, 2)
    attend(2, 1, 1)
    slabs[1].wait_recv()
    slabs[2].wait_recv()
    wo[0] = whole(wg, wpart, lane0, d)[:, -width:]
    for j in range(3):
        wo[j + 1] = slab[j].reshape(d, slab.shape[-1])[:, -width:]
    norm_one(0)
    attend(5, 1, 1)
    ran((2, 5))
    if ring:
        for s in range(3, len(steps)):
            ring_on(steps, s)
    for k in range(1, nch):
        norm_one(k)
    if ring:
        ring_end(steps)
    inv = 0.7071067811865476
    thirds = ff // BQ

    def feed(k):
        shared(0, k)
        def half(b):
            x = norm[k, 2 * b : 2 * b + 2].reshape(2 * ROWS, d)
            for c in range(0, ff, 256):
                pre[:, c : c + 256] = mm(x, whole(wf, fpart, c, c + 256)) + misc[6:7, c : c + 256]

        def act(i, b):
            u = pre[pl.ds(pl.multiple_of(i * 64, 64), 64), :]
            s = pl.ds(pl.multiple_of(b * 2 * ROWS + i * 64, 64), 64)
            cdf = 0.5 + 0.5 * lax.erf(u * inv)
            acted[k, s, :] = (u * cdf).astype(BF)
            slope = cdf + u * (jnp.exp(-0.5 * u * u) * 0.3989422804014327)
            for c in range(thirds):
                dgelu[k * thirds + c, s, :] = slope[:, c * BQ : (c + 1) * BQ]
            return b

        half(0)
        pl.when(k > 0)(lambda: across(0, k - 1))
        lax.fori_loop(0, 2 * ROWS // 64, act, 0)
        half(1)
        lax.fori_loop(0, 2 * ROWS // 64, act, 1)
        put(0, k, lambda j: mm(acted[k], some(wf, fpart, ff, 2 * ff, j, 2), 1, 1), 2)

    loop(feed)
    across(0, nch - 1)
    fetch.wait()

    def norm_two(k):
        branch = take(0, k) + misc[5:6, :]
        xh, r = moments(first[k] + branch)
        dy = out[rows_of(k), :].astype(F32)
        out[rows_of(k), :] = (xh * misc[1:2, :] + misc[3:4, :]).astype(BF)
        ds = norm_back(dy, misc[1:2, :], xh, r)
        first[k] = ds
        low = ds.astype(BF)
        dff[k, 0] = low
        share(1, k)
        note(2, live(k, branch))
        sums[1:2, :] += col_sum(dy * xh)
        sums[3:4, :] += col_sum(dy)
        sums[5:6, :] += col_sum(low.astype(F32))

    loop(norm_two)

    def feed_back(k):
        shared(1, k)
        def half(b):
            g = dff[k, 2 * b : 2 * b + 2].reshape(2 * ROWS, d)
            for c in range(0, ff, 256):
                pre[:, c : c + 256] = mm(g, whole(wf, fpart, ff + c, ff + c + 256))

        def act(i, b):
            r = pl.ds(pl.multiple_of(i * 64, 64), 64)
            s = pl.ds(pl.multiple_of(b * 2 * ROWS + i * 64, 64), 64)
            slope = jnp.concatenate([dgelu[k * thirds + c, s, :] for c in range(thirds)], axis=1)
            low = (pre[r, :] * slope).astype(BF)
            dpre[k, s, :] = low
            sums[6:7, :] += col_sum(low.astype(F32))
            return b

        half(0)
        pl.when(k > 0)(lambda: across(1, k - 1))
        lax.fori_loop(0, 2 * ROWS // 64, act, 0)
        half(1)
        lax.fori_loop(0, 2 * ROWS // 64, act, 1)
        put(1, k, lambda j: mm(dpre[k], some(wf, fpart, 0, ff, j, 2), 1, 1), 2)

    def weight_part(left, right, to):
        def cols(i, _):
            c = pl.ds(pl.multiple_of(i * 128, 128), 128)
            g = 0.0
            for k in range(nch):
                g = g + mm(left[k, :, :, c].reshape(4 * ROWS, 128), right[k], 0, 0)
            to[c, :] = g.astype(BF)
            return 0

        lax.fori_loop(0, d // 128, cols, 0)

    def norm_one_back(k):
        dy = first[k] + take(1, k)
        xh = xhat[k]
        ds = norm_back(dy, misc[0:1, :], xh, r1[k])
        dfirst[rows_of(k), :] = ds
        low = ds.astype(BF)
        for c in gs[1][:2]:
            c(k).wait_send()
        dff[k, 0] = low
        for j in (3, 2, 1):
            dsend[k, j - 1] = mm(low, wo[j]).astype(BF)
            back(j, k).start()
        dctx[rows_at(t, k), :] = mm(low, wo[0]).astype(BF)
        sums[0:1, :] += col_sum(dy * xh)
        sums[2:3, :] += col_sum(dy)
        sums[4:5, :] += col_sum(low.astype(F32))

    oc = send(ocs, ocr, osem[0].at[0], osem[1].at[0], tensor=core)
    ox = send(oxs, oxr, osem[2].at[0], osem[3].at[0], tensor=cross)

    def out_part():
        x = dff[:, 0].reshape(rows, d)
        for slot, j in ((0, 1), (1, 3)):
            ocs[slot] = mm(x, call[:, j].reshape(rows, width), 0, 0).astype(BF)
        oc.start()

    def out_across():
        p = mm(dff[:, 0].reshape(rows, d), call[:, 2].reshape(rows, width), 0, 0)
        oc.wait_recv()
        oxs[...] = (p + ocr[1].astype(F32)).astype(BF)
        ox.start()

    def out_take():
        p = mm(dff[:, 0].reshape(rows, d), call[:, 0].reshape(rows, width), 0, 0)
        ox.wait_recv()
        gout[...] = (p + ocr[0].astype(F32) + oxr[...].astype(F32)).astype(BF)

    loop(feed_back)
    if ring:
        weight_part(dff, acted, gdown)
        across(1, nch - 1)
        go, close = ring_group(n, place, at, gdown, tracks)
        go()
        norm_one_back(0)
        weight_part(norm, dpre, gup)
        go()
        for k in range(1, nch):
            norm_one_back(k)
            go()
        out_part()
        go()
        out_across()
        go()
        go()
        out_take()
        odown[...] = close()
    else:
        across(1, nch - 1)
        weight_part(dff, acted, gdown)
        weight_part(norm, dpre, gup)
        loop(norm_one_back)
        out_part()
        out_across()
        out_take()

    def finish(k, _):
        end(1, k)
        for j in (1, 2, 3):
            back(j, k).wait_recv()
            back(j, k).wait_send()
            give(j, k).wait_send()
        for c in gs[0] + gs[1][2:]:
            c(k).wait_send()
        return 0

    lax.fori_loop(0, nch, finish, 0)
    for c in slabs + (oc, ox):
        c.wait_send()


def middle(n, qkv, sq, sk, live_row, wg, misc, full, cot, pad, wh, wd, wf):
    ring = wf is None
    vm = pl.BlockSpec(memory_space=pltpu.VMEM)
    rows, d = cot.shape
    width = qkv.shape[2]
    heads = width // DH
    total = 4 * rows
    nch = rows // ROWS
    s = jax.ShapeDtypeStruct
    V = pltpu.VMEM
    ff = wh.shape[1] if ring else wf.shape[2] // 2
    outs = [
        s((rows, d), BF),
        s((rows, d), F32),
        s((total, width), BF),
        s((width, total), F32),
        s((heads, total), F32),
        s((d, width), BF),
        s((d, ff), BF),
        s((d // n, ff), F32) if ring else s((d, ff), BF),
        s((8, d), F32),
    ]
    far = pl.BlockSpec(memory_space=pltpu.HBM)
    pin = lambda x: pltpu.with_memory_space_constraint(x, pltpu.HBM)
    ops = (qkv, sq, sk, live_row, wg, misc, full, pin(cot), pad)
    ops += (pin(wh), pin(wd)) if ring else (wf,)
    g, gr = wg.shape[0], wg.shape[1] - MISC
    wide = -(-width // 128) * 128
    scratch = []
    if ring:
        scratch += [V((n, d // n, 2 * ff), BF), V((d, ff), BF)]
    scratch += [V((total, width), BF), V((nch, 4, ROWS, width), BF), V((3, g, gr, wide), BF), V((4, d, width), BF)]
    scratch += [V((nch, 3, ROWS, width), BF)]
    scratch += [V((nch, 4, ROWS, d), BF)] * 2
    scratch += [V((nch, 4 * ROWS, ff), BF), V((nch * (ff // BQ), 4 * ROWS, BQ), F32), V((2 * ROWS, ff), F32), V((nch, 4 * ROWS, ff), BF)]
    scratch += [V((nch, ROWS, d), F32)] * 2 + [V((nch, ROWS, 1), F32)]
    scratch += [V((nch, 2, ROWS, d), F32), DMA((1,)), DMA((2,))]
    scratch += [V((nch, 2, ROWS, d), BF)] * 2 + [V((nch, ROWS, d), BF)] * 2
    scratch += [V((2, d, width), BF)] * 2 + [V((d, width), BF)] * 2
    scratch += [DMA((2, nch))] * 10 + [DMA((1,))] * 10 + [DMA((nch,))] * 12
    if ring:
        scratch += [DMA((n // 2, 2))] * 4 + ring_scratch(n, d // n, (128,) * (ff // 128))
    return pl.pallas_call(
        functools.partial(middle_kernel, n, ring),
        in_specs=[vm] * 7 + [far, vm] + [far if ring else vm] * (len(ops) - 9),
        out_specs=[vm] * len(outs),
        out_shape=outs,
        scratch_shapes=scratch,
        compiler_params=pltpu.CompilerParams(
            collective_id=2, has_side_effects=True, vmem_limit_bytes=41 << 20
        ),
        name="middle",
    )(*ops)


def last_kernel(n, ring, *refs):
    refs = list(refs)
    pop = lambda m: [refs.pop(0) for _ in range(m)]
    dqkv, wg, full, gout, dfirst, sums = pop(6)
    if ring:
        (gup,) = pop(1)
        dtok, oattn, oout, oup, ogain, oshift, obias, ohb, oqvb, oroot = pop(10)
    else:
        dtok, gb, total = pop(3)
    part, cs, cr, xs, xr = pop(5)
    rsem = pop(4)
    msend, mrecv = pop(2)
    msem = pop(4)
    if ring:
        gb, mall = pop(2)
        mring = pop(4)
        tracks = [refs[i : i + 3] for i in range(0, len(refs), 3)]
    t, f, core, cross, diag, place, at = places(n)
    rows, d = dtok.shape
    nch = rows // ROWS
    wpart = wg.shape[1] - MISC
    w3 = dqkv.shape[1]
    width = w3 // 3
    where = (t, core, cross, diag)
    put, across, take, end = scatter_tools(core, cross, part, cs, cr, xs, xr, rsem)
    nxt, prv = at((place + 1) % n), at((place + n - 1) % n)

    def rows_of(k):
        return pl.ds(pl.multiple_of(k * ROWS, ROWS), ROWS)

    b = col_sum(dqkv[...].astype(F32))
    b = jnp.concatenate([b[:, :width], b[:, 2 * width :], jnp.zeros((1, d - 2 * width), F32)], axis=1)
    msend[0] = sums[...]
    msend[0, 7:8, :] = sums[7:8, :] + b
    meet(core, cross, (nxt, prv) if ring else ())
    m0 = send(msend.at[0], mrecv.at[0], msem[0].at[0], msem[1].at[0], tensor=core)
    m1 = send(msend.at[1], mrecv.at[1], msem[2].at[0], msem[3].at[0], tensor=cross)
    if ring:
        ups = gup.shape[1] // 128
        up, up_close = ring_group(n, place, at, gup, tracks[:ups])
        up()
    m0.start()

    def weight_part(i, _):
        c = pl.ds(pl.multiple_of(i * 128, 128), 128)
        g = 0.0
        for j in range(4):
            g = g + mm(full[j, :, c], dqkv[j * rows : (j + 1) * rows, :], 0, 0)
        gb[c, :] = jnp.concatenate([g.astype(BF), gout[c, :]], axis=1)
        return 0

    lax.fori_loop(0, d // 128, weight_part, 0)
    if ring:
        up()
        own, own_close = ring_group(n, place, at, gb, tracks[ups:])
        own()

        def go():
            up()
            own()

    def tokens_part(k):
        x = jnp.concatenate([dqkv[pl.ds(w * rows + k * ROWS, ROWS), :] for w in where], axis=0)
        put(0, k, lambda j: mm(x, some(wg, wpart, 0, w3, j, 2), 1, 1), 2)

    for k in range(nch):
        tokens_part(k)
        if k > 0:
            across(0, k - 1)
        if ring and k > 0:
            go()
    across(0, nch - 1)
    m0.wait_recv()
    msend[1] = msend[0] + mrecv[0]
    m1.start()
    if ring:
        go()
    m1.wait_recv()
    row = lax.broadcasted_iota(jnp.int32, (8, d), 0)
    col = lax.broadcasted_iota(jnp.int32, (8, d), 1)
    over_tensor = (row < 6) | ((row == 7) & (col >= 2 * width))
    small = jnp.where(over_tensor, msend[1] + mrecv[1], msend[0])

    def keep(k):
        dtok[rows_of(k), :] = dfirst[rows_of(k), :] + take(0, k)

    if ring:
        msend[2] = small
        mall[place] = small
        msteps = []
        far = n // 2
        for s in range(far):
            a, b = (place - s + n) % n, (place + s) % n
            src = msend.at[2] if s == 0 else mall.at[a]
            pair = [send(src, mall.at[a], mring[0].at[s], mring[1].at[s], fsdp=nxt)]
            if s < far - 1:
                src = msend.at[2] if s == 0 else mall.at[b]
                pair.append(send(src, mall.at[b], mring[2].at[s], mring[3].at[s], fsdp=prv))
            msteps.append(pair)
        todo = [functools.partial(keep, k) for k in range(nch)]
        r = 0
        for _ in range(max(nch, far, n)):
            if r < far:
                for i, c in enumerate(msteps[r]):
                    if r > 0:
                        msteps[r - 1][i].wait_recv()
                    c.start()
                r += 1
            go()
            if todo:
                todo.pop(0)()
        msteps[far - 2][1].wait_recv()
        msteps[far - 1][0].wait_recv()
        total = jnp.sum(mall[...], axis=0)
        gp = d // n
        mine = pltpu.roll(total, (d - f * gp) % d, 1)
        ogain[...] = mine[0:2, :gp]
        oshift[...] = mine[2:4, :gp]
        obias[...] = mine[4:6, :gp]
        k = DH // n
        mine = pltpu.roll(total, (d - f * k) % d, 1)
        ohb[...] = jnp.concatenate([mine[6:7, h * DH : (h + 1) * DH] for h in range(ohb.shape[1])], axis=0).T[:k]
        heads = oqvb.shape[0]
        for h in range(heads):
            for j in range(2):
                c = (j * heads + h) * DH
                oqvb[h, j : j + 1, :] = mine[7:8, c : c + DH][:, :k]
        spot = lax.broadcasted_iota(jnp.int32, (1, d), 1) - d // 2
        pick = lambda j: jnp.sum(jnp.where(spot == j, total[7:8], 0.0), axis=1, keepdims=True)
        count = pick(3)
        col = lax.broadcasted_iota(jnp.int32, (1, 128), 1)
        o = jnp.zeros((1, 128), F32)
        for j in range(3):
            o = jnp.where(col == j, jnp.sqrt(pick(j) / (count * d)), o)
        oroot[...] = o
        oup[...] = up_close()
        x = own_close()
        for j in range(3):
            oattn[j] = x[:, j * width : (j + 1) * width]
        oout[...] = x[:, 3 * width :].T
        for pair in msteps:
            for c in pair:
                c.wait_send()
    else:
        total[...] = small
        for k in range(nch):
            keep(k)

    def finish(k, _):
        end(0, k)
        return 0

    lax.fori_loop(0, nch, finish, 0)
    m0.wait_send()
    m1.wait_send()


def last(n, ring, dqkv, wg, full, gout, dfirst, sums, gup):
    vm = pl.BlockSpec(memory_space=pltpu.VMEM)
    rows, d = dfirst.shape
    width = dqkv.shape[1] // 3
    heads = width // DH
    nch = rows // ROWS
    s = jax.ShapeDtypeStruct
    V = pltpu.VMEM
    ops = (dqkv, wg, full, gout, dfirst, sums)
    outs = [s((rows, d), F32)]
    gp = d // n
    k = DH // n
    if ring:
        ops += (gup,)
        outs += [s((3, gp, width), F32), s((width, gp), F32), s((gp, gup.shape[1]), F32)] + [s((2, gp), F32)] * 3
        outs += [s((k, d // DH), F32), s((heads, 2, k), F32), s((1, 128), F32)]
    else:
        outs += [s((d, d), BF), s((8, d), F32)]
    scratch = [V((nch, 2, ROWS, d), F32)]
    scratch += [V((nch, 2, ROWS, d), BF)] * 2 + [V((nch, ROWS, d), BF)] * 2
    scratch += [DMA((1, nch))] * 4
    scratch += [V((3, 8, d), F32), V((2, 8, d), F32)] + [DMA((1,))] * 4
    if ring:
        scratch += [V((d, d), BF), V((n, 8, d), F32)] + [DMA((n // 2,))] * 4
        scratch += ring_scratch(n, gp, (128,) * ((gup.shape[1] + d) // 128))
    return pl.pallas_call(
        functools.partial(last_kernel, n, ring),
        in_specs=[vm] * len(ops),
        out_specs=[vm] * len(outs),
        out_shape=outs,
        scratch_shapes=scratch,
        compiler_params=pltpu.CompilerParams(
            collective_id=3, has_side_effects=True, vmem_limit_bytes=12 << 20
        ),
        name="last",
    )(*ops)


def deliver_kernel(*refs):
    m = (len(refs) - 3) // 2
    src, roots, dst, three, sem = refs[:m], refs[m], refs[m + 1 : -2], refs[-2], refs[-1]
    for j in range(m):
        pltpu.make_async_copy(src[j], dst[j], sem.at[j]).start()
    for j in range(three.shape[0]):
        three[j] = jnp.sum(roots[0:1, j : j + 1])
    for j in range(m):
        pltpu.make_async_copy(src[j], dst[j], sem.at[j]).wait()


def deliver(arrays, roots):
    vm = pl.BlockSpec(memory_space=pltpu.VMEM)
    return pl.pallas_call(
        deliver_kernel,
        in_specs=[vm] * (len(arrays) + 1),
        out_specs=[pl.BlockSpec(memory_space=pl.ANY)] * len(arrays) + [pl.BlockSpec(memory_space=pltpu.SMEM)],
        out_shape=[jax.ShapeDtypeStruct(x.shape, x.dtype) for x in arrays] + [jax.ShapeDtypeStruct((3,), F32)],
        scratch_shapes=[DMA((len(arrays),))],
        compiler_params=pltpu.CompilerParams(vmem_limit_bytes=1 << 20),
        name="deliver",
    )(*arrays, roots)


def bwd_kernel(heads, bounds, qkv_ref,dc_ref,oct_ref,lse_ref,sq_ref,sk_ref,pad_ref, dqkv_ref, qt, dt, kt, kh, vh, qh, dh, dqt, dsum, dka, dva):
    S=qkv_ref.shape[1]; W=heads*DH
    qs=(qkv_ref[0].astype(F32)*0.125)
    qsb=qs.astype(BF); qt[...]=qs.T.astype(BF)
    kk=qkv_ref[1]; vv=qkv_ref[2]
    kt[...]=kk.astype(F32).T.astype(BF)
    dct=dc_ref[...].astype(F32).T*pad_ref[0:1,:]
    dt[...]=dct.astype(BF)
    dcn=dct.T.astype(BF)
    prod=dct*oct_ref[...]
    for h in range(heads):
        c=slice(h*DH,(h+1)*DH)
        kh[h]=kk[:,c]; vh[h]=vv[:,c]; qh[h]=qsb[:,c]; dh[h]=dcn[:,c]
        dsum[h:h+1,:]=jnp.sum(prod[h*DH:(h+1)*DH],axis=0,keepdims=True)
    dqt[...]=jnp.zeros_like(dqt)
    def kblock(j,_):
        k0=pl.multiple_of(j*BK,BK)
        lo=bounds[2*j]; hi=bounds[2*j+1]
        sk=jnp.concatenate([sk_ref[pl.ds(k0,BK),:]]*(BQ//128),axis=1)
        kpos=k0+lax.broadcasted_iota(jnp.int32,(BK,BQ),0)
        dka[...]=jnp.zeros_like(dka); dva[...]=jnp.zeros_like(dva)
        def body(i,_):
            q0=pl.multiple_of(i*BQ,BQ)
            sq=sq_ref[0:1,pl.ds(q0,BQ)]
            qpos=q0+lax.broadcasted_iota(jnp.int32,(BK,BQ),1)
            ok=(sk==sq)|(kpos==qpos)
            for h in range(heads):
                r=slice(h*DH,(h+1)*DH)
                s=jnp.where(ok,mm(kh[h,pl.ds(k0,BK),:],qt[r,pl.ds(q0,BQ)]),-1e30)
                p=jnp.exp(s-lse_ref[h:h+1,pl.ds(q0,BQ)])
                dp=mm(vh[h,pl.ds(k0,BK),:],dt[r,pl.ds(q0,BQ)])
                ds=(p*(dp-dsum[h:h+1,pl.ds(q0,BQ)])).astype(BF)
                dva[h]+=mm(p.astype(BF),dh[h,pl.ds(q0,BQ),:])
                dka[h]+=mm(ds,qh[h,pl.ds(q0,BQ),:])
                dqt[r,pl.ds(q0,BQ)]+=mm(kt[r,pl.ds(k0,BK)],ds)
            return 0
        lax.fori_loop(lo,hi,body,0)
        dqkv_ref[pl.ds(k0,BK),W:]=jnp.concatenate([dka[h] for h in range(heads)]+[dva[h] for h in range(heads)],axis=1).astype(BF)
        return 0
    lax.fori_loop(0,S//BK,kblock,0)
    dqkv_ref[:,:W]=(dqt[...]*0.125).T.astype(BF)

def attn_bwd(bounds,qkv,dc,oct,lse,sq,sk,pad):
    _,S,W=qkv.shape; heads=W//DH
    vm=pl.BlockSpec(memory_space=pltpu.VMEM)
    return pl.pallas_call(functools.partial(bwd_kernel,heads),
        in_specs=[pl.BlockSpec(memory_space=pltpu.SMEM)]+[vm]*7,
        out_specs=vm,
        out_shape=jax.ShapeDtypeStruct((S,3*W),BF),
        scratch_shapes=[pltpu.VMEM((W,S),BF)]*3+[pltpu.VMEM((heads,S,DH),BF)]*4+[pltpu.VMEM((W,S),F32),pltpu.VMEM((heads,S),F32)]+[pltpu.VMEM((heads,BK,DH),F32)]*2,
        compiler_params=pltpu.CompilerParams(vmem_limit_bytes=13<<20),
        name="attend_backward")(bounds,qkv,dc,oct,lse,sq,sk,pad)


def split_up(value, dim, devices):
    before, after = (value.shape[:dim], value.shape[dim + 1 :])
    return jnp.moveaxis(value.reshape(*before, devices, -1, *after), dim, 0)


def summed_on_arrival(value, axis, dim):
    blocks = split_up(value, dim, lax.axis_size(axis))
    arrived = lax.all_to_all(blocks, axis, split_axis=0, concat_axis=0, tiled=True)
    return arrived.astype(F32).sum(axis=0)


def shards(
    tokens,
    attn_weight,
    query_value_bias,
    out_weight,
    hidden_weight,
    hidden_bias,
    down_weight,
    norm_gains,
    norm_biases,
    output_biases,
    segment_ids,
    padding,
    cotangent,
):
    n = lax.axis_size("fsdp")
    f = lax.axis_index("fsdp")
    t = lax.axis_index("tensor")
    rows, d = tokens.shape
    gp = d // n
    width = attn_weight.shape[2]
    heads = width // DH
    ff = hidden_weight.shape[1]
    ring = gp % 16 == 0 and n % 2 == 0 and n >= 4
    if ring:
        raw = (
            attn_weight,
            out_weight,
            norm_gains,
            norm_biases,
            output_biases,
            hidden_bias.T,
            query_value_bias.transpose(1, 0, 2),
        )
        got = project(n, tokens, width, segment_ids, padding, raw=raw)
        wh, wd, wf = hidden_weight, down_weight.T, None
    else:
        gather = lambda x, dim: lax.all_gather(x, "fsdp", axis=dim, tiled=True)
        w = gather(attn_weight, 1).transpose(1, 0, 2).reshape(d, 3 * width)
        wo = gather(out_weight, 1).T
        b = gather(query_value_bias, 2).reshape(2, width)
        b = jnp.concatenate([b[0], jnp.zeros((width,), BF), b[1], jnp.zeros((width,), BF)])
        misc = jnp.concatenate(
            [
                gather(norm_gains, 1),
                gather(norm_biases, 1),
                gather(output_biases, 1),
                gather(hidden_bias, 1).reshape(1, ff),
                b[None],
                jnp.zeros((MISC - 8, d), BF),
            ]
        )
        wg = jnp.concatenate([jnp.concatenate([w, wo], axis=1), misc])[None]
        got = project(n, tokens, width, segment_ids, padding, wg=wg)
        wf = jnp.concatenate([gather(hidden_weight, 0), gather(down_weight, 1).T], axis=1)[None]
        wh = wd = None
    full, qkv, misc, seg_row, seg_keys, pad_row, pad_cols, bounds, wg = got
    layer_out, d_first, d_ctx, ctx_t, lse, g_out, g_hidden, g_down, sums = middle(
        n, qkv, seg_row, seg_keys, pad_row, wg, misc, full, cotangent, pad_cols, wh, wd, wf
    )
    d_qkv = attn_bwd(bounds, qkv, d_ctx, ctx_t, lse, seg_row, seg_keys, pad_row)
    done = last(n, ring, d_qkv, wg, full, g_out, d_first, sums, g_hidden)
    if ring:
        done = deliver((layer_out, g_down) + tuple(done[:-1]), done[-1])
        layer_out, g_down, d_tokens, g_attn, g_proj, g_hidden, g_gain, g_shift, g_bias, g_hb, g_qvb, roots = done
        g_down = g_down.T
        g_hb = g_hb.T
        g_qvb = g_qvb.transpose(1, 0, 2)
    else:
        d_tokens, g, total = done
        total = lax.psum(total, "fsdp")
        g_attn = g[:, : 3 * width].reshape(d, 3, width).transpose(1, 0, 2)
        g_attn = summed_on_arrival(g_attn, "fsdp", 1)
        g_proj = summed_on_arrival(g[:, 3 * width :].T, "fsdp", 1)
        g_hidden = summed_on_arrival(g_hidden, "fsdp", 0)
        g_down = summed_on_arrival(g_down.T, "fsdp", 1)
        vectors = lax.dynamic_slice(total, (0, f * gp), (6, gp))
        g_gain, g_shift, g_bias = vectors[0:2], vectors[2:4], vectors[4:6]
        k = DH // n
        g_hb = lax.dynamic_slice(total[6].reshape(ff // DH, DH), (0, f * k), (ff // DH, k))
        g_qvb = lax.dynamic_slice(
            total[7, : 2 * width].reshape(2 * heads, DH), (0, f * k), (2 * heads, k)
        ).reshape(2, heads, k)
        squares = total[7, d // 2 : d // 2 + 4]
        roots = jnp.sqrt(squares[:3] / (squares[3] * d))
    return (
        layer_out,
        d_tokens,
        g_attn,
        g_qvb,
        g_proj,
        g_hidden,
        g_hb,
        g_down,
        g_gain,
        g_shift,
        g_bias,
        roots,
    )


def solution(mesh):
    placed = (
        P(("fsdp", "tensor"), None),
        P(None, "fsdp", "tensor"),
        P(None, "tensor", "fsdp"),
        P("tensor", "fsdp"),
        P("fsdp", "tensor"),
        P("tensor", "fsdp"),
        P("tensor", "fsdp"),
        P(None, "fsdp"),
        P(None, "fsdp"),
        P(None, "fsdp"),
        P("fsdp"),
        P("fsdp"),
        P(("fsdp", "tensor"), None),
    )
    return jax.shard_map(
        shards,
        mesh=mesh,
        in_specs=placed,
        out_specs=(
            P(("fsdp", "tensor"), None),
            P(("fsdp", "tensor"), None),
            P(None, "fsdp", "tensor"),
            P(None, "tensor", "fsdp"),
            P("tensor", "fsdp"),
            P("fsdp", "tensor"),
            P("tensor", "fsdp"),
            P("tensor", "fsdp"),
            P(None, "fsdp"),
            P(None, "fsdp"),
            P(None, "fsdp"),
            P(),
        ),
        check_vma=False,
    )
```

```python
import functools

import jax
import jax.numpy as jnp
from jax import lax
from jax.experimental import pallas as pl
from jax.experimental.pallas import tpu as pltpu
from jax.sharding import PartitionSpec as P

DH = 64
EPSILON = 1e-12
BQ = 256
BK = 256
F32 = jnp.float32
BF = jnp.bfloat16
MESH = pl.DeviceIdType.MESH
DMA = pltpu.SemaphoreType.DMA
ROWS = 128
MISC = 16
MOST = 768


def places(n):
    t = lax.axis_index("tensor")
    f = lax.axis_index("fsdp")
    c, x = t % 2, t // 2
    core, cross, diag = 2 * x + 1 - c, 2 * (1 - x) + c, 2 * (1 - x) + 1 - c
    y, z = f % 2, f // 2
    place = z + y * (n - 1 - 2 * z)

    def at(p):
        y = p // max(n // 2, 1)
        return 2 * (p + y * (n - 1 - 2 * p)) + y

    return t, f, core, cross, diag, place, at


def send(src, dst, ss, rs, **axes):
    return pltpu.make_async_remote_copy(
        src_ref=src, dst_ref=dst, send_sem=ss, recv_sem=rs, device_id=axes, device_id_type=MESH
    )


def meet(core, cross, ring, *more):
    gate = pltpu.get_barrier_semaphore()
    for where in (core, cross) + more:
        pl.semaphore_signal(gate, inc=1, device_id={"tensor": where}, device_id_type=MESH)
    for where in ring:
        pl.semaphore_signal(gate, inc=1, device_id={"fsdp": where}, device_id_type=MESH)
    pl.semaphore_wait(gate, 2 + len(ring) + len(more))


def both_ways(n, place, at, local, held, sems):
    rs, rr, ls, lr = sems
    nxt, prv = at((place + 1) % n), at((place + n - 1) % n)
    far = n // 2
    half = local.shape[0] // 2
    steps = []
    for s in range(far):
        a, b = at((place - s + n) % n), at((place + s) % n)
        up = local if s == 0 else held.at[a]
        down = local if s == 0 else held.at[b]
        row = []
        for k in (0, 1):
            part = pl.ds(k * half, half)
            if s < far - 1 or k == 0:
                row.append(send(up.at[part], held.at[a, part], rs.at[s, k], rr.at[s, k], fsdp=nxt))
            if s < far - 1 or k == 1:
                row.append(send(down.at[part], held.at[b, part], ls.at[s, k], lr.at[s, k], fsdp=prv))
        steps.append(row)
    return steps


def ring_on(steps, s):
    for i, c in enumerate(steps[s]):
        if s < len(steps) - 1:
            steps[s - 1][i].wait_recv()
            c.start()
    if s == len(steps) - 1:
        steps[s - 1][0].wait_recv()
        steps[s][0].start()
        steps[s - 1][1].wait_recv()
        steps[s - 1][2].wait_recv()
        steps[s - 1][3].wait_recv()
        steps[s][1].start()


def ring_end(steps):
    for c in steps[-1]:
        c.wait_recv()
    for row in steps:
        for c in row:
            c.wait_send()


def mm(a, b, ca=1, cb=0):
    return lax.dot_general(a, b, (((ca,), (cb,)), ((), ())), preferred_element_type=F32)


def some(ref, rows, c0, c1, j, count):
    g = ref.shape[0]
    if g % count:
        size = rows // count
        return ref[0, j * size : (j + 1) * size, c0:c1]
    g //= count
    return ref[j * g : (j + 1) * g, :rows, c0:c1].reshape(g * rows, c1 - c0)


def whole(ref, rows, c0, c1):
    g = ref.shape[0]
    return ref[:, :rows, c0:c1].reshape(g * rows, c1 - c0)


def fold_max(s):
    return jnp.max(s.reshape(s.shape[0] // 8, 8, s.shape[1]), axis=0)


def fold_sum(s):
    return jnp.sum(s.reshape(s.shape[0] // 8, 8, s.shape[1]), axis=0)


def col_sum(s):
    return jnp.sum(fold_sum(s), axis=0, keepdims=True)


def project_part(n, ring, tok, far, outs, wg, mine, near, nsem, sems, gsems, lead, follow, ready):
    full, qkv, misc, sq, sk, live, lives, bounds = outs
    if ring:
        for j in range(len(far)):
            pltpu.make_async_copy(far[j], near[j], nsem.at[j]).start()
    else:
        seg, alive = far
    lsem, xs, xr, cs, cr, fs, fr = sems
    t, f, core, cross, diag, place, at = places(n)
    rows, d = tok.shape
    part = wg.shape[1] - MISC
    head = qkv.shape[2]
    if ring:
        for j in range(len(far)):
            pltpu.make_async_copy(far[j], near[j], nsem.at[j]).wait()
        seg, alive, aw, ow, gains, shifts, biases, hb, qvb = near
        mine[:part] = jnp.concatenate([aw[0], aw[1], aw[2], ow[...].astype(F32).T.astype(BF)], axis=1)
        col = lax.broadcasted_iota(jnp.int32, (part, d), 1)
        row = lax.broadcasted_iota(jnp.int32, (part, d), 0)
        spread = (col == f * part + row).astype(BF)
        wide = [mm(r[...], spread) for r in (gains, shifts, biases)]
        k = hb.shape[0]
        col = lax.broadcasted_iota(jnp.int32, (k, d), 1)
        row = lax.broadcasted_iota(jnp.int32, (k, d), 0)
        spread = (col % DH == f * k + row).astype(BF)
        h = mm(hb[...].astype(F32).T.astype(BF), spread)
        col = lax.broadcasted_iota(jnp.int32, h.shape, 1) // DH
        row = lax.broadcasted_iota(jnp.int32, h.shape, 0)
        h = jnp.sum(jnp.where(col == row, h, 0.0), axis=0, keepdims=True)
        b = jnp.zeros((1, d), F32)
        col = lax.broadcasted_iota(jnp.int32, (1, d), 1) // DH
        heads = qvb.shape[0]
        for j in range(heads):
            x = mm(qvb[j], spread)
            b = jnp.where(col == j, x[0:1], jnp.where(col == 2 * heads + j, x[1:2], b))
        mine[part:] = jnp.concatenate(wide + [h, b, jnp.zeros((8, d), F32)], axis=0).astype(BF)
        steps = both_ways(n, place, at, mine, wg, gsems)
        lead()
        meet(core, cross, (at((place + 1) % n), at((place + n - 1) % n)), diag)
    else:
        meet(core, cross, (), diag)
    R = range(rows // ROWS)
    cut = lambda i: pl.ds(i * ROWS, ROWS)
    xc = [send(tok.at[cut(i)], full.at[t, cut(i)], xs.at[i], xr.at[i], tensor=cross) for i in R]
    cc = [send(tok.at[cut(i)], full.at[t, cut(i)], cs.at[i], cr.at[i], tensor=core) for i in R]
    fc = [send(full.at[cross, cut(i)], full.at[cross, cut(i)], fs.at[i], fr.at[i], tensor=core) for i in R]
    own = [pltpu.make_async_copy(tok, full.at[t], lsem.at[0])]
    if ring:
        own.append(pltpu.make_async_copy(mine, wg.at[f], lsem.at[1]))
        for c in steps[0]:
            c.start()
    for c in xc + cc + own:
        c.start()

    groups = seg.shape[0]
    ids = seg[...].astype(F32)
    on = alive[...]
    keys = jnp.where(on == 1, ids, -1.0)
    onf = on.astype(F32)
    for g in range(groups):
        c = slice(g * 128, (g + 1) * 128)
        sq[:, c] = ids[g : g + 1]
        live[:, c] = onf[g : g + 1]
        sk[c, :] = jnp.broadcast_to(keys[g : g + 1], (128, 128)).T
        lives[c, :] = jnp.broadcast_to(onf[g : g + 1], (128, 128)).T
    per = BQ // 128
    for i in range(groups // per):
        under = jnp.sum((ids < ids[i * per : i * per + 1, 0:1]).astype(F32))
        upto = jnp.sum((ids <= ids[(i + 1) * per - 1 : (i + 1) * per, 127:128]).astype(F32))
        bounds[2 * i] = under.astype(jnp.int32) // BK
        bounds[2 * i + 1] = (upto.astype(jnp.int32) + BK - 1) // BK

    if ring:
        for s in range(1, len(steps)):
            ring_on(steps, s)
        follow()
    for i in R:
        xc[i].wait_recv()
        fc[i].start()
    for c in own:
        c.wait()
    for c in cc:
        c.wait_recv()
    if ring:
        ring_end(steps)
    ready()
    misc[...] = jnp.sum(wg[:, part:, :].astype(F32), axis=0)
    w = 3 * head

    def block(i):
        p = mm(full[i], whole(wg, part, 0, w)) + misc[7:8, :w]
        for j in range(3):
            qkv[j, pl.ds(i * rows, rows), :] = p[:, j * head : (j + 1) * head].astype(BF)

    def three(j, _):
        block(lax.select(j == 0, t, lax.select(j == 1, core, cross)))
        return 0

    lax.fori_loop(0, 3, three, 0)
    for c in fc:
        c.wait_recv()
    block(diag)
    for c in xc + cc + fc:
        c.wait_send()


def moments(h):
    mean = jnp.mean(h, axis=-1, keepdims=True)
    c = h - mean
    r = lax.rsqrt(jnp.mean(c * c, axis=-1, keepdims=True) + EPSILON)
    return c * r, r


def norm_back(dy, g, xhat, r):
    dx = dy * g
    return r * (
        dx
        - jnp.mean(dx, axis=-1, keepdims=True)
        - xhat * jnp.mean(dx * xhat, axis=-1, keepdims=True)
    )


def scatter_tools(core, cross, part, cs, cr, xs, xr, sems):
    ccs, ccr, xxs, xxr = sems
    a = lambda i, k: send(cs.at[k], cr.at[k], ccs.at[i, k], ccr.at[i, k], tensor=core)
    b = lambda i, k: send(xs.at[k], xr.at[k], xxs.at[i, k], xxr.at[i, k], tensor=cross)

    def put(i, k, tile, count):
        if i > 0:
            a(i - 1, k).wait_send()
        width = part.shape[-1] // count
        for j in range(count):
            p = tile(j)
            m = p.shape[0] // 4
            c = slice(j * width, (j + 1) * width)
            cs[k, 0, :, c] = p[m : 2 * m].astype(BF)
            cs[k, 1, :, c] = p[3 * m :].astype(BF)
            part[k, 0, :, c] = p[:m]
            part[k, 1, :, c] = p[2 * m : 3 * m]
        a(i, k).start()

    def across(i, k):
        a(i, k).wait_recv()
        if i > 0:
            b(i - 1, k).wait_send()
        xs[k] = (part[k, 1] + cr[k, 1].astype(F32)).astype(BF)
        b(i, k).start()
        part[k, 0] = part[k, 0] + cr[k, 0].astype(F32)

    def take(i, k):
        b(i, k).wait_recv()
        return part[k, 0] + xr[k].astype(F32)

    def end(i, k):
        a(i, k).wait_send()
        b(i, k).wait_send()

    return put, across, take, end


def block_rows(ref, device, c0, c1, n):
    size = ref.shape[0] // n
    return ref.at[pl.ds(pl.multiple_of(device * size, size), size), pl.ds(c0, c1 - c0)]


class RingSum:
    def __init__(self, n, place, at, local, c0, c1, buf, ss, rs, longer):
        nxt, prv = at((place + 1) % n), at((place + n - 1) % n)
        right = n // 2 if longer else n - 1 - n // 2
        self.buf, self.local = buf, lambda p: block_rows(local, at((p + n) % n), c0, c1, n)
        self.place = place
        self.chains = (
            (0, right, lambda s: place + right - s, nxt),
            (right, n - 1 - right, lambda s: place - (n - 1 - right) + s, prv),
        )
        self.ss, self.rs = ss, rs

    def copy(self, chain, s):
        base, _, owner, target = chain
        src = self.local(owner(0)) if s == 0 else self.buf.at[base + s - 1]
        j = base + s
        return send(src, self.buf.at[j], self.ss.at[j], self.rs.at[j], fsdp=target)

    def go(self, s):
        for chain in self.chains:
            base, hops, owner, _ = chain
            if s >= hops:
                continue
            if s > 0:
                self.copy(chain, s - 1).wait_recv()
                j = base + s - 1
                self.buf[j] = (self.buf[j].astype(F32) + self.local(owner(s))[...].astype(F32)).astype(BF)
            self.copy(chain, s).start()

    def close(self):
        total = self.local(self.place)[...].astype(F32)
        for chain in self.chains:
            self.copy(chain, chain[1] - 1).wait_recv()
            total = total + self.buf[chain[0] + chain[1] - 1].astype(F32)
        return total

    def sent(self):
        for chain in self.chains:
            for s in range(chain[1]):
                self.copy(chain, s).wait_send()


def ring_group(n, place, at, local, tracks):
    m = len(tracks)
    q = [RingSum(n, place, at, local, j * 128, j * 128 + 128, *tracks[j], j % 2) for j in range(m)]
    left = list(range(n // 2))

    def go():
        if left:
            s = left.pop(0)
            for r in q:
                r.go(s)

    def close():
        while left:
            go()
        x = jnp.concatenate([r.close() for r in q], axis=1)
        for r in q:
            r.sent()
        return x

    return go, close


def ring_scratch(n, rows, widths):
    out = []
    for w in widths:
        out += [pltpu.VMEM((n - 1, rows, w), BF)]
        out += [DMA((n - 1,)), DMA((n - 1,))]
    return out


def attend_block(i, lo, hi, heads, sq_ref, sk_ref, pad_ref, qt, kh, vt, sc, ctx_ref, octx_ref, lse_ref):
    q0 = pl.multiple_of(i * BQ, BQ)
    sq = sq_ref[0:1, pl.ds(q0, BQ)]
    qpos = q0 + lax.broadcasted_iota(jnp.int32, (BK, BQ), 1)
    part = sc.shape[1] // BK
    spot = lambda h, j: (sc.shape[0] // heads * h + j // part, pl.ds(pl.multiple_of(j % part * BK, BK), BK), slice(None))

    def first(j, c):
        k0 = pl.multiple_of(j * BK, BK)
        sk = jnp.concatenate([sk_ref[pl.ds(k0, BK), :]] * (BQ // 128), axis=1)
        kpos = k0 + lax.broadcasted_iota(jnp.int32, (BK, BQ), 0)
        ok = (sk == sq) | (kpos == qpos)
        out = []
        for h in range(heads):
            s = jnp.where(ok, mm(kh(h, j)[...], qt(h, i)[...]), -1e30)
            sc[spot(h, j)] = s
            out.append(jnp.maximum(c[h], fold_max(s)))
        return tuple(out)

    m = lax.fori_loop(lo, hi, first, (jnp.full((8, BQ), -3e38, F32),) * heads)
    m = [jnp.max(x, axis=0, keepdims=True) for x in m]

    def second(j, c):
        out = []
        for h in range(heads):
            l, acc = c[2 * h : 2 * h + 2]
            p = jnp.exp(sc[spot(h, j)] - m[h])
            out += [l + fold_sum(p), acc + mm(vt(h, j)[...], p.astype(BF))]
        return tuple(out)

    c = lax.fori_loop(lo, hi, second, (jnp.zeros((8, BQ), F32), jnp.zeros((DH, BQ), F32)) * heads)
    o = []
    for h in range(heads):
        l, acc = c[2 * h : 2 * h + 2]
        l = jnp.sum(l, axis=0, keepdims=True)
        lse_ref[h : h + 1, pl.ds(q0, BQ)] = m[h] + jnp.log(l)
        o.append(acc / l)
    ot = jnp.concatenate(o, axis=0) * pad_ref[0:1, pl.ds(q0, BQ)]
    octx_ref[:, pl.ds(q0, BQ)] = ot
    ctx_ref[pl.ds(q0, BQ), :] = ot.T.astype(BF)


def middle_kernel(n, ring, *refs):
    refs = list(refs)
    pop = lambda m: [refs.pop(0) for _ in range(m)]
    tok, cot_hbm = pop(2)
    raw = pop(9 if ring else 2)
    if ring:
        wh, wd = pop(2)
    else:
        wg, wf = pop(2)
    full, qkv, sq, sk, live_row, bounds = pop(6)
    if ring:
        (wg,) = pop(1)
    out, dfirst, dctx, octx, lse, gown, gsend, gup, odown, sums = pop(10)
    gdown = odown
    misc, pad = pop(2)
    mine = near = nsem = psems = None
    if ring:
        mine = pop(1)[0]
        near = pop(len(raw))
        nsem = pop(1)[0]
    tsems = pop(7)
    if ring:
        psems = pop(4)
    if ring:
        (wf, gdown) = pop(2)
    ctx, call, slab, wo, dsend = pop(5)
    (norm, dff, acted, dgelu, pre, dpre, first, xhat, r1, part, csem, lsem) = pop(12)
    cs, cr, xs, xr = pop(4)
    ocs, ocr = pop(2)
    rsem = pop(4)
    gsem = pop(6)
    osem = pop(2)
    ssem = pop(6)
    asem = pop(6)
    dsem = pop(6)
    ff = wf.shape[2] // 2
    if ring:
        wsem = pop(4)
        tracks = [pop(3) for _ in range(ff // 128)]
    t, f, core, cross, diag, place, at = places(n)
    rows, d = out.shape
    fetch = pltpu.make_async_copy(cot_hbm, out, csem.at[0])
    fetch.start()
    nch = rows // ROWS
    wpart = wg.shape[1] - MISC
    fpart = wf.shape[1]
    width = ctx.shape[1]
    heads = width // DH
    where = (t, core, cross, diag)
    put, across, take, end = scatter_tools(core, cross, part, cs, cr, xs, xr, rsem)
    gs = {}
    for i, buf in enumerate((norm, dff)):
        gs[i] = (
            lambda k, buf=buf, i=i: send(buf.at[k, 0], buf.at[k, 2], gsem[0].at[i, k], gsem[1].at[i, k], tensor=cross),
            lambda k, buf=buf, i=i: send(buf.at[k, 0], buf.at[k, 1], gsem[2].at[i, k], gsem[3].at[i, k], tensor=core),
            lambda k, buf=buf, i=i: send(buf.at[k, 2], buf.at[k, 3], gsem[4].at[i, k], gsem[5].at[i, k], tensor=core),
        )

    def share(i, k):
        gs[i][0](k).start()
        gs[i][1](k).start()

    def shared(i, k):
        gs[i][0](k).wait_recv()
        gs[i][2](k).start()
        gs[i][1](k).wait_recv()
        gs[i][2](k).wait_recv()

    lane0 = d - slab.shape[-1]
    slab0 = wg.at[:, pl.ds(0, wpart), pl.ds(lane0, slab.shape[-1])]
    slabs = (
        send(slab0, slab.at[1], ssem[0].at[0], ssem[1].at[0], tensor=cross),
        send(slab0, slab.at[0], ssem[2].at[0], ssem[3].at[0], tensor=core),
        send(slab.at[1], slab.at[2], ssem[4].at[0], ssem[5].at[0], tensor=core),
    )

    def rows_at(w, k):
        return pl.ds(pl.multiple_of(w * rows + k * ROWS, ROWS), ROWS)

    def give(j, k):
        return send(ctx.at[rows_at(where[j], k), :], call.at[k, j], asem[2 * j - 2].at[k], asem[2 * j - 1].at[k], tensor=where[j])

    def back(j, k):
        return send(dsend.at[k, j - 1], dctx.at[rows_at(t, k), :], dsem[2 * j - 2].at[k], dsem[2 * j - 1].at[k], tensor=where[j])

    load = []
    steps = []
    if ring:
        load = [
            pltpu.make_async_copy(wh, wf.at[f, :, pl.ds(0, ff)], lsem.at[0]),
            pltpu.make_async_copy(wd, wf.at[f, :, pl.ds(ff, ff)], lsem.at[1]),
        ]
        steps = both_ways(n, place, at, wf.at[f], wf, wsem)

    def lead():
        for c in load:
            c.start()

    def follow():
        for c in load:
            c.wait()
        for c in steps[0]:
            c.start()

    def ready():
        slabs[0].start()
        slabs[1].start()

    outs = (full, qkv, misc, sq, sk, live_row, pad, bounds)
    project_part(n, ring, tok, raw, outs, wg, mine, near, nsem, tsems, psems, lead, follow, ready)
    sums[...] = jnp.zeros_like(sums)

    blocks = 4 * rows // BQ
    across_lanes = d // BQ

    def turned(top):
        def tile(h, i):
            lanes = pl.ds(pl.multiple_of(i % across_lanes * BQ, BQ), BQ)
            return dff.at[h, i // across_lanes, pl.ds(top, DH), lanes]

        return tile

    qt, vt = turned(0), turned(DH)
    stack = 4 * ROWS // BK

    def kh(h, j):
        lanes = pl.ds(pl.multiple_of(j // stack * 128, 128), DH)
        return acted.at[h, pl.ds(pl.multiple_of(j % stack * BK, BK), BK), lanes]

    def prepare(i, _):
        r = pl.ds(pl.multiple_of(i * BQ, BQ), BQ)
        qs = (qkv[0, r, :].astype(F32) * 0.125).T.astype(BF)
        vs = qkv[2, r, :].astype(F32).T.astype(BF)
        ks = qkv[1, r, :]
        for h in range(heads):
            c = slice(h * DH, (h + 1) * DH)
            qt(h, i)[...] = qs[c]
            vt(h, i)[...] = vs[c]
            kh(h, i)[...] = ks[:, c]
        return 0

    lax.fori_loop(0, blocks, prepare, 0)
    reach = (MOST - 2 + BK) // BK

    def attend(base, stride, count):
        def body(i, _):
            b = base + i * stride
            lo = jnp.maximum(b - reach, 0)
            hi = jnp.minimum(b + reach + 1, blocks)
            attend_block(b, lo, hi, heads, sq, sk, live_row, qt, kh, vt, dgelu, ctx, octx, lse)
            return 0

        lax.fori_loop(0, count, body, 0)

    def give_when(sent):
        for w in range(4):
            ks = [k for k in range(nch) if k in sent[w]]
            for j in (3, 2, 1):

                @pl.when(where[j] == w)
                def _(j=j, ks=ks):
                    for k in ks:
                        give(j, k).start()

    def rows_of(k):
        return pl.ds(pl.multiple_of(k * ROWS, ROWS), ROWS)

    def pad_rows(k):
        return pad[rows_at(t, k), 0:1]

    def live(k, x):
        s = jnp.sum(x * x, axis=-1, keepdims=True) * pad_rows(k)
        return jnp.sum(s, axis=0, keepdims=True)

    lane = lax.broadcasted_iota(jnp.int32, (1, d), 1)

    def note(j, v):
        sums[7:8, :] += jnp.where(lane == d // 2 + j, v, 0.0)

    def norm_one(k):
        for j in (1, 2, 3):
            give(j, k).wait_recv()
        call[k, 0] = ctx[rows_at(t, k), :]
        x = full[t, rows_of(k), :].astype(F32)
        branch = misc[4:5, :]
        for j in range(4):
            branch = branch + mm(call[k, j], wo[j], 1, 1)
        xh, r = moments(x + branch)
        y = xh * misc[0:1, :] + misc[2:3, :]
        first[k] = y
        xhat[k] = xh
        r1[k] = r
        norm[k, 0] = y.astype(BF)
        share(0, k)
        note(0, live(k, x))
        note(1, live(k, branch))
        note(3, jnp.sum(pad_rows(k), axis=0, keepdims=True))

    def loop(fn):
        def body(k, _):
            fn(k)
            return 0

        lax.fori_loop(0, nch, body, 0)

    done, whole_rows = set(), [set() for _ in range(4)]

    def ran(ids):
        done.update(r for b in ids for r in range(b * BQ // ROWS, (b + 1) * BQ // ROWS))
        fresh = [
            {k for k in range(nch) if w * nch + k in done and k not in whole_rows[w]} for w in range(4)
        ]
        for w in range(4):
            whole_rows[w] |= fresh[w]
        give_when(fresh)

    attend(0, 1, 2)
    ran((0, 1))
    if ring:
        ring_on(steps, 1)
    attend(3, 1, 2)
    ran((3, 4))
    slabs[0].wait_recv()
    slabs[2].start()
    if ring:
        ring_on(steps, 2)
    attend(2, 1, 1)
    slabs[1].wait_recv()
    slabs[2].wait_recv()
    wo[0] = whole(wg, wpart, lane0, d)[:, -width:]
    for j in range(3):
        wo[j + 1] = slab[j].reshape(d, slab.shape[-1])[:, -width:]
    norm_one(0)
    attend(5, 1, 1)
    ran((2, 5))
    if ring:
        for s in range(3, len(steps)):
            ring_on(steps, s)
    for k in range(1, nch):
        norm_one(k)
    if ring:
        ring_end(steps)
    inv = 0.7071067811865476
    thirds = ff // BQ

    def feed(k):
        shared(0, k)
        def half(b):
            x = norm[k, 2 * b : 2 * b + 2].reshape(2 * ROWS, d)
            for c in range(0, ff, 256):
                pre[:, c : c + 256] = mm(x, whole(wf, fpart, c, c + 256)) + misc[6:7, c : c + 256]

        def act(i, b):
            u = pre[pl.ds(pl.multiple_of(i * 64, 64), 64), :]
            s = pl.ds(pl.multiple_of(b * 2 * ROWS + i * 64, 64), 64)
            cdf = 0.5 + 0.5 * lax.erf(u * inv)
            acted[k, s, :] = (u * cdf).astype(BF)
            slope = cdf + u * (jnp.exp(-0.5 * u * u) * 0.3989422804014327)
            for c in range(thirds):
                dgelu[k * thirds + c, s, :] = slope[:, c * BQ : (c + 1) * BQ]
            return b

        half(0)
        pl.when(k > 0)(lambda: across(0, k - 1))
        lax.fori_loop(0, 2 * ROWS // 64, act, 0)
        half(1)
        lax.fori_loop(0, 2 * ROWS // 64, act, 1)
        put(0, k, lambda j: mm(acted[k], some(wf, fpart, ff, 2 * ff, j, 2), 1, 1), 2)

    loop(feed)
    across(0, nch - 1)
    fetch.wait()

    def norm_two(k):
        branch = take(0, k) + misc[5:6, :]
        xh, r = moments(first[k] + branch)
        dy = out[rows_of(k), :].astype(F32)
        out[rows_of(k), :] = (xh * misc[1:2, :] + misc[3:4, :]).astype(BF)
        ds = norm_back(dy, misc[1:2, :], xh, r)
        first[k] = ds
        low = ds.astype(BF)
        dff[k, 0] = low
        share(1, k)
        note(2, live(k, branch))
        sums[1:2, :] += col_sum(dy * xh)
        sums[3:4, :] += col_sum(dy)
        sums[5:6, :] += col_sum(low.astype(F32))

    loop(norm_two)

    def feed_back(k):
        shared(1, k)
        def half(b):
            g = dff[k, 2 * b : 2 * b + 2].reshape(2 * ROWS, d)
            for c in range(0, ff, 256):
                pre[:, c : c + 256] = mm(g, whole(wf, fpart, ff + c, ff + c + 256))

        def act(i, b):
            r = pl.ds(pl.multiple_of(i * 64, 64), 64)
            s = pl.ds(pl.multiple_of(b * 2 * ROWS + i * 64, 64), 64)
            slope = jnp.concatenate([dgelu[k * thirds + c, s, :] for c in range(thirds)], axis=1)
            low = (pre[r, :] * slope).astype(BF)
            dpre[k, s, :] = low
            sums[6:7, :] += col_sum(low.astype(F32))
            return b

        half(0)
        pl.when(k > 0)(lambda: across(1, k - 1))
        lax.fori_loop(0, 2 * ROWS // 64, act, 0)
        half(1)
        lax.fori_loop(0, 2 * ROWS // 64, act, 1)
        put(1, k, lambda j: mm(dpre[k], some(wf, fpart, 0, ff, j, 2), 1, 1), 2)

    def weight_part(left, right, to):
        def cols(i, _):
            c = pl.ds(pl.multiple_of(i * 128, 128), 128)
            g = 0.0
            for k in range(nch):
                g = g + mm(left[k, :, :, c].reshape(4 * ROWS, 128), right[k], 0, 0)
            to[c, :] = g.astype(BF)
            return 0

        lax.fori_loop(0, d // 128, cols, 0)

    def norm_one_back(k):
        dy = first[k] + take(1, k)
        xh = xhat[k]
        ds = norm_back(dy, misc[0:1, :], xh, r1[k])
        dfirst[rows_of(k), :] = ds
        low = ds.astype(BF)
        for c in gs[1][:2]:
            c(k).wait_send()
        dff[k, 0] = low
        for j in (3, 2, 1):
            dsend[k, j - 1] = mm(low, wo[j]).astype(BF)
            back(j, k).start()
        dctx[rows_at(t, k), :] = mm(low, wo[0]).astype(BF)
        sums[0:1, :] += col_sum(dy * xh)
        sums[2:3, :] += col_sum(dy)
        sums[4:5, :] += col_sum(low.astype(F32))

    oc = send(ocs, ocr, osem[0].at[0], osem[1].at[0], tensor=core)

    def out_part():
        x = dff[:, 0].reshape(rows, d)
        for slot, j in ((0, 1), (1, 3)):
            ocs[slot] = mm(x, call[:, j].reshape(rows, width), 0, 0).astype(BF)
        oc.start()

    def out_take():
        x = dff[:, 0].reshape(rows, d)
        for slot, j, to in ((1, 2, gsend), (0, 0, gown)):
            p = mm(x, call[:, j].reshape(rows, width), 0, 0)
            if slot:
                oc.wait_recv()
            to[...] = (p + ocr[slot].astype(F32)).astype(BF)

    loop(feed_back)
    if ring:
        weight_part(dff, acted, gdown)
        across(1, nch - 1)
        go, close = ring_group(n, place, at, gdown, tracks)
        go()
        norm_one_back(0)
        weight_part(norm, dpre, gup)
        go()
        for k in range(1, nch):
            norm_one_back(k)
            go()
        out_part()
        go()
        out_take()
        odown[...] = close()
    else:
        across(1, nch - 1)
        weight_part(dff, acted, gdown)
        weight_part(norm, dpre, gup)
        loop(norm_one_back)
        out_part()
        out_take()

    def finish(k, _):
        end(1, k)
        for j in (1, 2, 3):
            back(j, k).wait_recv()
            back(j, k).wait_send()
            give(j, k).wait_send()
        for c in gs[0] + gs[1][2:]:
            c(k).wait_send()
        return 0

    lax.fori_loop(0, nch, finish, 0)
    for c in slabs + (oc,):
        c.wait_send()


def middle(n, tok, cot, head, seg, alive, raw, wh, wd, wg, wf):
    ring = wf is None
    vm = pl.BlockSpec(memory_space=pltpu.VMEM)
    far = pl.BlockSpec(memory_space=pltpu.HBM)
    pin = lambda x: pltpu.with_memory_space_constraint(x, pltpu.HBM)
    rows, d = cot.shape
    width = head
    heads = width // DH
    total = 4 * rows
    nch = rows // ROWS
    s = jax.ShapeDtypeStruct
    V = pltpu.VMEM
    ff = wh.shape[1] if ring else wf.shape[2] // 2
    tables = (seg.reshape(-1, 128), alive.reshape(-1, 128))
    if ring:
        ops = tuple(pin(x) for x in (tok, cot) + tables + raw + (wh, wd))
        specs = [far] * len(ops)
    else:
        ops = (tok, pin(cot)) + tables + (wg, wf)
        specs = [vm, far] + [vm] * 4
    outs = [
        s((4, rows, d), BF),
        s((3, total, width), BF),
        s((1, total), F32),
        s((total, 128), F32),
        s((1, total), F32),
        s((2 * total // BQ,), jnp.int32),
    ]
    ospecs = [vm] * 5 + [pl.BlockSpec(memory_space=pltpu.SMEM)]
    if ring:
        outs.append(s((n, d // n + MISC, d), BF))
    outs += [
        s((rows, d), BF),
        s((rows, d), F32),
        s((total, width), BF),
        s((width, total), F32),
        s((heads, total), F32),
        s((d, width), BF),
        s((d, width), BF),
        s((d, ff), BF),
        s((d // n, ff), F32) if ring else s((d, ff), BF),
        s((8, d), F32),
    ]
    ospecs += [vm] * (len(outs) - len(ospecs))
    g, gr = (n, d // n) if ring else (wg.shape[0], wg.shape[1] - MISC)
    wide = -(-width // 128) * 128
    scratch = [V((MISC, d), F32), V((total, 128), F32)]
    if ring:
        held = tables + raw
        scratch += [V((d // n + MISC, d), BF)] + [V(x.shape, x.dtype) for x in held] + [DMA((len(held),))]
    scratch += [DMA((2,))] + [DMA((nch,))] * 6
    if ring:
        scratch += [DMA((n // 2, 2))] * 4
        scratch += [V((n, d // n, 2 * ff), BF), V((d, ff), BF)]
    scratch += [V((total, width), BF), V((nch, 4, ROWS, width), BF), V((3, g, gr, wide), BF), V((4, d, width), BF)]
    scratch += [V((nch, 3, ROWS, width), BF)]
    scratch += [V((nch, 4, ROWS, d), BF)] * 2
    scratch += [V((nch, 4 * ROWS, ff), BF), V((nch * (ff // BQ), 4 * ROWS, BQ), F32), V((2 * ROWS, ff), F32), V((nch, 4 * ROWS, ff), BF)]
    scratch += [V((nch, ROWS, d), F32)] * 2 + [V((nch, ROWS, 1), F32)]
    scratch += [V((nch, 2, ROWS, d), F32), DMA((1,)), DMA((2,))]
    scratch += [V((nch, 2, ROWS, d), BF)] * 2 + [V((nch, ROWS, d), BF)] * 2
    scratch += [V((2, d, width), BF)] * 2
    scratch += [DMA((2, nch))] * 10 + [DMA((1,))] * 8 + [DMA((nch,))] * 12
    if ring:
        scratch += [DMA((n // 2, 2))] * 4 + ring_scratch(n, d // n, (128,) * (ff // 128))
    return pl.pallas_call(
        functools.partial(middle_kernel, n, ring),
        in_specs=specs,
        out_specs=ospecs,
        out_shape=outs,
        scratch_shapes=scratch,
        compiler_params=pltpu.CompilerParams(
            collective_id=2, has_side_effects=True, vmem_limit_bytes=38 << 20
        ),
        name="middle",
    )(*ops)


def last_kernel(n, ring, *refs):
    refs = list(refs)
    pop = lambda m: [refs.pop(0) for _ in range(m)]
    dqkv, wg, full, gown, gfar, dfirst, sums = pop(7)
    if ring:
        (gup,) = pop(1)
        dtok, oattn, oout, oup, ogain, oshift, obias, ohb, oqvb, oroot = pop(10)
    else:
        dtok, gb, total = pop(3)
    part, cs, cr, xs, xr = pop(5)
    rsem = pop(4)
    msend, mrecv = pop(2)
    msem = pop(4)
    if ring:
        gb, mall = pop(2)
        mring = pop(4)
        tracks = [refs[i : i + 3] for i in range(0, len(refs), 3)]
    t, f, core, cross, diag, place, at = places(n)
    rows, d = dtok.shape
    nch = rows // ROWS
    wpart = wg.shape[1] - MISC
    w3 = dqkv.shape[1]
    width = w3 // 3
    where = (t, core, cross, diag)
    put, across, take, end = scatter_tools(core, cross, part, cs, cr, xs, xr, rsem)
    nxt, prv = at((place + 1) % n), at((place + n - 1) % n)

    def rows_of(k):
        return pl.ds(pl.multiple_of(k * ROWS, ROWS), ROWS)

    b = col_sum(dqkv[...].astype(F32))
    b = jnp.concatenate([b[:, :width], b[:, 2 * width :], jnp.zeros((1, d - 2 * width), F32)], axis=1)
    msend[0] = sums[...]
    msend[0, 7:8, :] = sums[7:8, :] + b
    meet(core, cross, (nxt, prv) if ring else ())
    m0 = send(msend.at[0], mrecv.at[0], msem[0].at[0], msem[1].at[0], tensor=core)
    m1 = send(msend.at[1], mrecv.at[1], msem[2].at[0], msem[3].at[0], tensor=cross)
    if ring:
        ups = gup.shape[1] // 128
        up, up_close = ring_group(n, place, at, gup, tracks[:ups])
        up()
    m0.start()

    def weight_part(i, _):
        c = pl.ds(pl.multiple_of(i * 128, 128), 128)
        g = 0.0
        for j in range(4):
            g = g + mm(full[j, :, c], dqkv[j * rows : (j + 1) * rows, :], 0, 0)
        o = gown[c, :].astype(F32) + gfar[c, :].astype(F32)
        gb[c, :] = jnp.concatenate([g, o], axis=1).astype(BF)
        return 0

    lax.fori_loop(0, d // 128, weight_part, 0)
    if ring:
        up()
        own, own_close = ring_group(n, place, at, gb, tracks[ups:])
        own()

        def go():
            up()
            own()

    def tokens_part(k):
        x = jnp.concatenate([dqkv[pl.ds(w * rows + k * ROWS, ROWS), :] for w in where], axis=0)
        put(0, k, lambda j: mm(x, some(wg, wpart, 0, w3, j, 2), 1, 1), 2)

    for k in range(nch):
        tokens_part(k)
        if k > 0:
            across(0, k - 1)
        if ring and k > 0:
            go()
    across(0, nch - 1)
    m0.wait_recv()
    msend[1] = msend[0] + mrecv[0]
    m1.start()
    if ring:
        go()
    m1.wait_recv()
    row = lax.broadcasted_iota(jnp.int32, (8, d), 0)
    col = lax.broadcasted_iota(jnp.int32, (8, d), 1)
    over_tensor = (row < 6) | ((row == 7) & (col >= 2 * width))
    small = jnp.where(over_tensor, msend[1] + mrecv[1], msend[0])

    def keep(k):
        dtok[rows_of(k), :] = dfirst[rows_of(k), :] + take(0, k)

    if ring:
        msend[2] = small
        mall[place] = small
        msteps = []
        far = n // 2
        for s in range(far):
            a, b = (place - s + n) % n, (place + s) % n
            src = msend.at[2] if s == 0 else mall.at[a]
            pair = [send(src, mall.at[a], mring[0].at[s], mring[1].at[s], fsdp=nxt)]
            if s < far - 1:
                src = msend.at[2] if s == 0 else mall.at[b]
                pair.append(send(src, mall.at[b], mring[2].at[s], mring[3].at[s], fsdp=prv))
            msteps.append(pair)
        todo = [functools.partial(keep, k) for k in range(nch)]
        r = 0
        for _ in range(max(nch, far, n)):
            if r < far:
                for i, c in enumerate(msteps[r]):
                    if r > 0:
                        msteps[r - 1][i].wait_recv()
                    c.start()
                r += 1
            go()
            if todo:
                todo.pop(0)()
        msteps[far - 2][1].wait_recv()
        msteps[far - 1][0].wait_recv()
        total = jnp.sum(mall[...], axis=0)
        gp = d // n
        mine = pltpu.roll(total, (d - f * gp) % d, 1)
        ogain[...] = mine[0:2, :gp]
        oshift[...] = mine[2:4, :gp]
        obias[...] = mine[4:6, :gp]
        k = DH // n
        mine = pltpu.roll(total, (d - f * k) % d, 1)
        ohb[...] = jnp.concatenate([mine[6:7, h * DH : (h + 1) * DH] for h in range(ohb.shape[1])], axis=0).T[:k]
        heads = oqvb.shape[0]
        for h in range(heads):
            for j in range(2):
                c = (j * heads + h) * DH
                oqvb[h, j : j + 1, :] = mine[7:8, c : c + DH][:, :k]
        spot = lax.broadcasted_iota(jnp.int32, (1, d), 1) - d // 2
        pick = lambda j: jnp.sum(jnp.where(spot == j, total[7:8], 0.0), axis=1, keepdims=True)
        count = pick(3)
        col = lax.broadcasted_iota(jnp.int32, (1, 128), 1)
        o = jnp.zeros((1, 128), F32)
        for j in range(3):
            o = jnp.where(col == j, jnp.sqrt(pick(j) / (count * d)), o)
        oroot[...] = o
        oup[...] = up_close()
        x = own_close()
        for j in range(3):
            oattn[j] = x[:, j * width : (j + 1) * width]
        oout[...] = x[:, 3 * width :].T
        for pair in msteps:
            for c in pair:
                c.wait_send()
    else:
        total[...] = small
        for k in range(nch):
            keep(k)

    def finish(k, _):
        end(0, k)
        return 0

    lax.fori_loop(0, nch, finish, 0)
    m0.wait_send()
    m1.wait_send()


def last(n, ring, dqkv, wg, full, gown, gfar, dfirst, sums, gup):
    vm = pl.BlockSpec(memory_space=pltpu.VMEM)
    rows, d = dfirst.shape
    width = dqkv.shape[1] // 3
    heads = width // DH
    nch = rows // ROWS
    s = jax.ShapeDtypeStruct
    V = pltpu.VMEM
    ops = (dqkv, wg, full, gown, gfar, dfirst, sums)
    outs = [s((rows, d), F32)]
    gp = d // n
    k = DH // n
    if ring:
        ops += (gup,)
        outs += [s((3, gp, width), F32), s((width, gp), F32), s((gp, gup.shape[1]), F32)] + [s((2, gp), F32)] * 3
        outs += [s((k, d // DH), F32), s((heads, 2, k), F32), s((1, 128), F32)]
    else:
        outs += [s((d, d), BF), s((8, d), F32)]
    scratch = [V((nch, 2, ROWS, d), F32)]
    scratch += [V((nch, 2, ROWS, d), BF)] * 2 + [V((nch, ROWS, d), BF)] * 2
    scratch += [DMA((1, nch))] * 4
    scratch += [V((3, 8, d), F32), V((2, 8, d), F32)] + [DMA((1,))] * 4
    if ring:
        scratch += [V((d, d), BF), V((n, 8, d), F32)] + [DMA((n // 2,))] * 4
        scratch += ring_scratch(n, gp, (128,) * ((gup.shape[1] + d) // 128))
    return pl.pallas_call(
        functools.partial(last_kernel, n, ring),
        in_specs=[vm] * len(ops),
        out_specs=[vm] * len(outs),
        out_shape=outs,
        scratch_shapes=scratch,
        compiler_params=pltpu.CompilerParams(
            collective_id=3, has_side_effects=True, vmem_limit_bytes=12 << 20
        ),
        name="last",
    )(*ops)


def deliver_kernel(*refs):
    m = (len(refs) - 3) // 2
    src, roots, dst, three, sem = refs[:m], refs[m], refs[m + 1 : -2], refs[-2], refs[-1]
    for j in range(m):
        pltpu.make_async_copy(src[j], dst[j], sem.at[j]).start()
    for j in range(three.shape[0]):
        three[j] = jnp.sum(roots[0:1, j : j + 1])
    for j in range(m):
        pltpu.make_async_copy(src[j], dst[j], sem.at[j]).wait()


def deliver(arrays, roots):
    vm = pl.BlockSpec(memory_space=pltpu.VMEM)
    return pl.pallas_call(
        deliver_kernel,
        in_specs=[vm] * (len(arrays) + 1),
        out_specs=[pl.BlockSpec(memory_space=pl.ANY)] * len(arrays) + [pl.BlockSpec(memory_space=pltpu.SMEM)],
        out_shape=[jax.ShapeDtypeStruct(x.shape, x.dtype) for x in arrays] + [jax.ShapeDtypeStruct((3,), F32)],
        scratch_shapes=[DMA((len(arrays),))],
        compiler_params=pltpu.CompilerParams(vmem_limit_bytes=1 << 20),
        name="deliver",
    )(*arrays, roots)


def bwd_kernel(heads, bounds, qkv_ref,dc_ref,oct_ref,lse_ref,sq_ref,sk_ref,pad_ref, dqkv_ref, qt, dt, kt, kh, vh, qh, dh, dqt, dsum, dka, dva):
    S=qkv_ref.shape[1]; W=heads*DH
    qs=(qkv_ref[0].astype(F32)*0.125)
    qsb=qs.astype(BF); qt[...]=qs.T.astype(BF)
    kk=qkv_ref[1]; vv=qkv_ref[2]
    kt[...]=kk.astype(F32).T.astype(BF)
    dct=dc_ref[...].astype(F32).T*pad_ref[0:1,:]
    dt[...]=dct.astype(BF)
    dcn=dct.T.astype(BF)
    prod=dct*oct_ref[...]
    for h in range(heads):
        c=slice(h*DH,(h+1)*DH)
        kh[h]=kk[:,c]; vh[h]=vv[:,c]; qh[h]=qsb[:,c]; dh[h]=dcn[:,c]
        dsum[h:h+1,:]=jnp.sum(prod[h*DH:(h+1)*DH],axis=0,keepdims=True)
    dqt[...]=jnp.zeros_like(dqt)
    def kblock(j,_):
        k0=pl.multiple_of(j*BK,BK)
        lo=bounds[2*j]; hi=bounds[2*j+1]
        sk=jnp.concatenate([sk_ref[pl.ds(k0,BK),:]]*(BQ//128),axis=1)
        kpos=k0+lax.broadcasted_iota(jnp.int32,(BK,BQ),0)
        dka[...]=jnp.zeros_like(dka); dva[...]=jnp.zeros_like(dva)
        def body(i,_):
            q0=pl.multiple_of(i*BQ,BQ)
            sq=sq_ref[0:1,pl.ds(q0,BQ)]
            qpos=q0+lax.broadcasted_iota(jnp.int32,(BK,BQ),1)
            ok=(sk==sq)|(kpos==qpos)
            for h in range(heads):
                r=slice(h*DH,(h+1)*DH)
                s=jnp.where(ok,mm(kh[h,pl.ds(k0,BK),:],qt[r,pl.ds(q0,BQ)]),-1e30)
                p=jnp.exp(s-lse_ref[h:h+1,pl.ds(q0,BQ)])
                dp=mm(vh[h,pl.ds(k0,BK),:],dt[r,pl.ds(q0,BQ)])
                ds=(p*(dp-dsum[h:h+1,pl.ds(q0,BQ)])).astype(BF)
                dva[h]+=mm(p.astype(BF),dh[h,pl.ds(q0,BQ),:])
                dka[h]+=mm(ds,qh[h,pl.ds(q0,BQ),:])
                dqt[r,pl.ds(q0,BQ)]+=mm(kt[r,pl.ds(k0,BK)],ds)
            return 0
        lax.fori_loop(lo,hi,body,0)
        dqkv_ref[pl.ds(k0,BK),W:]=jnp.concatenate([dka[h] for h in range(heads)]+[dva[h] for h in range(heads)],axis=1).astype(BF)
        return 0
    lax.fori_loop(0,S//BK,kblock,0)
    dqkv_ref[:,:W]=(dqt[...]*0.125).T.astype(BF)

def attn_bwd(bounds,qkv,dc,oct,lse,sq,sk,pad):
    _,S,W=qkv.shape; heads=W//DH
    vm=pl.BlockSpec(memory_space=pltpu.VMEM)
    return pl.pallas_call(functools.partial(bwd_kernel,heads),
        in_specs=[pl.BlockSpec(memory_space=pltpu.SMEM)]+[vm]*7,
        out_specs=vm,
        out_shape=jax.ShapeDtypeStruct((S,3*W),BF),
        scratch_shapes=[pltpu.VMEM((W,S),BF)]*3+[pltpu.VMEM((heads,S,DH),BF)]*4+[pltpu.VMEM((W,S),F32),pltpu.VMEM((heads,S),F32)]+[pltpu.VMEM((heads,BK,DH),F32)]*2,
        compiler_params=pltpu.CompilerParams(vmem_limit_bytes=13<<20),
        name="attend_backward")(bounds,qkv,dc,oct,lse,sq,sk,pad)


def split_up(value, dim, devices):
    before, after = (value.shape[:dim], value.shape[dim + 1 :])
    return jnp.moveaxis(value.reshape(*before, devices, -1, *after), dim, 0)


def summed_on_arrival(value, axis, dim):
    blocks = split_up(value, dim, lax.axis_size(axis))
    arrived = lax.all_to_all(blocks, axis, split_axis=0, concat_axis=0, tiled=True)
    return arrived.astype(F32).sum(axis=0)


def shards(
    tokens,
    attn_weight,
    query_value_bias,
    out_weight,
    hidden_weight,
    hidden_bias,
    down_weight,
    norm_gains,
    norm_biases,
    output_biases,
    segment_ids,
    padding,
    cotangent,
):
    n = lax.axis_size("fsdp")
    f = lax.axis_index("fsdp")
    t = lax.axis_index("tensor")
    rows, d = tokens.shape
    gp = d // n
    width = attn_weight.shape[2]
    heads = width // DH
    ff = hidden_weight.shape[1]
    ring = gp % 16 == 0 and n % 2 == 0 and n >= 4
    if ring:
        raw = (
            attn_weight,
            out_weight,
            norm_gains,
            norm_biases,
            output_biases,
            hidden_bias.T,
            query_value_bias.transpose(1, 0, 2),
        )
        wh, wd, wg, wf = hidden_weight, down_weight.T, None, None
    else:
        gather = lambda x, dim: lax.all_gather(x, "fsdp", axis=dim, tiled=True)
        w = gather(attn_weight, 1).transpose(1, 0, 2).reshape(d, 3 * width)
        wo = gather(out_weight, 1).T
        b = gather(query_value_bias, 2).reshape(2, width)
        b = jnp.concatenate([b[0], jnp.zeros((width,), BF), b[1], jnp.zeros((width,), BF)])
        misc = jnp.concatenate(
            [
                gather(norm_gains, 1),
                gather(norm_biases, 1),
                gather(output_biases, 1),
                gather(hidden_bias, 1).reshape(1, ff),
                b[None],
                jnp.zeros((MISC - 8, d), BF),
            ]
        )
        wg = jnp.concatenate([jnp.concatenate([w, wo], axis=1), misc])[None]
        wf = jnp.concatenate([gather(hidden_weight, 0), gather(down_weight, 1).T], axis=1)[None]
        wh = wd = raw = None
    got = list(
        middle(n, tokens, cotangent, width, segment_ids, padding, raw, wh, wd, wg, wf)
    )
    full, qkv, seg_row, seg_keys, pad_row, bounds = got[:6]
    if ring:
        wg = got.pop(6)
    layer_out, d_first, d_ctx, ctx_t, lse, g_own, g_send, g_hidden, g_down, sums = got[6:]
    g_far = lax.ppermute(g_send, "tensor", [(i, (i + 2) % 4) for i in range(4)])
    d_qkv = attn_bwd(bounds, qkv, d_ctx, ctx_t, lse, seg_row, seg_keys, pad_row)
    done = last(n, ring, d_qkv, wg, full, g_own, g_far, d_first, sums, g_hidden)
    if ring:
        done = deliver((layer_out, g_down) + tuple(done[:-1]), done[-1])
        layer_out, g_down, d_tokens, g_attn, g_proj, g_hidden, g_gain, g_shift, g_bias, g_hb, g_qvb, roots = done
        g_down = g_down.T
        g_hb = g_hb.T
        g_qvb = g_qvb.transpose(1, 0, 2)
    else:
        d_tokens, g, total = done
        total = lax.psum(total, "fsdp")
        g_attn = g[:, : 3 * width].reshape(d, 3, width).transpose(1, 0, 2)
        g_attn = summed_on_arrival(g_attn, "fsdp", 1)
        g_proj = summed_on_arrival(g[:, 3 * width :].T, "fsdp", 1)
        g_hidden = summed_on_arrival(g_hidden, "fsdp", 0)
        g_down = summed_on_arrival(g_down.T, "fsdp", 1)
        vectors = lax.dynamic_slice(total, (0, f * gp), (6, gp))
        g_gain, g_shift, g_bias = vectors[0:2], vectors[2:4], vectors[4:6]
        k = DH // n
        g_hb = lax.dynamic_slice(total[6].reshape(ff // DH, DH), (0, f * k), (ff // DH, k))
        g_qvb = lax.dynamic_slice(
            total[7, : 2 * width].reshape(2 * heads, DH), (0, f * k), (2 * heads, k)
        ).reshape(2, heads, k)
        squares = total[7, d // 2 : d // 2 + 4]
        roots = jnp.sqrt(squares[:3] / (squares[3] * d))
    return (
        layer_out,
        d_tokens,
        g_attn,
        g_qvb,
        g_proj,
        g_hidden,
        g_hb,
        g_down,
        g_gain,
        g_shift,
        g_bias,
        roots,
    )


def solution(mesh):
    placed = (
        P(("fsdp", "tensor"), None),
        P(None, "fsdp", "tensor"),
        P(None, "tensor", "fsdp"),
        P("tensor", "fsdp"),
        P("fsdp", "tensor"),
        P("tensor", "fsdp"),
        P("tensor", "fsdp"),
        P(None, "fsdp"),
        P(None, "fsdp"),
        P(None, "fsdp"),
        P("fsdp"),
        P("fsdp"),
        P(("fsdp", "tensor"), None),
    )
    return jax.shard_map(
        shards,
        mesh=mesh,
        in_specs=placed,
        out_specs=(
            P(("fsdp", "tensor"), None),
            P(("fsdp", "tensor"), None),
            P(None, "fsdp", "tensor"),
            P(None, "tensor", "fsdp"),
            P("tensor", "fsdp"),
            P("fsdp", "tensor"),
            P("tensor", "fsdp"),
            P("tensor", "fsdp"),
            P(None, "fsdp"),
            P(None, "fsdp"),
            P(None, "fsdp"),
            P(),
        ),
        check_vma=False,
    )
```

```python
import functools

import jax
import jax.numpy as jnp
from jax import lax
from jax.experimental import pallas as pl
from jax.experimental.pallas import tpu as pltpu
from jax.sharding import PartitionSpec as P

DH = 64
EPSILON = 1e-12
BQ = 256
BK = 256
F32 = jnp.float32
BF = jnp.bfloat16
MESH = pl.DeviceIdType.MESH
DMA = pltpu.SemaphoreType.DMA
ROWS = 128
MISC = 16
MOST = 768


def places(n):
    t = lax.axis_index("tensor")
    f = lax.axis_index("fsdp")
    c, x = t % 2, t // 2
    core, cross, diag = 2 * x + 1 - c, 2 * (1 - x) + c, 2 * (1 - x) + 1 - c
    y, z = f % 2, f // 2
    place = z + y * (n - 1 - 2 * z)

    def at(p):
        y = p // max(n // 2, 1)
        return 2 * (p + y * (n - 1 - 2 * p)) + y

    return t, f, core, cross, diag, place, at


def send(src, dst, ss, rs, **axes):
    return pltpu.make_async_remote_copy(
        src_ref=src, dst_ref=dst, send_sem=ss, recv_sem=rs, device_id=axes, device_id_type=MESH
    )


def meet(core, cross, ring, *more):
    gate = pltpu.get_barrier_semaphore()
    for where in (core, cross) + more:
        pl.semaphore_signal(gate, inc=1, device_id={"tensor": where}, device_id_type=MESH)
    for where in ring:
        pl.semaphore_signal(gate, inc=1, device_id={"fsdp": where}, device_id_type=MESH)
    pl.semaphore_wait(gate, 2 + len(ring) + len(more))


def both_ways(n, place, at, local, held, sems):
    rs, rr, ls, lr = sems
    nxt, prv = at((place + 1) % n), at((place + n - 1) % n)
    far = n // 2
    half = local.shape[0] // 2
    steps = []
    for s in range(far):
        a, b = at((place - s + n) % n), at((place + s) % n)
        up = local if s == 0 else held.at[a]
        down = local if s == 0 else held.at[b]
        row = []
        for k in (0, 1):
            part = pl.ds(k * half, half)
            if s < far - 1 or k == 0:
                row.append(send(up.at[part], held.at[a, part], rs.at[s, k], rr.at[s, k], fsdp=nxt))
            if s < far - 1 or k == 1:
                row.append(send(down.at[part], held.at[b, part], ls.at[s, k], lr.at[s, k], fsdp=prv))
        steps.append(row)
    return steps


def ring_on(steps, s):
    for i, c in enumerate(steps[s]):
        if s < len(steps) - 1:
            steps[s - 1][i].wait_recv()
            c.start()
    if s == len(steps) - 1:
        steps[s - 1][0].wait_recv()
        steps[s][0].start()
        steps[s - 1][1].wait_recv()
        steps[s - 1][2].wait_recv()
        steps[s - 1][3].wait_recv()
        steps[s][1].start()


def ring_end(steps):
    for c in steps[-1]:
        c.wait_recv()
    for row in steps:
        for c in row:
            c.wait_send()


def mm(a, b, ca=1, cb=0):
    return lax.dot_general(a, b, (((ca,), (cb,)), ((), ())), preferred_element_type=F32)


def some(ref, rows, c0, c1, j, count):
    g = ref.shape[0]
    if g % count:
        size = rows // count
        return ref[0, j * size : (j + 1) * size, c0:c1]
    g //= count
    return ref[j * g : (j + 1) * g, :rows, c0:c1].reshape(g * rows, c1 - c0)


def whole(ref, rows, c0, c1):
    g = ref.shape[0]
    return ref[:, :rows, c0:c1].reshape(g * rows, c1 - c0)


def fold_max(s):
    return jnp.max(s.reshape(s.shape[0] // 8, 8, s.shape[1]), axis=0)


def fold_sum(s):
    return jnp.sum(s.reshape(s.shape[0] // 8, 8, s.shape[1]), axis=0)


def col_sum(s):
    return jnp.sum(fold_sum(s), axis=0, keepdims=True)


def project_part(n, ring, tok, far, outs, wg, mine, near, nsem, sems, gsems, lead, follow, ready):
    full, qkv, misc, sq, sk, live, lives, bounds = outs
    if ring:
        for j in range(len(far)):
            pltpu.make_async_copy(far[j], near[j], nsem.at[j]).start()
    else:
        seg, alive = far
    lsem, xs, xr, cs, cr, fs, fr = sems
    t, f, core, cross, diag, place, at = places(n)
    rows, d = tok.shape
    part = wg.shape[1] - MISC
    head = qkv.shape[2]
    if ring:
        for j in range(len(far)):
            pltpu.make_async_copy(far[j], near[j], nsem.at[j]).wait()
        seg, alive, aw, ow, gains, shifts, biases, hb, qvb = near
        mine[:part] = jnp.concatenate([aw[0], aw[1], aw[2], ow[...].astype(F32).T.astype(BF)], axis=1)
        col = lax.broadcasted_iota(jnp.int32, (part, d), 1)
        row = lax.broadcasted_iota(jnp.int32, (part, d), 0)
        spread = (col == f * part + row).astype(BF)
        wide = [mm(r[...], spread) for r in (gains, shifts, biases)]
        k = hb.shape[0]
        col = lax.broadcasted_iota(jnp.int32, (k, d), 1)
        row = lax.broadcasted_iota(jnp.int32, (k, d), 0)
        spread = (col % DH == f * k + row).astype(BF)
        h = mm(hb[...].astype(F32).T.astype(BF), spread)
        col = lax.broadcasted_iota(jnp.int32, h.shape, 1) // DH
        row = lax.broadcasted_iota(jnp.int32, h.shape, 0)
        h = jnp.sum(jnp.where(col == row, h, 0.0), axis=0, keepdims=True)
        b = jnp.zeros((1, d), F32)
        col = lax.broadcasted_iota(jnp.int32, (1, d), 1) // DH
        heads = qvb.shape[0]
        for j in range(heads):
            x = mm(qvb[j], spread)
            b = jnp.where(col == j, x[0:1], jnp.where(col == 2 * heads + j, x[1:2], b))
        mine[part:] = jnp.concatenate(wide + [h, b, jnp.zeros((8, d), F32)], axis=0).astype(BF)
        steps = both_ways(n, place, at, mine, wg, gsems)
        lead()
        meet(core, cross, (at((place + 1) % n), at((place + n - 1) % n)), diag)
    else:
        meet(core, cross, (), diag)
    R = range(rows // ROWS)
    cut = lambda i: pl.ds(i * ROWS, ROWS)
    xc = [send(tok.at[cut(i)], full.at[t, cut(i)], xs.at[i], xr.at[i], tensor=cross) for i in R]
    cc = [send(tok.at[cut(i)], full.at[t, cut(i)], cs.at[i], cr.at[i], tensor=core) for i in R]
    fc = [send(full.at[cross, cut(i)], full.at[cross, cut(i)], fs.at[i], fr.at[i], tensor=core) for i in R]
    own = [pltpu.make_async_copy(tok, full.at[t], lsem.at[0])]
    if ring:
        own.append(pltpu.make_async_copy(mine, wg.at[f], lsem.at[1]))
        for c in steps[0]:
            c.start()
    for c in xc + cc + own:
        c.start()

    groups = seg.shape[0]
    ids = seg[...].astype(F32)
    on = alive[...]
    keys = jnp.where(on == 1, ids, -1.0)
    onf = on.astype(F32)
    for g in range(groups):
        c = slice(g * 128, (g + 1) * 128)
        sq[:, c] = ids[g : g + 1]
        live[:, c] = onf[g : g + 1]
        sk[c, :] = jnp.broadcast_to(keys[g : g + 1], (128, 128)).T
        lives[c, :] = jnp.broadcast_to(onf[g : g + 1], (128, 128)).T
    per = BQ // 128
    for i in range(groups // per):
        under = jnp.sum((ids < ids[i * per : i * per + 1, 0:1]).astype(F32))
        upto = jnp.sum((ids <= ids[(i + 1) * per - 1 : (i + 1) * per, 127:128]).astype(F32))
        bounds[2 * i] = under.astype(jnp.int32) // BK
        bounds[2 * i + 1] = (upto.astype(jnp.int32) + BK - 1) // BK

    if ring:
        for s in range(1, len(steps)):
            ring_on(steps, s)
        follow()
    for i in R:
        xc[i].wait_recv()
        fc[i].start()
    for c in own:
        c.wait()
    for c in cc:
        c.wait_recv()
    if ring:
        ring_end(steps)
    ready()
    misc[...] = jnp.sum(wg[:, part:, :].astype(F32), axis=0)
    w = 3 * head

    def block(i):
        p = mm(full[i], whole(wg, part, 0, w)) + misc[7:8, :w]
        for j in range(3):
            qkv[j, pl.ds(i * rows, rows), :] = p[:, j * head : (j + 1) * head].astype(BF)

    def three(j, _):
        block(lax.select(j == 0, t, lax.select(j == 1, core, cross)))
        return 0

    lax.fori_loop(0, 3, three, 0)
    for c in fc:
        c.wait_recv()
    block(diag)
    for c in xc + cc + fc:
        c.wait_send()


def moments(h):
    mean = jnp.mean(h, axis=-1, keepdims=True)
    c = h - mean
    r = lax.rsqrt(jnp.mean(c * c, axis=-1, keepdims=True) + EPSILON)
    return c * r, r


def norm_back(dy, g, xhat, r):
    dx = dy * g
    return r * (
        dx
        - jnp.mean(dx, axis=-1, keepdims=True)
        - xhat * jnp.mean(dx * xhat, axis=-1, keepdims=True)
    )


def scatter_tools(core, cross, part, cs, cr, xs, xr, sems):
    ccs, ccr, xxs, xxr = sems
    a = lambda i, k: send(cs.at[k], cr.at[k], ccs.at[i, k], ccr.at[i, k], tensor=core)
    b = lambda i, k: send(xs.at[k], xr.at[k], xxs.at[i, k], xxr.at[i, k], tensor=cross)

    def put(i, k, tile, count):
        if i > 0:
            a(i - 1, k).wait_send()
        width = part.shape[-1] // count
        for j in range(count):
            p = tile(j)
            m = p.shape[0] // 4
            c = slice(j * width, (j + 1) * width)
            cs[k, 0, :, c] = p[m : 2 * m].astype(BF)
            cs[k, 1, :, c] = p[3 * m :].astype(BF)
            part[k, 0, :, c] = p[:m]
            part[k, 1, :, c] = p[2 * m : 3 * m]
        a(i, k).start()

    def across(i, k):
        a(i, k).wait_recv()
        if i > 0:
            b(i - 1, k).wait_send()
        xs[k] = (part[k, 1] + cr[k, 1].astype(F32)).astype(BF)
        b(i, k).start()
        part[k, 0] = part[k, 0] + cr[k, 0].astype(F32)

    def take(i, k):
        b(i, k).wait_recv()
        return part[k, 0] + xr[k].astype(F32)

    def end(i, k):
        a(i, k).wait_send()
        b(i, k).wait_send()

    return put, across, take, end


def block_rows(ref, device, c0, c1, n):
    size = ref.shape[0] // n
    return ref.at[pl.ds(pl.multiple_of(device * size, size), size), pl.ds(c0, c1 - c0)]


class RingSum:
    def __init__(self, n, place, at, local, c0, c1, buf, ss, rs, longer):
        nxt, prv = at((place + 1) % n), at((place + n - 1) % n)
        right = n // 2 if longer else n - 1 - n // 2
        self.buf, self.local = buf, lambda p: block_rows(local, at((p + n) % n), c0, c1, n)
        self.place = place
        self.chains = (
            (0, right, lambda s: place + right - s, nxt),
            (right, n - 1 - right, lambda s: place - (n - 1 - right) + s, prv),
        )
        self.ss, self.rs = ss, rs

    def copy(self, chain, s):
        base, _, owner, target = chain
        src = self.local(owner(0)) if s == 0 else self.buf.at[base + s - 1]
        j = base + s
        return send(src, self.buf.at[j], self.ss.at[j], self.rs.at[j], fsdp=target)

    def go(self, s):
        for chain in self.chains:
            base, hops, owner, _ = chain
            if s >= hops:
                continue
            if s > 0:
                self.copy(chain, s - 1).wait_recv()
                j = base + s - 1
                self.buf[j] = (self.buf[j].astype(F32) + self.local(owner(s))[...].astype(F32)).astype(BF)
            self.copy(chain, s).start()

    def close(self):
        total = self.local(self.place)[...].astype(F32)
        for chain in self.chains:
            self.copy(chain, chain[1] - 1).wait_recv()
            total = total + self.buf[chain[0] + chain[1] - 1].astype(F32)
        return total

    def sent(self):
        for chain in self.chains:
            for s in range(chain[1]):
                self.copy(chain, s).wait_send()


def ring_group(n, place, at, local, tracks):
    m = len(tracks)
    q = [RingSum(n, place, at, local, j * 128, j * 128 + 128, *tracks[j], j % 2) for j in range(m)]
    left = list(range(n // 2))

    def go():
        if left:
            s = left.pop(0)
            for r in q:
                r.go(s)

    def close():
        while left:
            go()
        x = jnp.concatenate([r.close() for r in q], axis=1)
        for r in q:
            r.sent()
        return x

    return go, close


def ring_scratch(n, rows, widths):
    out = []
    for w in widths:
        out += [pltpu.VMEM((n - 1, rows, w), BF)]
        out += [DMA((n - 1,)), DMA((n - 1,))]
    return out


def attend_block(i, lo, hi, heads, sq_ref, sk_ref, pad_ref, qt, kh, vt, sc, ctx_ref, octx_ref, lse_ref):
    q0 = pl.multiple_of(i * BQ, BQ)
    sq = sq_ref[0:1, pl.ds(q0, BQ)]
    qpos = q0 + lax.broadcasted_iota(jnp.int32, (BK, BQ), 1)
    part = sc.shape[1] // BK
    spot = lambda h, j: (sc.shape[0] // heads * h + j // part, pl.ds(pl.multiple_of(j % part * BK, BK), BK), slice(None))

    def first(j, c):
        k0 = pl.multiple_of(j * BK, BK)
        sk = jnp.concatenate([sk_ref[pl.ds(k0, BK), :]] * (BQ // 128), axis=1)
        kpos = k0 + lax.broadcasted_iota(jnp.int32, (BK, BQ), 0)
        ok = (sk == sq) | (kpos == qpos)
        out = []
        for h in range(heads):
            s = jnp.where(ok, mm(kh(h, j)[...], qt(h, i)[...]), -1e30)
            sc[spot(h, j)] = s
            out.append(jnp.maximum(c[h], fold_max(s)))
        return tuple(out)

    m = lax.fori_loop(lo, hi, first, (jnp.full((8, BQ), -3e38, F32),) * heads)
    m = [jnp.max(x, axis=0, keepdims=True) for x in m]

    def second(j, c):
        out = []
        for h in range(heads):
            l, acc = c[2 * h : 2 * h + 2]
            p = jnp.exp(sc[spot(h, j)] - m[h])
            out += [l + fold_sum(p), acc + mm(vt(h, j)[...], p.astype(BF))]
        return tuple(out)

    c = lax.fori_loop(lo, hi, second, (jnp.zeros((8, BQ), F32), jnp.zeros((DH, BQ), F32)) * heads)
    o = []
    for h in range(heads):
        l, acc = c[2 * h : 2 * h + 2]
        l = jnp.sum(l, axis=0, keepdims=True)
        lse_ref[h : h + 1, pl.ds(q0, BQ)] = m[h] + jnp.log(l)
        o.append(acc / l)
    ot = jnp.concatenate(o, axis=0) * pad_ref[0:1, pl.ds(q0, BQ)]
    octx_ref[:, pl.ds(q0, BQ)] = ot
    ctx_ref[pl.ds(q0, BQ), :] = ot.T.astype(BF)


def middle_kernel(n, ring, *refs):
    refs = list(refs)
    pop = lambda m: [refs.pop(0) for _ in range(m)]
    tok, cot_hbm = pop(2)
    raw = pop(9 if ring else 2)
    if ring:
        wh, wd = pop(2)
    else:
        wg, wf = pop(2)
    full, qkv, sq, sk, live_row, bounds = pop(6)
    if ring:
        (wg,) = pop(1)
    out, dfirst, dctx, octx, lse, gown, gsend, gup, gdown, sums = pop(10)
    misc, pad = pop(2)
    mine = near = nsem = psems = None
    if ring:
        mine = pop(1)[0]
        near = pop(len(raw))
        nsem = pop(1)[0]
    tsems = pop(7)
    if ring:
        psems = pop(4)
    if ring:
        (wf,) = pop(1)
    ctx, call, slab, wo, dsend = pop(5)
    (norm, dff, acted, dgelu, pre, dpre, first, xhat, r1, part, csem, lsem) = pop(12)
    cs, cr, xs, xr = pop(4)
    ocs, ocr = pop(2)
    rsem = pop(4)
    gsem = pop(6)
    osem = pop(2)
    ssem = pop(6)
    asem = pop(6)
    dsem = pop(6)
    ff = wf.shape[2] // 2
    if ring:
        wsem = pop(4)
    t, f, core, cross, diag, place, at = places(n)
    rows, d = out.shape
    fetch = pltpu.make_async_copy(cot_hbm, out, csem.at[0])
    fetch.start()
    nch = rows // ROWS
    wpart = wg.shape[1] - MISC
    fpart = wf.shape[1]
    width = ctx.shape[1]
    heads = width // DH
    where = (t, core, cross, diag)
    put, across, take, end = scatter_tools(core, cross, part, cs, cr, xs, xr, rsem)
    gs = {}
    for i, buf in enumerate((norm, dff)):
        gs[i] = (
            lambda k, buf=buf, i=i: send(buf.at[k, 0], buf.at[k, 2], gsem[0].at[i, k], gsem[1].at[i, k], tensor=cross),
            lambda k, buf=buf, i=i: send(buf.at[k, 0], buf.at[k, 1], gsem[2].at[i, k], gsem[3].at[i, k], tensor=core),
            lambda k, buf=buf, i=i: send(buf.at[k, 2], buf.at[k, 3], gsem[4].at[i, k], gsem[5].at[i, k], tensor=core),
        )

    def share(i, k):
        gs[i][0](k).start()
        gs[i][1](k).start()

    def shared(i, k):
        gs[i][0](k).wait_recv()
        gs[i][2](k).start()
        gs[i][1](k).wait_recv()
        gs[i][2](k).wait_recv()

    lane0 = d - slab.shape[-1]
    slab0 = wg.at[:, pl.ds(0, wpart), pl.ds(lane0, slab.shape[-1])]
    slabs = (
        send(slab0, slab.at[1], ssem[0].at[0], ssem[1].at[0], tensor=cross),
        send(slab0, slab.at[0], ssem[2].at[0], ssem[3].at[0], tensor=core),
        send(slab.at[1], slab.at[2], ssem[4].at[0], ssem[5].at[0], tensor=core),
    )

    def rows_at(w, k):
        return pl.ds(pl.multiple_of(w * rows + k * ROWS, ROWS), ROWS)

    def give(j, k):
        return send(ctx.at[rows_at(where[j], k), :], call.at[k, j], asem[2 * j - 2].at[k], asem[2 * j - 1].at[k], tensor=where[j])

    def back(j, k):
        return send(dsend.at[k, j - 1], dctx.at[rows_at(t, k), :], dsem[2 * j - 2].at[k], dsem[2 * j - 1].at[k], tensor=where[j])

    load = []
    steps = []
    if ring:
        load = [
            pltpu.make_async_copy(wh, wf.at[f, :, pl.ds(0, ff)], lsem.at[0]),
            pltpu.make_async_copy(wd, wf.at[f, :, pl.ds(ff, ff)], lsem.at[1]),
        ]
        steps = both_ways(n, place, at, wf.at[f], wf, wsem)

    def lead():
        for c in load:
            c.start()

    def follow():
        for c in load:
            c.wait()
        for c in steps[0]:
            c.start()

    def ready():
        slabs[0].start()
        slabs[1].start()

    outs = (full, qkv, misc, sq, sk, live_row, pad, bounds)
    project_part(n, ring, tok, raw, outs, wg, mine, near, nsem, tsems, psems, lead, follow, ready)
    sums[...] = jnp.zeros_like(sums)

    blocks = 4 * rows // BQ
    across_lanes = d // BQ

    def turned(top):
        def tile(h, i):
            lanes = pl.ds(pl.multiple_of(i % across_lanes * BQ, BQ), BQ)
            return dff.at[h, i // across_lanes, pl.ds(top, DH), lanes]

        return tile

    qt, vt = turned(0), turned(DH)
    stack = 4 * ROWS // BK

    def kh(h, j):
        lanes = pl.ds(pl.multiple_of(j // stack * 128, 128), DH)
        return acted.at[h, pl.ds(pl.multiple_of(j % stack * BK, BK), BK), lanes]

    def prepare(i, _):
        r = pl.ds(pl.multiple_of(i * BQ, BQ), BQ)
        qs = (qkv[0, r, :].astype(F32) * 0.125).T.astype(BF)
        vs = qkv[2, r, :].astype(F32).T.astype(BF)
        ks = qkv[1, r, :]
        for h in range(heads):
            c = slice(h * DH, (h + 1) * DH)
            qt(h, i)[...] = qs[c]
            vt(h, i)[...] = vs[c]
            kh(h, i)[...] = ks[:, c]
        return 0

    lax.fori_loop(0, blocks, prepare, 0)
    reach = (MOST - 2 + BK) // BK

    def attend(base, stride, count):
        def body(i, _):
            b = base + i * stride
            lo = jnp.maximum(b - reach, 0)
            hi = jnp.minimum(b + reach + 1, blocks)
            attend_block(b, lo, hi, heads, sq, sk, live_row, qt, kh, vt, dgelu, ctx, octx, lse)
            return 0

        lax.fori_loop(0, count, body, 0)

    def give_when(sent):
        for w in range(4):
            ks = [k for k in range(nch) if k in sent[w]]
            for j in (3, 2, 1):

                @pl.when(where[j] == w)
                def _(j=j, ks=ks):
                    for k in ks:
                        give(j, k).start()

    def rows_of(k):
        return pl.ds(pl.multiple_of(k * ROWS, ROWS), ROWS)

    def pad_rows(k):
        return pad[rows_at(t, k), 0:1]

    def live(k, x):
        s = jnp.sum(x * x, axis=-1, keepdims=True) * pad_rows(k)
        return jnp.sum(s, axis=0, keepdims=True)

    lane = lax.broadcasted_iota(jnp.int32, (1, d), 1)

    def note(j, v):
        sums[7:8, :] += jnp.where(lane == d // 2 + j, v, 0.0)

    def norm_one(k):
        for j in (1, 2, 3):
            give(j, k).wait_recv()
        call[k, 0] = ctx[rows_at(t, k), :]
        x = full[t, rows_of(k), :].astype(F32)
        branch = misc[4:5, :]
        for j in range(4):
            branch = branch + mm(call[k, j], wo[j], 1, 1)
        xh, r = moments(x + branch)
        y = xh * misc[0:1, :] + misc[2:3, :]
        first[k] = y
        xhat[k] = xh
        r1[k] = r
        norm[k, 0] = y.astype(BF)
        share(0, k)
        note(0, live(k, x))
        note(1, live(k, branch))
        note(3, jnp.sum(pad_rows(k), axis=0, keepdims=True))

    def loop(fn):
        def body(k, _):
            fn(k)
            return 0

        lax.fori_loop(0, nch, body, 0)

    done, whole_rows = set(), [set() for _ in range(4)]

    def ran(ids):
        done.update(r for b in ids for r in range(b * BQ // ROWS, (b + 1) * BQ // ROWS))
        fresh = [
            {k for k in range(nch) if w * nch + k in done and k not in whole_rows[w]} for w in range(4)
        ]
        for w in range(4):
            whole_rows[w] |= fresh[w]
        give_when(fresh)

    attend(0, 1, 2)
    ran((0, 1))
    if ring:
        ring_on(steps, 1)
    attend(3, 1, 2)
    ran((3, 4))
    slabs[0].wait_recv()
    slabs[2].start()
    if ring:
        ring_on(steps, 2)
    attend(2, 1, 1)
    slabs[1].wait_recv()
    slabs[2].wait_recv()
    wo[0] = whole(wg, wpart, lane0, d)[:, -width:]
    for j in range(3):
        wo[j + 1] = slab[j].reshape(d, slab.shape[-1])[:, -width:]
    norm_one(0)
    attend(5, 1, 1)
    ran((2, 5))
    if ring:
        for s in range(3, len(steps)):
            ring_on(steps, s)
    for k in range(1, nch):
        norm_one(k)
    if ring:
        ring_end(steps)
    inv = 0.7071067811865476
    thirds = ff // BQ

    def feed(k):
        shared(0, k)
        def half(b):
            x = norm[k, 2 * b : 2 * b + 2].reshape(2 * ROWS, d)
            for c in range(0, ff, 256):
                pre[:, c : c + 256] = mm(x, whole(wf, fpart, c, c + 256)) + misc[6:7, c : c + 256]

        def act(i, b):
            u = pre[pl.ds(pl.multiple_of(i * 64, 64), 64), :]
            s = pl.ds(pl.multiple_of(b * 2 * ROWS + i * 64, 64), 64)
            cdf = 0.5 + 0.5 * lax.erf(u * inv)
            acted[k, s, :] = (u * cdf).astype(BF)
            slope = cdf + u * (jnp.exp(-0.5 * u * u) * 0.3989422804014327)
            for c in range(thirds):
                dgelu[k * thirds + c, s, :] = slope[:, c * BQ : (c + 1) * BQ]
            return b

        half(0)
        pl.when(k > 0)(lambda: across(0, k - 1))
        lax.fori_loop(0, 2 * ROWS // 64, act, 0)
        half(1)
        lax.fori_loop(0, 2 * ROWS // 64, act, 1)
        put(0, k, lambda j: mm(acted[k], some(wf, fpart, ff, 2 * ff, j, 2), 1, 1), 2)

    loop(feed)
    across(0, nch - 1)
    fetch.wait()

    def norm_two(k):
        branch = take(0, k) + misc[5:6, :]
        xh, r = moments(first[k] + branch)
        dy = out[rows_of(k), :].astype(F32)
        out[rows_of(k), :] = (xh * misc[1:2, :] + misc[3:4, :]).astype(BF)
        ds = norm_back(dy, misc[1:2, :], xh, r)
        first[k] = ds
        low = ds.astype(BF)
        dff[k, 0] = low
        share(1, k)
        note(2, live(k, branch))
        sums[1:2, :] += col_sum(dy * xh)
        sums[3:4, :] += col_sum(dy)
        sums[5:6, :] += col_sum(low.astype(F32))

    loop(norm_two)

    def feed_back(k):
        shared(1, k)
        def half(b):
            g = dff[k, 2 * b : 2 * b + 2].reshape(2 * ROWS, d)
            for c in range(0, ff, 256):
                pre[:, c : c + 256] = mm(g, whole(wf, fpart, ff + c, ff + c + 256))

        def act(i, b):
            r = pl.ds(pl.multiple_of(i * 64, 64), 64)
            s = pl.ds(pl.multiple_of(b * 2 * ROWS + i * 64, 64), 64)
            slope = jnp.concatenate([dgelu[k * thirds + c, s, :] for c in range(thirds)], axis=1)
            low = (pre[r, :] * slope).astype(BF)
            dpre[k, s, :] = low
            sums[6:7, :] += col_sum(low.astype(F32))
            return b

        half(0)
        pl.when(k > 0)(lambda: across(1, k - 1))
        lax.fori_loop(0, 2 * ROWS // 64, act, 0)
        half(1)
        lax.fori_loop(0, 2 * ROWS // 64, act, 1)
        put(1, k, lambda j: mm(dpre[k], some(wf, fpart, 0, ff, j, 2), 1, 1), 2)

    def weight_part(left, right, to):
        def cols(i, _):
            c = pl.ds(pl.multiple_of(i * 128, 128), 128)
            g = 0.0
            for k in range(nch):
                g = g + mm(left[k, :, :, c].reshape(4 * ROWS, 128), right[k], 0, 0)
            to[c, :] = g.astype(BF)
            return 0

        lax.fori_loop(0, d // 128, cols, 0)

    def norm_one_back(k):
        dy = first[k] + take(1, k)
        xh = xhat[k]
        ds = norm_back(dy, misc[0:1, :], xh, r1[k])
        dfirst[rows_of(k), :] = ds
        low = ds.astype(BF)
        for c in gs[1][:2]:
            c(k).wait_send()
        dff[k, 0] = low
        for j in (3, 2, 1):
            dsend[k, j - 1] = mm(low, wo[j]).astype(BF)
            back(j, k).start()
        dctx[rows_at(t, k), :] = mm(low, wo[0]).astype(BF)
        sums[0:1, :] += col_sum(dy * xh)
        sums[2:3, :] += col_sum(dy)
        sums[4:5, :] += col_sum(low.astype(F32))

    oc = send(ocs, ocr, osem[0].at[0], osem[1].at[0], tensor=core)

    def out_part():
        x = dff[:, 0].reshape(rows, d)
        for slot, j in ((0, 1), (1, 3)):
            ocs[slot] = mm(x, call[:, j].reshape(rows, width), 0, 0).astype(BF)
        oc.start()

    def out_take():
        x = dff[:, 0].reshape(rows, d)
        for slot, j, to in ((1, 2, gsend), (0, 0, gown)):
            p = mm(x, call[:, j].reshape(rows, width), 0, 0)
            if slot:
                oc.wait_recv()
            to[...] = (p + ocr[slot].astype(F32)).astype(BF)

    loop(feed_back)
    across(1, nch - 1)
    weight_part(dff, acted, gdown)
    norm_one_back(0)
    weight_part(norm, dpre, gup)
    for k in range(1, nch):
        norm_one_back(k)
    out_part()
    out_take()

    def finish(k, _):
        end(1, k)
        for j in (1, 2, 3):
            back(j, k).wait_recv()
            back(j, k).wait_send()
            give(j, k).wait_send()
        for c in gs[0] + gs[1][2:]:
            c(k).wait_send()
        return 0

    lax.fori_loop(0, nch, finish, 0)
    for c in slabs + (oc,):
        c.wait_send()


def middle(n, tok, cot, head, seg, alive, raw, wh, wd, wg, wf):
    ring = wf is None
    vm = pl.BlockSpec(memory_space=pltpu.VMEM)
    far = pl.BlockSpec(memory_space=pltpu.HBM)
    pin = lambda x: pltpu.with_memory_space_constraint(x, pltpu.HBM)
    rows, d = cot.shape
    width = head
    heads = width // DH
    total = 4 * rows
    nch = rows // ROWS
    s = jax.ShapeDtypeStruct
    V = pltpu.VMEM
    ff = wh.shape[1] if ring else wf.shape[2] // 2
    tables = (seg.reshape(-1, 128), alive.reshape(-1, 128))
    if ring:
        ops = tuple(pin(x) for x in (tok, cot) + tables + raw + (wh, wd))
        specs = [far] * len(ops)
    else:
        ops = (tok, pin(cot)) + tables + (wg, wf)
        specs = [vm, far] + [vm] * 4
    outs = [
        s((4, rows, d), BF),
        s((3, total, width), BF),
        s((1, total), F32),
        s((total, 128), F32),
        s((1, total), F32),
        s((2 * total // BQ,), jnp.int32),
    ]
    ospecs = [vm] * 5 + [pl.BlockSpec(memory_space=pltpu.SMEM)]
    if ring:
        outs.append(s((n, d // n + MISC, d), BF))
    outs += [
        s((rows, d), BF),
        s((rows, d), F32),
        s((total, width), BF),
        s((width, total), F32),
        s((heads, total), F32),
        s((d, width), BF),
        s((d, width), BF),
        s((d, ff), BF),
        s((d, ff), BF),
        s((8, d), F32),
    ]
    ospecs += [vm] * (len(outs) - len(ospecs))
    g, gr = (n, d // n) if ring else (wg.shape[0], wg.shape[1] - MISC)
    wide = -(-width // 128) * 128
    scratch = [V((MISC, d), F32), V((total, 128), F32)]
    if ring:
        held = tables + raw
        scratch += [V((d // n + MISC, d), BF)] + [V(x.shape, x.dtype) for x in held] + [DMA((len(held),))]
    scratch += [DMA((2,))] + [DMA((nch,))] * 6
    if ring:
        scratch += [DMA((n // 2, 2))] * 4
        scratch += [V((n, d // n, 2 * ff), BF)]
    scratch += [V((total, width), BF), V((nch, 4, ROWS, width), BF), V((3, g, gr, wide), BF), V((4, d, width), BF)]
    scratch += [V((nch, 3, ROWS, width), BF)]
    scratch += [V((nch, 4, ROWS, d), BF)] * 2
    scratch += [V((nch, 4 * ROWS, ff), BF), V((nch * (ff // BQ), 4 * ROWS, BQ), F32), V((2 * ROWS, ff), F32), V((nch, 4 * ROWS, ff), BF)]
    scratch += [V((nch, ROWS, d), F32)] * 2 + [V((nch, ROWS, 1), F32)]
    scratch += [V((nch, 2, ROWS, d), F32), DMA((1,)), DMA((2,))]
    scratch += [V((nch, 2, ROWS, d), BF)] * 2 + [V((nch, ROWS, d), BF)] * 2
    scratch += [V((2, d, width), BF)] * 2
    scratch += [DMA((2, nch))] * 10 + [DMA((1,))] * 8 + [DMA((nch,))] * 12
    if ring:
        scratch += [DMA((n // 2, 2))] * 4
    return pl.pallas_call(
        functools.partial(middle_kernel, n, ring),
        in_specs=specs,
        out_specs=ospecs,
        out_shape=outs,
        scratch_shapes=scratch,
        compiler_params=pltpu.CompilerParams(
            collective_id=2, has_side_effects=True, vmem_limit_bytes=38 << 20
        ),
        name="middle",
    )(*ops)


def attend_back_part(heads, reach, hook, qkv_ref, dc_ref, oct_ref, lse_ref, sq_ref, sk_ref, pad_ref, dqkv_ref, scratch):
    qt, dt, kt, kh, vh, qh, dh, dqt, dsum, dka, dva = scratch
    S=qkv_ref.shape[1]; W=heads*DH
    qs=(qkv_ref[0].astype(F32)*0.125)
    qsb=qs.astype(BF); qt[...]=qs.T.astype(BF)
    kk=qkv_ref[1]; vv=qkv_ref[2]
    kt[...]=kk.astype(F32).T.astype(BF)
    dct=dc_ref[...].astype(F32).T*pad_ref[0:1,:]
    dt[...]=dct.astype(BF)
    dcn=dct.T.astype(BF)
    prod=dct*oct_ref[...]
    for h in range(heads):
        c=slice(h*DH,(h+1)*DH)
        kh[h]=kk[:,c]; vh[h]=vv[:,c]; qh[h]=qsb[:,c]; dh[h]=dcn[:,c]
        dsum[h:h+1,:]=jnp.sum(prod[h*DH:(h+1)*DH],axis=0,keepdims=True)
    dqt[...]=jnp.zeros_like(dqt)
    def kblock(j):
        k0=j*BK
        lo=max(j-reach,0); hi=min(j+reach+1,S//BQ)
        sk=jnp.concatenate([sk_ref[pl.ds(k0,BK),:]]*(BQ//128),axis=1)
        kpos=k0+lax.broadcasted_iota(jnp.int32,(BK,BQ),0)
        dka[...]=jnp.zeros_like(dka); dva[...]=jnp.zeros_like(dva)
        def body(i,_):
            q0=pl.multiple_of(i*BQ,BQ)
            sq=sq_ref[0:1,pl.ds(q0,BQ)]
            qpos=q0+lax.broadcasted_iota(jnp.int32,(BK,BQ),1)
            ok=(sk==sq)|(kpos==qpos)
            for h in range(heads):
                r=slice(h*DH,(h+1)*DH)
                s=jnp.where(ok,mm(kh[h,pl.ds(k0,BK),:],qt[r,pl.ds(q0,BQ)]),-1e30)
                p=jnp.exp(s-lse_ref[h:h+1,pl.ds(q0,BQ)])
                dp=mm(vh[h,pl.ds(k0,BK),:],dt[r,pl.ds(q0,BQ)])
                ds=(p*(dp-dsum[h:h+1,pl.ds(q0,BQ)])).astype(BF)
                dva[h]+=mm(p.astype(BF),dh[h,pl.ds(q0,BQ),:])
                dka[h]+=mm(ds,qh[h,pl.ds(q0,BQ),:])
                dqt[r,pl.ds(q0,BQ)]+=mm(kt[r,pl.ds(k0,BK)],ds)
            return 0
        lax.fori_loop(lo,hi,body,0)
        dqkv_ref[pl.ds(k0,BK),W:]=jnp.concatenate([dka[h] for h in range(heads)]+[dva[h] for h in range(heads)],axis=1).astype(BF)
    for j in range(S//BK):
        kblock(j)
        hook(j)
    dqkv_ref[:,:W]=(dqt[...]*0.125).T.astype(BF)


def last_kernel(n, ring, *refs):
    refs = list(refs)
    pop = lambda m: [refs.pop(0) for _ in range(m)]
    qkv, dctx, octx, lse, sq, sk, live_row = pop(7)
    wg, full, gown, gsend, dfirst, sums = pop(6)
    if ring:
        gup, gdown = pop(2)
        dtok, oattn, oout, oup, odown, ogain, oshift, obias, ohb, oqvb, oroot = pop(11)
    else:
        dtok, gb, total = pop(3)
    dqkv, gfar = pop(2)
    bscratch = pop(11)
    osem = pop(2)
    part, cs, cr, xs, xr = pop(5)
    rsem = pop(4)
    msend, mrecv = pop(2)
    msem = pop(4)
    if ring:
        gb, mall = pop(2)
        mring = pop(4)
        tracks = [refs[i : i + 3] for i in range(0, len(refs), 3)]
    t, f, core, cross, diag, place, at = places(n)
    rows, d = dtok.shape
    nch = rows // ROWS
    wpart = wg.shape[1] - MISC
    width = qkv.shape[2]
    w3 = 3 * width
    where = (t, core, cross, diag)
    put, across, take, end = scatter_tools(core, cross, part, cs, cr, xs, xr, rsem)
    nxt, prv = at((place + 1) % n), at((place + n - 1) % n)

    def rows_of(k):
        return pl.ds(pl.multiple_of(k * ROWS, ROWS), ROWS)

    meet(core, cross, (nxt, prv) if ring else ())
    ox = send(gsend, gfar, osem[0].at[0], osem[1].at[0], tensor=cross)
    ox.start()
    hooks = []
    if ring:
        ups, downs = gup.shape[1] // 128, gdown.shape[1] // 128
        down, down_close = ring_group(n, place, at, gdown, tracks[:downs])
        up, up_close = ring_group(n, place, at, gup, tracks[downs : downs + ups])
        down()
        up()
        hooks = [down, up] * (n // 2)

    def hook(j):
        if j < len(hooks):
            hooks[j]()

    reach = (MOST - 2 + BK) // BK
    attend_back_part(width // DH, reach, hook, qkv, dctx, octx, lse, sq, sk, live_row, dqkv, bscratch)

    b = col_sum(dqkv[...].astype(F32))
    b = jnp.concatenate([b[:, :width], b[:, 2 * width :], jnp.zeros((1, d - 2 * width), F32)], axis=1)
    msend[0] = sums[...]
    msend[0, 7:8, :] = sums[7:8, :] + b
    m0 = send(msend.at[0], mrecv.at[0], msem[0].at[0], msem[1].at[0], tensor=core)
    m1 = send(msend.at[1], mrecv.at[1], msem[2].at[0], msem[3].at[0], tensor=cross)
    m0.start()
    ox.wait_recv()

    def weight_part(i, _):
        c = pl.ds(pl.multiple_of(i * 128, 128), 128)
        g = 0.0
        for j in range(4):
            g = g + mm(full[j, :, c], dqkv[j * rows : (j + 1) * rows, :], 0, 0)
        o = gown[c, :].astype(F32) + gfar[c, :].astype(F32)
        gb[c, :] = jnp.concatenate([g, o], axis=1).astype(BF)
        return 0

    def tokens_part(k):
        x = jnp.concatenate([dqkv[pl.ds(w * rows + k * ROWS, ROWS), :] for w in where], axis=0)
        put(0, k, lambda j: mm(x, some(wg, wpart, 0, w3, j, 2), 1, 1), 2)

    tokens_part(0)
    lax.fori_loop(0, d // 256, weight_part, 0)
    m0.wait_recv()
    msend[1] = msend[0] + mrecv[0]
    m1.start()
    across(0, 0)
    lax.fori_loop(d // 256, d // 128, weight_part, 0)
    if ring:
        go, own_close = ring_group(n, place, at, gb, tracks[ups + downs :])
        go()
    for k in range(1, nch):
        tokens_part(k)
        if k > 1:
            across(0, k - 1)
    m1.wait_recv()
    row = lax.broadcasted_iota(jnp.int32, (8, d), 0)
    col = lax.broadcasted_iota(jnp.int32, (8, d), 1)
    over_tensor = (row < 6) | ((row == 7) & (col >= 2 * width))
    small = jnp.where(over_tensor, msend[1] + mrecv[1], msend[0])

    def keep(k):
        dtok[rows_of(k), :] = dfirst[rows_of(k), :] + take(0, k)

    if ring:
        msend[2] = small
        mall[place] = small
        msteps = []
        far = n // 2
        for s in range(far):
            a, b = (place - s + n) % n, (place + s) % n
            src = msend.at[2] if s == 0 else mall.at[a]
            pair = [send(src, mall.at[a], mring[0].at[s], mring[1].at[s], fsdp=nxt)]
            if s < far - 1:
                src = msend.at[2] if s == 0 else mall.at[b]
                pair.append(send(src, mall.at[b], mring[2].at[s], mring[3].at[s], fsdp=prv))
            msteps.append(pair)
        def spread(r):
            for i, c in enumerate(msteps[r]):
                if r > 0:
                    msteps[r - 1][i].wait_recv()
                c.start()

        spread(0)
        across(0, nch - 1)
        go()
        odown[...] = down_close()
        todo = [functools.partial(keep, k) for k in range(nch)]
        for r in range(1, far):
            spread(r)
            go()
            if r == 1:
                oup[...] = up_close()
            if todo:
                todo.pop(0)()
        for f_ in todo:
            f_()
        msteps[far - 2][1].wait_recv()
        msteps[far - 1][0].wait_recv()
        total = jnp.sum(mall[...], axis=0)
        gp = d // n
        mine = pltpu.roll(total, (d - f * gp) % d, 1)
        ogain[...] = mine[0:2, :gp]
        oshift[...] = mine[2:4, :gp]
        obias[...] = mine[4:6, :gp]
        k = DH // n
        mine = pltpu.roll(total, (d - f * k) % d, 1)
        ohb[...] = jnp.concatenate([mine[6:7, h * DH : (h + 1) * DH] for h in range(ohb.shape[1])], axis=0).T[:k]
        heads = oqvb.shape[0]
        for h in range(heads):
            for j in range(2):
                c = (j * heads + h) * DH
                oqvb[h, j : j + 1, :] = mine[7:8, c : c + DH][:, :k]
        spot = lax.broadcasted_iota(jnp.int32, (1, d), 1) - d // 2
        pick = lambda j: jnp.sum(jnp.where(spot == j, total[7:8], 0.0), axis=1, keepdims=True)
        count = pick(3)
        col = lax.broadcasted_iota(jnp.int32, (1, 128), 1)
        o = jnp.zeros((1, 128), F32)
        for j in range(3):
            o = jnp.where(col == j, jnp.sqrt(pick(j) / (count * d)), o)
        oroot[...] = o
        x = own_close()
        for j in range(3):
            oattn[j] = x[:, j * width : (j + 1) * width]
        oout[...] = x[:, 3 * width :].T
        for pair in msteps:
            for c in pair:
                c.wait_send()
    else:
        across(0, nch - 1)
        total[...] = small
        for k in range(nch):
            keep(k)

    def finish(k, _):
        end(0, k)
        return 0

    lax.fori_loop(0, nch, finish, 0)
    for c in (m0, m1, ox):
        c.wait_send()


def last(n, ring, qkv, dctx, octx, lse, sq, sk, live_row, wg, full, gown, gsend, dfirst, sums, gup, gdown):
    vm = pl.BlockSpec(memory_space=pltpu.VMEM)
    rows, d = dfirst.shape
    width, total = qkv.shape[2], qkv.shape[1]
    heads = width // DH
    nch = rows // ROWS
    s = jax.ShapeDtypeStruct
    V = pltpu.VMEM
    ops = (qkv, dctx, octx, lse, sq, sk, live_row, wg, full, gown, gsend, dfirst, sums)
    outs = [s((rows, d), F32)]
    gp = d // n
    k = DH // n
    if ring:
        ops += (gup, gdown)
        outs += [s((3, gp, width), F32), s((width, gp), F32), s((gp, gup.shape[1]), F32), s((gp, gdown.shape[1]), F32)] + [s((2, gp), F32)] * 3
        outs += [s((k, d // DH), F32), s((heads, 2, k), F32), s((1, 128), F32)]
    else:
        outs += [s((d, d), BF), s((8, d), F32)]
    scratch = [V((total, 3 * width), BF), V((d, width), BF)]
    scratch += [V((width, total), BF)] * 3 + [V((heads, total, DH), BF)] * 4
    scratch += [V((width, total), F32), V((heads, total), F32)] + [V((heads, BK, DH), F32)] * 2
    scratch += [DMA((1,))] * 2
    scratch += [V((nch, 2, ROWS, d), F32)]
    scratch += [V((nch, 2, ROWS, d), BF)] * 2 + [V((nch, ROWS, d), BF)] * 2
    scratch += [DMA((1, nch))] * 4
    scratch += [V((3, 8, d), F32), V((2, 8, d), F32)] + [DMA((1,))] * 4
    if ring:
        scratch += [V((d, d), BF), V((n, 8, d), F32)] + [DMA((n // 2,))] * 4
        scratch += ring_scratch(n, gp, (128,) * ((gup.shape[1] + gdown.shape[1] + d) // 128))
    return pl.pallas_call(
        functools.partial(last_kernel, n, ring),
        in_specs=[vm] * len(ops),
        out_specs=[vm] * len(outs),
        out_shape=outs,
        scratch_shapes=scratch,
        compiler_params=pltpu.CompilerParams(
            collective_id=3, has_side_effects=True, vmem_limit_bytes=30 << 20
        ),
        name="last",
    )(*ops)


def deliver_kernel(*refs):
    m = (len(refs) - 3) // 2
    src, roots, dst, three, sem = refs[:m], refs[m], refs[m + 1 : -2], refs[-2], refs[-1]
    for j in range(m):
        pltpu.make_async_copy(src[j], dst[j], sem.at[j]).start()
    for j in range(three.shape[0]):
        three[j] = jnp.sum(roots[0:1, j : j + 1])
    for j in range(m):
        pltpu.make_async_copy(src[j], dst[j], sem.at[j]).wait()


def deliver(arrays, roots):
    vm = pl.BlockSpec(memory_space=pltpu.VMEM)
    return pl.pallas_call(
        deliver_kernel,
        in_specs=[vm] * (len(arrays) + 1),
        out_specs=[pl.BlockSpec(memory_space=pl.ANY)] * len(arrays) + [pl.BlockSpec(memory_space=pltpu.SMEM)],
        out_shape=[jax.ShapeDtypeStruct(x.shape, x.dtype) for x in arrays] + [jax.ShapeDtypeStruct((3,), F32)],
        scratch_shapes=[DMA((len(arrays),))],
        compiler_params=pltpu.CompilerParams(vmem_limit_bytes=1 << 20),
        name="deliver",
    )(*arrays, roots)


def split_up(value, dim, devices):
    before, after = (value.shape[:dim], value.shape[dim + 1 :])
    return jnp.moveaxis(value.reshape(*before, devices, -1, *after), dim, 0)


def summed_on_arrival(value, axis, dim):
    blocks = split_up(value, dim, lax.axis_size(axis))
    arrived = lax.all_to_all(blocks, axis, split_axis=0, concat_axis=0, tiled=True)
    return arrived.astype(F32).sum(axis=0)


def shards(
    tokens,
    attn_weight,
    query_value_bias,
    out_weight,
    hidden_weight,
    hidden_bias,
    down_weight,
    norm_gains,
    norm_biases,
    output_biases,
    segment_ids,
    padding,
    cotangent,
):
    n = lax.axis_size("fsdp")
    f = lax.axis_index("fsdp")
    t = lax.axis_index("tensor")
    rows, d = tokens.shape
    gp = d // n
    width = attn_weight.shape[2]
    heads = width // DH
    ff = hidden_weight.shape[1]
    ring = gp % 16 == 0 and n % 2 == 0 and n >= 4
    if ring:
        raw = (
            attn_weight,
            out_weight,
            norm_gains,
            norm_biases,
            output_biases,
            hidden_bias.T,
            query_value_bias.transpose(1, 0, 2),
        )
        wh, wd, wg, wf = hidden_weight, down_weight.T, None, None
    else:
        gather = lambda x, dim: lax.all_gather(x, "fsdp", axis=dim, tiled=True)
        w = gather(attn_weight, 1).transpose(1, 0, 2).reshape(d, 3 * width)
        wo = gather(out_weight, 1).T
        b = gather(query_value_bias, 2).reshape(2, width)
        b = jnp.concatenate([b[0], jnp.zeros((width,), BF), b[1], jnp.zeros((width,), BF)])
        misc = jnp.concatenate(
            [
                gather(norm_gains, 1),
                gather(norm_biases, 1),
                gather(output_biases, 1),
                gather(hidden_bias, 1).reshape(1, ff),
                b[None],
                jnp.zeros((MISC - 8, d), BF),
            ]
        )
        wg = jnp.concatenate([jnp.concatenate([w, wo], axis=1), misc])[None]
        wf = jnp.concatenate([gather(hidden_weight, 0), gather(down_weight, 1).T], axis=1)[None]
        wh = wd = raw = None
    got = list(
        middle(n, tokens, cotangent, width, segment_ids, padding, raw, wh, wd, wg, wf)
    )
    full, qkv, seg_row, seg_keys, pad_row, bounds = got[:6]
    if ring:
        wg = got.pop(6)
    layer_out, d_first, d_ctx, ctx_t, lse, g_own, g_send, g_hidden, g_down, sums = got[6:]
    done = last(
        n, ring, qkv, d_ctx, ctx_t, lse, seg_row, seg_keys, pad_row,
        wg, full, g_own, g_send, d_first, sums, g_hidden, g_down,
    )
    if ring:
        done = deliver((layer_out,) + tuple(done[:-1]), done[-1])
        layer_out, d_tokens, g_attn, g_proj, g_hidden, g_down, g_gain, g_shift, g_bias, g_hb, g_qvb, roots = done
        g_down = g_down.T
        g_hb = g_hb.T
        g_qvb = g_qvb.transpose(1, 0, 2)
    else:
        d_tokens, g, total = done
        total = lax.psum(total, "fsdp")
        g_attn = g[:, : 3 * width].reshape(d, 3, width).transpose(1, 0, 2)
        g_attn = summed_on_arrival(g_attn, "fsdp", 1)
        g_proj = summed_on_arrival(g[:, 3 * width :].T, "fsdp", 1)
        g_hidden = summed_on_arrival(g_hidden, "fsdp", 0)
        g_down = summed_on_arrival(g_down.T, "fsdp", 1)
        vectors = lax.dynamic_slice(total, (0, f * gp), (6, gp))
        g_gain, g_shift, g_bias = vectors[0:2], vectors[2:4], vectors[4:6]
        k = DH // n
        g_hb = lax.dynamic_slice(total[6].reshape(ff // DH, DH), (0, f * k), (ff // DH, k))
        g_qvb = lax.dynamic_slice(
            total[7, : 2 * width].reshape(2 * heads, DH), (0, f * k), (2 * heads, k)
        ).reshape(2, heads, k)
        squares = total[7, d // 2 : d // 2 + 4]
        roots = jnp.sqrt(squares[:3] / (squares[3] * d))
    return (
        layer_out,
        d_tokens,
        g_attn,
        g_qvb,
        g_proj,
        g_hidden,
        g_hb,
        g_down,
        g_gain,
        g_shift,
        g_bias,
        roots,
    )


def solution(mesh):
    placed = (
        P(("fsdp", "tensor"), None),
        P(None, "fsdp", "tensor"),
        P(None, "tensor", "fsdp"),
        P("tensor", "fsdp"),
        P("fsdp", "tensor"),
        P("tensor", "fsdp"),
        P("tensor", "fsdp"),
        P(None, "fsdp"),
        P(None, "fsdp"),
        P(None, "fsdp"),
        P("fsdp"),
        P("fsdp"),
        P(("fsdp", "tensor"), None),
    )
    return jax.shard_map(
        shards,
        mesh=mesh,
        in_specs=placed,
        out_specs=(
            P(("fsdp", "tensor"), None),
            P(("fsdp", "tensor"), None),
            P(None, "fsdp", "tensor"),
            P(None, "tensor", "fsdp"),
            P("tensor", "fsdp"),
            P("fsdp", "tensor"),
            P("tensor", "fsdp"),
            P("tensor", "fsdp"),
            P(None, "fsdp"),
            P(None, "fsdp"),
            P(None, "fsdp"),
            P(),
        ),
        check_vma=False,
    )
```

```python
import functools

import jax
import jax.numpy as jnp
from jax import lax
from jax.experimental import pallas as pl
from jax.experimental.pallas import tpu as pltpu
from jax.sharding import PartitionSpec as P

DH = 64
EPSILON = 1e-12
BQ = 256
BK = 256
F32 = jnp.float32
BF = jnp.bfloat16
MESH = pl.DeviceIdType.MESH
DMA = pltpu.SemaphoreType.DMA
ROWS = 128
MISC = 16
MOST = 768


def places(n):
    t = lax.axis_index("tensor")
    f = lax.axis_index("fsdp")
    c, x = t % 2, t // 2
    core, cross, diag = 2 * x + 1 - c, 2 * (1 - x) + c, 2 * (1 - x) + 1 - c
    y, z = f % 2, f // 2
    place = z + y * (n - 1 - 2 * z)

    def at(p):
        y = p // max(n // 2, 1)
        return 2 * (p + y * (n - 1 - 2 * p)) + y

    return t, f, core, cross, diag, place, at


def send(src, dst, ss, rs, **axes):
    return pltpu.make_async_remote_copy(
        src_ref=src, dst_ref=dst, send_sem=ss, recv_sem=rs, device_id=axes, device_id_type=MESH
    )


def meet(core, cross, ring, *more):
    gate = pltpu.get_barrier_semaphore()
    for where in (core, cross) + more:
        pl.semaphore_signal(gate, inc=1, device_id={"tensor": where}, device_id_type=MESH)
    for where in ring:
        pl.semaphore_signal(gate, inc=1, device_id={"fsdp": where}, device_id_type=MESH)
    pl.semaphore_wait(gate, 2 + len(ring) + len(more))


def both_ways(n, place, at, local, held, sems):
    rs, rr, ls, lr = sems
    nxt, prv = at((place + 1) % n), at((place + n - 1) % n)
    far = n // 2
    half = local.shape[0] // 2
    steps = []
    for s in range(far):
        a, b = at((place - s + n) % n), at((place + s) % n)
        up = local if s == 0 else held.at[a]
        down = local if s == 0 else held.at[b]
        row = []
        for k in (0, 1):
            part = pl.ds(k * half, half)
            if s < far - 1 or k == 0:
                row.append(send(up.at[part], held.at[a, part], rs.at[s, k], rr.at[s, k], fsdp=nxt))
            if s < far - 1 or k == 1:
                row.append(send(down.at[part], held.at[b, part], ls.at[s, k], lr.at[s, k], fsdp=prv))
        steps.append(row)
    return steps


def ring_on(steps, s):
    for i, c in enumerate(steps[s]):
        if s < len(steps) - 1:
            steps[s - 1][i].wait_recv()
            c.start()
    if s == len(steps) - 1:
        steps[s - 1][0].wait_recv()
        steps[s][0].start()
        steps[s - 1][1].wait_recv()
        steps[s - 1][2].wait_recv()
        steps[s - 1][3].wait_recv()
        steps[s][1].start()


def ring_end(steps):
    for c in steps[-1]:
        c.wait_recv()
    for row in steps:
        for c in row:
            c.wait_send()


def mm(a, b, ca=1, cb=0):
    return lax.dot_general(a, b, (((ca,), (cb,)), ((), ())), preferred_element_type=F32)


def some(ref, rows, c0, c1, j, count):
    g = ref.shape[0]
    if g % count:
        size = rows // count
        return ref[0, j * size : (j + 1) * size, c0:c1]
    g //= count
    return ref[j * g : (j + 1) * g, :rows, c0:c1].reshape(g * rows, c1 - c0)


def whole(ref, rows, c0, c1):
    g = ref.shape[0]
    return ref[:, :rows, c0:c1].reshape(g * rows, c1 - c0)


def fold_max(s):
    return jnp.max(s.reshape(s.shape[0] // 8, 8, s.shape[1]), axis=0)


def fold_sum(s):
    return jnp.sum(s.reshape(s.shape[0] // 8, 8, s.shape[1]), axis=0)


def col_sum(s):
    return jnp.sum(fold_sum(s), axis=0, keepdims=True)


def project_part(n, ring, tok, far, outs, wg, mine, near, nsem, sems, gsems, lead, follow, ready):
    full, qkv, misc, sq, sk, live, lives, bounds = outs
    if ring:
        for j in range(len(far)):
            pltpu.make_async_copy(far[j], near[j], nsem.at[j]).start()
    else:
        seg, alive = far
    lsem, xs, xr, cs, cr, fs, fr = sems
    t, f, core, cross, diag, place, at = places(n)
    rows, d = tok.shape
    part = wg.shape[1] - MISC
    head = qkv.shape[2]
    if ring:
        for j in range(len(far)):
            pltpu.make_async_copy(far[j], near[j], nsem.at[j]).wait()
        seg, alive, aw, ow, gains, shifts, biases, hb, qvb = near
        mine[:part] = jnp.concatenate([aw[0], aw[1], aw[2], ow[...].astype(F32).T.astype(BF)], axis=1)
        col = lax.broadcasted_iota(jnp.int32, (part, d), 1)
        row = lax.broadcasted_iota(jnp.int32, (part, d), 0)
        spread = (col == f * part + row).astype(BF)
        wide = [mm(r[...], spread) for r in (gains, shifts, biases)]
        k = hb.shape[0]
        col = lax.broadcasted_iota(jnp.int32, (k, d), 1)
        row = lax.broadcasted_iota(jnp.int32, (k, d), 0)
        spread = (col % DH == f * k + row).astype(BF)
        h = mm(hb[...].astype(F32).T.astype(BF), spread)
        col = lax.broadcasted_iota(jnp.int32, h.shape, 1) // DH
        row = lax.broadcasted_iota(jnp.int32, h.shape, 0)
        h = jnp.sum(jnp.where(col == row, h, 0.0), axis=0, keepdims=True)
        b = jnp.zeros((1, d), F32)
        col = lax.broadcasted_iota(jnp.int32, (1, d), 1) // DH
        heads = qvb.shape[0]
        for j in range(heads):
            x = mm(qvb[j], spread)
            b = jnp.where(col == j, x[0:1], jnp.where(col == 2 * heads + j, x[1:2], b))
        mine[part:] = jnp.concatenate(wide + [h, b, jnp.zeros((8, d), F32)], axis=0).astype(BF)
        steps = both_ways(n, place, at, mine, wg, gsems)
        lead()
        meet(core, cross, (at((place + 1) % n), at((place + n - 1) % n)), diag)
    else:
        meet(core, cross, (), diag)
    R = range(rows // ROWS)
    cut = lambda i: pl.ds(i * ROWS, ROWS)
    xc = [send(tok.at[cut(i)], full.at[t, cut(i)], xs.at[i], xr.at[i], tensor=cross) for i in R]
    cc = [send(tok.at[cut(i)], full.at[t, cut(i)], cs.at[i], cr.at[i], tensor=core) for i in R]
    fc = [send(full.at[cross, cut(i)], full.at[cross, cut(i)], fs.at[i], fr.at[i], tensor=core) for i in R]
    own = [pltpu.make_async_copy(tok, full.at[t], lsem.at[0])]
    if ring:
        own.append(pltpu.make_async_copy(mine, wg.at[f], lsem.at[1]))
        for c in steps[0]:
            c.start()
    for c in xc + cc + own:
        c.start()

    groups = seg.shape[0]
    ids = seg[...].astype(F32)
    on = alive[...]
    keys = jnp.where(on == 1, ids, -1.0)
    onf = on.astype(F32)
    for g in range(groups):
        c = slice(g * 128, (g + 1) * 128)
        sq[:, c] = ids[g : g + 1]
        live[:, c] = onf[g : g + 1]
        sk[c, :] = jnp.broadcast_to(keys[g : g + 1], (128, 128)).T
        lives[c, :] = jnp.broadcast_to(onf[g : g + 1], (128, 128)).T
    per = BQ // 128
    for i in range(groups // per):
        under = jnp.sum((ids < ids[i * per : i * per + 1, 0:1]).astype(F32))
        upto = jnp.sum((ids <= ids[(i + 1) * per - 1 : (i + 1) * per, 127:128]).astype(F32))
        bounds[2 * i] = under.astype(jnp.int32) // BK
        bounds[2 * i + 1] = (upto.astype(jnp.int32) + BK - 1) // BK

    if ring:
        for s in range(1, len(steps)):
            ring_on(steps, s)
        follow()
    for i in R:
        xc[i].wait_recv()
        fc[i].start()
    for c in own:
        c.wait()
    for c in cc:
        c.wait_recv()
    if ring:
        ring_end(steps)
    ready()
    misc[...] = jnp.sum(wg[:, part:, :].astype(F32), axis=0)
    w = 3 * head

    def block(i):
        p = mm(full[i], whole(wg, part, 0, w)) + misc[7:8, :w]
        for j in range(3):
            qkv[j, pl.ds(i * rows, rows), :] = p[:, j * head : (j + 1) * head].astype(BF)

    def three(j, _):
        block(lax.select(j == 0, t, lax.select(j == 1, core, cross)))
        return 0

    lax.fori_loop(0, 3, three, 0)
    for c in fc:
        c.wait_recv()
    block(diag)
    for c in xc + cc + fc:
        c.wait_send()


def moments(h):
    mean = jnp.mean(h, axis=-1, keepdims=True)
    c = h - mean
    r = lax.rsqrt(jnp.mean(c * c, axis=-1, keepdims=True) + EPSILON)
    return c * r, r


def norm_back(dy, g, xhat, r):
    dx = dy * g
    return r * (
        dx
        - jnp.mean(dx, axis=-1, keepdims=True)
        - xhat * jnp.mean(dx * xhat, axis=-1, keepdims=True)
    )


def scatter_tools(core, cross, part, cs, cr, xs, xr, sems):
    ccs, ccr, xxs, xxr = sems
    a = lambda i, k: send(cs.at[k], cr.at[k], ccs.at[i, k], ccr.at[i, k], tensor=core)
    b = lambda i, k: send(xs.at[k], xr.at[k], xxs.at[i, k], xxr.at[i, k], tensor=cross)

    def put(i, k, tile, count):
        if i > 0:
            a(i - 1, k).wait_send()
        width = part.shape[-1] // count
        for j in range(count):
            p = tile(j)
            m = p.shape[0] // 4
            c = slice(j * width, (j + 1) * width)
            cs[k, 0, :, c] = p[m : 2 * m].astype(BF)
            cs[k, 1, :, c] = p[3 * m :].astype(BF)
            part[k, 0, :, c] = p[:m]
            part[k, 1, :, c] = p[2 * m : 3 * m]
        a(i, k).start()

    def put_half(i, k, b, tile, count):
        if i > 0 and b == 0:
            a(i - 1, k).wait_send()
        width = part.shape[-1] // count
        for j in range(count):
            p = tile(j)
            m = p.shape[0] // 2
            c = slice(j * width, (j + 1) * width)
            part[k, b, :, c] = p[:m]
            cs[k, b, :, c] = p[m:].astype(BF)
        if b == 1:
            a(i, k).start()

    def across(i, k):
        a(i, k).wait_recv()
        if i > 0:
            b(i - 1, k).wait_send()
        xs[k] = (part[k, 1] + cr[k, 1].astype(F32)).astype(BF)
        b(i, k).start()
        part[k, 0] = part[k, 0] + cr[k, 0].astype(F32)

    def take(i, k):
        b(i, k).wait_recv()
        return part[k, 0] + xr[k].astype(F32)

    def end(i, k):
        a(i, k).wait_send()
        b(i, k).wait_send()

    return put, put_half, across, take, end


def block_rows(ref, device, c0, c1, n):
    size = ref.shape[0] // n
    return ref.at[pl.ds(pl.multiple_of(device * size, size), size), pl.ds(c0, c1 - c0)]


class RingSum:
    def __init__(self, n, place, at, local, c0, c1, buf, ss, rs, longer):
        nxt, prv = at((place + 1) % n), at((place + n - 1) % n)
        right = n // 2 if longer else n - 1 - n // 2
        self.buf, self.local = buf, lambda p: block_rows(local, at((p + n) % n), c0, c1, n)
        self.place = place
        self.chains = (
            (0, right, lambda s: place + right - s, nxt),
            (right, n - 1 - right, lambda s: place - (n - 1 - right) + s, prv),
        )
        self.ss, self.rs = ss, rs

    def copy(self, chain, s):
        base, _, owner, target = chain
        src = self.local(owner(0)) if s == 0 else self.buf.at[base + s - 1]
        j = base + s
        return send(src, self.buf.at[j], self.ss.at[j], self.rs.at[j], fsdp=target)

    def go(self, s):
        for chain in self.chains:
            base, hops, owner, _ = chain
            if s >= hops:
                continue
            if s > 0:
                self.copy(chain, s - 1).wait_recv()
                j = base + s - 1
                self.buf[j] = (self.buf[j].astype(F32) + self.local(owner(s))[...].astype(F32)).astype(BF)
            self.copy(chain, s).start()

    def close(self):
        total = self.local(self.place)[...].astype(F32)
        for chain in self.chains:
            self.copy(chain, chain[1] - 1).wait_recv()
            total = total + self.buf[chain[0] + chain[1] - 1].astype(F32)
        return total

    def sent(self):
        for chain in self.chains:
            for s in range(chain[1]):
                self.copy(chain, s).wait_send()


def ring_group(n, place, at, local, tracks):
    m = len(tracks)
    q = [RingSum(n, place, at, local, j * 128, j * 128 + 128, *tracks[j], j % 2) for j in range(m)]
    left = list(range(n // 2))

    def go():
        if left:
            s = left.pop(0)
            for r in q:
                r.go(s)

    def close():
        while left:
            go()
        x = jnp.concatenate([r.close() for r in q], axis=1)
        for r in q:
            r.sent()
        return x

    return go, close


def ring_scratch(n, rows, widths):
    out = []
    for w in widths:
        out += [pltpu.VMEM((n - 1, rows, w), BF)]
        out += [DMA((n - 1,)), DMA((n - 1,))]
    return out


def attend_block(i, lo, hi, heads, sq_ref, sk_ref, pad_ref, qt, kh, vt, sc, ctx_ref, octx_ref, lse_ref):
    q0 = pl.multiple_of(i * BQ, BQ)
    sq = sq_ref[0:1, pl.ds(q0, BQ)]
    qpos = q0 + lax.broadcasted_iota(jnp.int32, (BK, BQ), 1)
    part = sc.shape[1] // BK
    spot = lambda h, j: (sc.shape[0] // heads * h + j // part, pl.ds(pl.multiple_of(j % part * BK, BK), BK), slice(None))

    def first(j, c):
        k0 = pl.multiple_of(j * BK, BK)
        sk = jnp.concatenate([sk_ref[pl.ds(k0, BK), :]] * (BQ // 128), axis=1)
        kpos = k0 + lax.broadcasted_iota(jnp.int32, (BK, BQ), 0)
        ok = (sk == sq) | (kpos == qpos)
        out = []
        for h in range(heads):
            s = jnp.where(ok, mm(kh(h, j)[...], qt(h, i)[...]), -1e30)
            sc[spot(h, j)] = s
            out.append(jnp.maximum(c[h], fold_max(s)))
        return tuple(out)

    m = lax.fori_loop(lo, hi, first, (jnp.full((8, BQ), -3e38, F32),) * heads)
    m = [jnp.max(x, axis=0, keepdims=True) for x in m]

    def second(j, c):
        out = []
        for h in range(heads):
            l, acc = c[2 * h : 2 * h + 2]
            p = jnp.exp(sc[spot(h, j)] - m[h])
            out += [l + fold_sum(p), acc + mm(vt(h, j)[...], p.astype(BF))]
        return tuple(out)

    c = lax.fori_loop(lo, hi, second, (jnp.zeros((8, BQ), F32), jnp.zeros((DH, BQ), F32)) * heads)
    o = []
    for h in range(heads):
        l, acc = c[2 * h : 2 * h + 2]
        l = jnp.sum(l, axis=0, keepdims=True)
        lse_ref[h : h + 1, pl.ds(q0, BQ)] = m[h] + jnp.log(l)
        o.append(acc / l)
    ot = jnp.concatenate(o, axis=0) * pad_ref[0:1, pl.ds(q0, BQ)]
    octx_ref[:, pl.ds(q0, BQ)] = ot
    ctx_ref[pl.ds(q0, BQ), :] = ot.T.astype(BF)


def middle_kernel(n, ring, *refs):
    refs = list(refs)
    pop = lambda m: [refs.pop(0) for _ in range(m)]
    tok, cot_hbm = pop(2)
    raw = pop(9 if ring else 2)
    if ring:
        wh, wd = pop(2)
    else:
        wg, wf = pop(2)
    full, qkv, sq, sk, live_row, bounds = pop(6)
    if ring:
        (wg,) = pop(1)
    out, dfirst, dctx, octx, lse, gown, gsend, gup, gdown, sums = pop(10)
    misc, pad = pop(2)
    mine = near = nsem = psems = None
    if ring:
        mine = pop(1)[0]
        near = pop(len(raw))
        nsem = pop(1)[0]
    tsems = pop(7)
    if ring:
        psems = pop(4)
    if ring:
        (wf,) = pop(1)
    ctx, call, slab, wo, dsend = pop(5)
    (norm, dff, acted, dgelu, pre, dpre, first, xhat, r1, part, csem, lsem) = pop(12)
    cs, cr, xs, xr = pop(4)
    ocs, ocr = pop(2)
    rsem = pop(4)
    gsem = pop(6)
    osem = pop(2)
    ssem = pop(6)
    asem = pop(6)
    dsem = pop(6)
    ff = wf.shape[2] // 2
    if ring:
        wsem = pop(4)
    t, f, core, cross, diag, place, at = places(n)
    rows, d = out.shape
    fetch = pltpu.make_async_copy(cot_hbm, out, csem.at[0])
    fetch.start()
    nch = rows // ROWS
    wpart = wg.shape[1] - MISC
    fpart = wf.shape[1]
    width = ctx.shape[1]
    heads = width // DH
    where = (t, core, cross, diag)
    put, put_half, across, take, end = scatter_tools(core, cross, part, cs, cr, xs, xr, rsem)
    gs = {}
    for i, buf in enumerate((norm, dff)):
        gs[i] = (
            lambda k, buf=buf, i=i: send(buf.at[k, 0], buf.at[k, 2], gsem[0].at[i, k], gsem[1].at[i, k], tensor=cross),
            lambda k, buf=buf, i=i: send(buf.at[k, 0], buf.at[k, 1], gsem[2].at[i, k], gsem[3].at[i, k], tensor=core),
            lambda k, buf=buf, i=i: send(buf.at[k, 2], buf.at[k, 3], gsem[4].at[i, k], gsem[5].at[i, k], tensor=core),
        )

    def share(i, k):
        gs[i][0](k).start()
        gs[i][1](k).start()

    def shared(i, k):
        gs[i][0](k).wait_recv()
        gs[i][2](k).start()
        gs[i][1](k).wait_recv()
        gs[i][2](k).wait_recv()

    lane0 = d - slab.shape[-1]
    slab0 = wg.at[:, pl.ds(0, wpart), pl.ds(lane0, slab.shape[-1])]
    slabs = (
        send(slab0, slab.at[1], ssem[0].at[0], ssem[1].at[0], tensor=cross),
        send(slab0, slab.at[0], ssem[2].at[0], ssem[3].at[0], tensor=core),
        send(slab.at[1], slab.at[2], ssem[4].at[0], ssem[5].at[0], tensor=core),
    )

    def rows_at(w, k):
        return pl.ds(pl.multiple_of(w * rows + k * ROWS, ROWS), ROWS)

    def give(j, k):
        return send(ctx.at[rows_at(where[j], k), :], call.at[k, j], asem[2 * j - 2].at[k], asem[2 * j - 1].at[k], tensor=where[j])

    def back(j, k):
        return send(dsend.at[k, j - 1], dctx.at[rows_at(t, k), :], dsem[2 * j - 2].at[k], dsem[2 * j - 1].at[k], tensor=where[j])

    load = []
    steps = []
    if ring:
        load = [
            pltpu.make_async_copy(wh, wf.at[f, :, pl.ds(0, ff)], lsem.at[0]),
            pltpu.make_async_copy(wd, wf.at[f, :, pl.ds(ff, ff)], lsem.at[1]),
        ]
        steps = both_ways(n, place, at, wf.at[f], wf, wsem)

    def lead():
        for c in load:
            c.start()

    def follow():
        for c in load:
            c.wait()
        for c in steps[0]:
            c.start()

    def ready():
        slabs[0].start()
        slabs[1].start()

    outs = (full, qkv, misc, sq, sk, live_row, pad, bounds)
    project_part(n, ring, tok, raw, outs, wg, mine, near, nsem, tsems, psems, lead, follow, ready)
    sums[...] = jnp.zeros_like(sums)

    blocks = 4 * rows // BQ
    across_lanes = d // BQ

    def turned(top):
        def tile(h, i):
            lanes = pl.ds(pl.multiple_of(i % across_lanes * BQ, BQ), BQ)
            return dff.at[h, i // across_lanes, pl.ds(top, DH), lanes]

        return tile

    qt, vt = turned(0), turned(DH)
    stack = 4 * ROWS // BK

    def kh(h, j):
        lanes = pl.ds(pl.multiple_of(j // stack * 128, 128), DH)
        return acted.at[h, pl.ds(pl.multiple_of(j % stack * BK, BK), BK), lanes]

    def prepare(i, _):
        r = pl.ds(pl.multiple_of(i * BQ, BQ), BQ)
        qs = (qkv[0, r, :].astype(F32) * 0.125).T.astype(BF)
        vs = qkv[2, r, :].astype(F32).T.astype(BF)
        ks = qkv[1, r, :]
        for h in range(heads):
            c = slice(h * DH, (h + 1) * DH)
            qt(h, i)[...] = qs[c]
            vt(h, i)[...] = vs[c]
            kh(h, i)[...] = ks[:, c]
        return 0

    lax.fori_loop(0, blocks, prepare, 0)
    reach = (MOST - 2 + BK) // BK

    def attend(base, stride, count):
        def body(i, _):
            b = base + i * stride
            lo = jnp.maximum(b - reach, 0)
            hi = jnp.minimum(b + reach + 1, blocks)
            attend_block(b, lo, hi, heads, sq, sk, live_row, qt, kh, vt, dgelu, ctx, octx, lse)
            return 0

        lax.fori_loop(0, count, body, 0)

    def give_when(sent):
        for w in range(4):
            ks = [k for k in range(nch) if k in sent[w]]
            for j in (3, 2, 1):

                @pl.when(where[j] == w)
                def _(j=j, ks=ks):
                    for k in ks:
                        give(j, k).start()

    def rows_of(k):
        return pl.ds(pl.multiple_of(k * ROWS, ROWS), ROWS)

    def pad_rows(k):
        return pad[rows_at(t, k), 0:1]

    def live(k, x):
        s = jnp.sum(x * x, axis=-1, keepdims=True) * pad_rows(k)
        return jnp.sum(s, axis=0, keepdims=True)

    lane = lax.broadcasted_iota(jnp.int32, (1, d), 1)

    def note(j, v):
        sums[7:8, :] += jnp.where(lane == d // 2 + j, v, 0.0)

    def norm_one(k):
        for j in (1, 2, 3):
            give(j, k).wait_recv()
        call[k, 0] = ctx[rows_at(t, k), :]
        x = full[t, rows_of(k), :].astype(F32)
        branch = misc[4:5, :]
        for j in range(4):
            branch = branch + mm(call[k, j], wo[j], 1, 1)
        xh, r = moments(x + branch)
        y = xh * misc[0:1, :] + misc[2:3, :]
        first[k] = y
        xhat[k] = xh
        r1[k] = r
        norm[k, 0] = y.astype(BF)
        share(0, k)
        note(0, live(k, x))
        note(1, live(k, branch))
        note(3, jnp.sum(pad_rows(k), axis=0, keepdims=True))

    def loop(fn):
        def body(k, _):
            fn(k)
            return 0

        lax.fori_loop(0, nch, body, 0)

    done, whole_rows = set(), [set() for _ in range(4)]

    def ran(ids):
        done.update(r for b in ids for r in range(b * BQ // ROWS, (b + 1) * BQ // ROWS))
        fresh = [
            {k for k in range(nch) if w * nch + k in done and k not in whole_rows[w]} for w in range(4)
        ]
        for w in range(4):
            whole_rows[w] |= fresh[w]
        give_when(fresh)

    attend(0, 1, 2)
    ran((0, 1))
    if ring:
        ring_on(steps, 1)
    attend(3, 1, 2)
    ran((3, 4))
    slabs[0].wait_recv()
    slabs[2].start()
    if ring:
        ring_on(steps, 2)
    attend(2, 1, 1)
    slabs[1].wait_recv()
    slabs[2].wait_recv()
    wo[0] = whole(wg, wpart, lane0, d)[:, -width:]
    for j in range(3):
        wo[j + 1] = slab[j].reshape(d, slab.shape[-1])[:, -width:]
    norm_one(0)
    attend(5, 1, 1)
    ran((2, 5))
    if ring:
        for s in range(3, len(steps)):
            ring_on(steps, s)
    for k in range(1, nch):
        norm_one(k)
    if ring:
        ring_end(steps)
    inv = 0.7071067811865476
    thirds = ff // BQ

    def far_rows(i, k):
        gs[i][0](k).wait_recv()
        gs[i][2](k).start()
        if isinstance(k, int):
            if k > 0:
                across(i, k - 1)
        else:
            pl.when(k > 0)(lambda: across(i, k - 1))
        gs[i][2](k).wait_recv()

    def feed(k, b):
        x = norm[k, 2 * b : 2 * b + 2].reshape(2 * ROWS, d)
        for c in range(0, ff, 256):
            pre[:, c : c + 256] = mm(x, whole(wf, fpart, c, c + 256)) + misc[6:7, c : c + 256]

        def act(i, _):
            u = pre[pl.ds(pl.multiple_of(i * 64, 64), 64), :]
            s = pl.ds(pl.multiple_of(b * 2 * ROWS + i * 64, 64), 64)
            cdf = 0.5 + 0.5 * lax.erf(u * inv)
            acted[k, s, :] = (u * cdf).astype(BF)
            slope = cdf + u * (jnp.exp(-0.5 * u * u) * 0.3989422804014327)
            for c in range(thirds):
                dgelu[k * thirds + c, s, :] = slope[:, c * BQ : (c + 1) * BQ]
            return 0

        lax.fori_loop(0, 2 * ROWS // 64, act, 0)
        y = acted[k, 2 * b * ROWS : 2 * (b + 1) * ROWS, :]
        put_half(0, k, b, lambda j: mm(y, some(wf, fpart, ff, 2 * ff, j, 2), 1, 1), 2)

    def feed_near(k):
        gs[0][1](k).wait_recv()
        feed(k, 0)

    def feed_far(k):
        far_rows(0, k)
        feed(k, 1)

    def feed_all(k):
        feed_near(k)
        feed_far(k)

    loop(feed_all)
    across(0, nch - 1)
    fetch.wait()

    def norm_two(k):
        branch = take(0, k) + misc[5:6, :]
        xh, r = moments(first[k] + branch)
        dy = out[rows_of(k), :].astype(F32)
        out[rows_of(k), :] = (xh * misc[1:2, :] + misc[3:4, :]).astype(BF)
        ds = norm_back(dy, misc[1:2, :], xh, r)
        first[k] = ds
        low = ds.astype(BF)
        dff[k, 0] = low
        share(1, k)
        note(2, live(k, branch))
        sums[1:2, :] += col_sum(dy * xh)
        sums[3:4, :] += col_sum(dy)
        sums[5:6, :] += col_sum(low.astype(F32))

    loop(norm_two)

    def feed_back(k, b):
        g = dff[k, 2 * b : 2 * b + 2].reshape(2 * ROWS, d)
        for c in range(0, ff, 256):
            pre[:, c : c + 256] = mm(g, whole(wf, fpart, ff + c, ff + c + 256))

        def act(i, _):
            r = pl.ds(pl.multiple_of(i * 64, 64), 64)
            s = pl.ds(pl.multiple_of(b * 2 * ROWS + i * 64, 64), 64)
            slope = jnp.concatenate([dgelu[k * thirds + c, s, :] for c in range(thirds)], axis=1)
            low = (pre[r, :] * slope).astype(BF)
            dpre[k, s, :] = low
            sums[6:7, :] += col_sum(low.astype(F32))
            return 0

        lax.fori_loop(0, 2 * ROWS // 64, act, 0)
        y = dpre[k, 2 * b * ROWS : 2 * (b + 1) * ROWS, :]
        put_half(1, k, b, lambda j: mm(y, some(wf, fpart, 0, ff, j, 2), 1, 1), 2)

    def back_near(k):
        gs[1][1](k).wait_recv()
        feed_back(k, 0)

    def back_far(k):
        far_rows(1, k)
        feed_back(k, 1)

    def weight_part(left, right, to):
        def cols(i, _):
            c = pl.ds(pl.multiple_of(i * 128, 128), 128)
            g = 0.0
            for k in range(nch):
                g = g + mm(left[k, :, :, c].reshape(4 * ROWS, 128), right[k], 0, 0)
            to[c, :] = g.astype(BF)
            return 0

        lax.fori_loop(0, d // 128, cols, 0)

    def norm_one_back(k):
        dy = first[k] + take(1, k)
        xh = xhat[k]
        ds = norm_back(dy, misc[0:1, :], xh, r1[k])
        dfirst[rows_of(k), :] = ds
        low = ds.astype(BF)
        for c in gs[1][:2]:
            c(k).wait_send()
        dff[k, 0] = low
        for j in (3, 2, 1):
            dsend[k, j - 1] = mm(low, wo[j]).astype(BF)
            back(j, k).start()
        dctx[rows_at(t, k), :] = mm(low, wo[0]).astype(BF)
        sums[0:1, :] += col_sum(dy * xh)
        sums[2:3, :] += col_sum(dy)
        sums[4:5, :] += col_sum(low.astype(F32))

    oc = send(ocs, ocr, osem[0].at[0], osem[1].at[0], tensor=core)

    def out_part():
        x = dff[:, 0].reshape(rows, d)
        for slot, j in ((0, 1), (1, 3)):
            ocs[slot] = mm(x, call[:, j].reshape(rows, width), 0, 0).astype(BF)
        oc.start()

    def out_take():
        x = dff[:, 0].reshape(rows, d)
        for slot, j, to in ((1, 2, gsend), (0, 0, gown)):
            p = mm(x, call[:, j].reshape(rows, width), 0, 0)
            if slot:
                oc.wait_recv()
            to[...] = (p + ocr[slot].astype(F32)).astype(BF)

    for k in range(2):
        back_near(k)
    back_far(0)
    for k in range(2, nch):
        back_near(k)
    for k in range(1, nch):
        back_far(k)
    across(1, nch - 1)
    weight_part(dff, acted, gdown)
    norm_one_back(0)
    weight_part(norm, dpre, gup)
    for k in range(1, nch):
        norm_one_back(k)
    out_part()
    out_take()

    def finish(k, _):
        end(1, k)
        for j in (1, 2, 3):
            back(j, k).wait_recv()
            back(j, k).wait_send()
            give(j, k).wait_send()
        for c in gs[0] + gs[1][2:]:
            c(k).wait_send()
        return 0

    lax.fori_loop(0, nch, finish, 0)
    for c in slabs + (oc,):
        c.wait_send()


def middle(n, tok, cot, head, seg, alive, raw, wh, wd, wg, wf):
    ring = wf is None
    vm = pl.BlockSpec(memory_space=pltpu.VMEM)
    far = pl.BlockSpec(memory_space=pltpu.HBM)
    pin = lambda x: pltpu.with_memory_space_constraint(x, pltpu.HBM)
    rows, d = cot.shape
    width = head
    heads = width // DH
    total = 4 * rows
    nch = rows // ROWS
    s = jax.ShapeDtypeStruct
    V = pltpu.VMEM
    ff = wh.shape[1] if ring else wf.shape[2] // 2
    tables = (seg.reshape(-1, 128), alive.reshape(-1, 128))
    if ring:
        ops = tuple(pin(x) for x in (tok, cot) + tables + raw + (wh, wd))
        specs = [far] * len(ops)
    else:
        ops = (tok, pin(cot)) + tables + (wg, wf)
        specs = [vm, far] + [vm] * 4
    outs = [
        s((4, rows, d), BF),
        s((3, total, width), BF),
        s((1, total), F32),
        s((total, 128), F32),
        s((1, total), F32),
        s((2 * total // BQ,), jnp.int32),
    ]
    ospecs = [vm] * 5 + [pl.BlockSpec(memory_space=pltpu.SMEM)]
    if ring:
        outs.append(s((n, d // n + MISC, d), BF))
    outs += [
        s((rows, d), BF),
        s((rows, d), F32),
        s((total, width), BF),
        s((width, total), F32),
        s((heads, total), F32),
        s((d, width), BF),
        s((d, width), BF),
        s((d, ff), BF),
        s((d, ff), BF),
        s((8, d), F32),
    ]
    ospecs += [vm] * (len(outs) - len(ospecs))
    g, gr = (n, d // n) if ring else (wg.shape[0], wg.shape[1] - MISC)
    wide = -(-width // 128) * 128
    scratch = [V((MISC, d), F32), V((total, 128), F32)]
    if ring:
        held = tables + raw
        scratch += [V((d // n + MISC, d), BF)] + [V(x.shape, x.dtype) for x in held] + [DMA((len(held),))]
    scratch += [DMA((2,))] + [DMA((nch,))] * 6
    if ring:
        scratch += [DMA((n // 2, 2))] * 4
        scratch += [V((n, d // n, 2 * ff), BF)]
    scratch += [V((total, width), BF), V((nch, 4, ROWS, width), BF), V((3, g, gr, wide), BF), V((4, d, width), BF)]
    scratch += [V((nch, 3, ROWS, width), BF)]
    scratch += [V((nch, 4, ROWS, d), BF)] * 2
    scratch += [V((nch, 4 * ROWS, ff), BF), V((nch * (ff // BQ), 4 * ROWS, BQ), F32), V((2 * ROWS, ff), F32), V((nch, 4 * ROWS, ff), BF)]
    scratch += [V((nch, ROWS, d), F32)] * 2 + [V((nch, ROWS, 1), F32)]
    scratch += [V((nch, 2, ROWS, d), F32), DMA((1,)), DMA((2,))]
    scratch += [V((nch, 2, ROWS, d), BF)] * 2 + [V((nch, ROWS, d), BF)] * 2
    scratch += [V((2, d, width), BF)] * 2
    scratch += [DMA((2, nch))] * 10 + [DMA((1,))] * 8 + [DMA((nch,))] * 12
    if ring:
        scratch += [DMA((n // 2, 2))] * 4
    return pl.pallas_call(
        functools.partial(middle_kernel, n, ring),
        in_specs=specs,
        out_specs=ospecs,
        out_shape=outs,
        scratch_shapes=scratch,
        compiler_params=pltpu.CompilerParams(
            collective_id=2, has_side_effects=True, vmem_limit_bytes=38 << 20
        ),
        name="middle",
    )(*ops)


def attend_back_part(heads, reach, hook, qkv_ref, dc_ref, oct_ref, lse_ref, sq_ref, sk_ref, pad_ref, dqkv_ref, scratch):
    qt, dt, kt, kh, vh, qh, dh, dqt, dsum, dka, dva = scratch
    S=qkv_ref.shape[1]; W=heads*DH
    qs=(qkv_ref[0].astype(F32)*0.125)
    qsb=qs.astype(BF); qt[...]=qs.T.astype(BF)
    kk=qkv_ref[1]; vv=qkv_ref[2]
    kt[...]=kk.astype(F32).T.astype(BF)
    dct=dc_ref[...].astype(F32).T*pad_ref[0:1,:]
    dt[...]=dct.astype(BF)
    dcn=dct.T.astype(BF)
    prod=dct*oct_ref[...]
    for h in range(heads):
        c=slice(h*DH,(h+1)*DH)
        kh[h]=kk[:,c]; vh[h]=vv[:,c]; qh[h]=qsb[:,c]; dh[h]=dcn[:,c]
        dsum[h:h+1,:]=jnp.sum(prod[h*DH:(h+1)*DH],axis=0,keepdims=True)
    dqt[...]=jnp.zeros_like(dqt)
    def kblock(j):
        k0=j*BK
        lo=max(j-reach,0); hi=min(j+reach+1,S//BQ)
        sk=jnp.concatenate([sk_ref[pl.ds(k0,BK),:]]*(BQ//128),axis=1)
        kpos=k0+lax.broadcasted_iota(jnp.int32,(BK,BQ),0)
        dka[...]=jnp.zeros_like(dka); dva[...]=jnp.zeros_like(dva)
        def body(i,_):
            q0=pl.multiple_of(i*BQ,BQ)
            sq=sq_ref[0:1,pl.ds(q0,BQ)]
            qpos=q0+lax.broadcasted_iota(jnp.int32,(BK,BQ),1)
            ok=(sk==sq)|(kpos==qpos)
            for h in range(heads):
                r=slice(h*DH,(h+1)*DH)
                s=jnp.where(ok,mm(kh[h,pl.ds(k0,BK),:],qt[r,pl.ds(q0,BQ)]),-1e30)
                p=jnp.exp(s-lse_ref[h:h+1,pl.ds(q0,BQ)])
                dp=mm(vh[h,pl.ds(k0,BK),:],dt[r,pl.ds(q0,BQ)])
                ds=(p*(dp-dsum[h:h+1,pl.ds(q0,BQ)])).astype(BF)
                dva[h]+=mm(p.astype(BF),dh[h,pl.ds(q0,BQ),:])
                dka[h]+=mm(ds,qh[h,pl.ds(q0,BQ),:])
                dqt[r,pl.ds(q0,BQ)]+=mm(kt[r,pl.ds(k0,BK)],ds)
            return 0
        lax.fori_loop(lo,hi,body,0)
        dqkv_ref[pl.ds(k0,BK),W:]=jnp.concatenate([dka[h] for h in range(heads)]+[dva[h] for h in range(heads)],axis=1).astype(BF)
    for j in range(S//BK):
        kblock(j)
        hook(j)
    dqkv_ref[:,:W]=(dqt[...]*0.125).T.astype(BF)


def last_kernel(n, ring, *refs):
    refs = list(refs)
    pop = lambda m: [refs.pop(0) for _ in range(m)]
    qkv, dctx, octx, lse, sq, sk, live_row = pop(7)
    wg, full, gown, gsend, dfirst, sums = pop(6)
    if ring:
        gup, gdown = pop(2)
        dtok, oattn, oout, oup, odown, ogain, oshift, obias, ohb, oqvb, oroot = pop(11)
    else:
        dtok, gb, total = pop(3)
    dqkv, gfar = pop(2)
    bscratch = pop(11)
    osem = pop(2)
    part, cs, cr, xs, xr = pop(5)
    rsem = pop(4)
    msend, mrecv = pop(2)
    msem = pop(4)
    if ring:
        gb, mall = pop(2)
        mring = pop(4)
        tracks = [refs[i : i + 3] for i in range(0, len(refs), 3)]
    t, f, core, cross, diag, place, at = places(n)
    rows, d = dtok.shape
    nch = rows // ROWS
    wpart = wg.shape[1] - MISC
    width = qkv.shape[2]
    w3 = 3 * width
    where = (t, core, cross, diag)
    put, put_half, across, take, end = scatter_tools(core, cross, part, cs, cr, xs, xr, rsem)
    nxt, prv = at((place + 1) % n), at((place + n - 1) % n)

    def rows_of(k):
        return pl.ds(pl.multiple_of(k * ROWS, ROWS), ROWS)

    meet(core, cross, (nxt, prv) if ring else ())
    ox = send(gsend, gfar, osem[0].at[0], osem[1].at[0], tensor=cross)
    ox.start()
    hooks = []
    if ring:
        ups, downs = gup.shape[1] // 128, gdown.shape[1] // 128
        down, down_close = ring_group(n, place, at, gdown, tracks[:downs])
        up, up_close = ring_group(n, place, at, gup, tracks[downs : downs + ups])
        down()
        up()
        hooks = [down, up] * (n // 2)

    def hook(j):
        if j < len(hooks):
            hooks[j]()

    reach = (MOST - 2 + BK) // BK
    attend_back_part(width // DH, reach, hook, qkv, dctx, octx, lse, sq, sk, live_row, dqkv, bscratch)

    b = col_sum(dqkv[...].astype(F32))
    b = jnp.concatenate([b[:, :width], b[:, 2 * width :], jnp.zeros((1, d - 2 * width), F32)], axis=1)
    msend[0] = sums[...]
    msend[0, 7:8, :] = sums[7:8, :] + b
    m0 = send(msend.at[0], mrecv.at[0], msem[0].at[0], msem[1].at[0], tensor=core)
    m1 = send(msend.at[1], mrecv.at[1], msem[2].at[0], msem[3].at[0], tensor=cross)
    m0.start()
    ox.wait_recv()

    def weight_part(i, _):
        c = pl.ds(pl.multiple_of(i * 128, 128), 128)
        g = 0.0
        for j in range(4):
            g = g + mm(full[j, :, c], dqkv[j * rows : (j + 1) * rows, :], 0, 0)
        o = gown[c, :].astype(F32) + gfar[c, :].astype(F32)
        gb[c, :] = jnp.concatenate([g, o], axis=1).astype(BF)
        return 0

    def tokens_part(k):
        x = jnp.concatenate([dqkv[pl.ds(w * rows + k * ROWS, ROWS), :] for w in where], axis=0)
        put(0, k, lambda j: mm(x, some(wg, wpart, 0, w3, j, 2), 1, 1), 2)

    tokens_part(0)
    lax.fori_loop(0, d // 256, weight_part, 0)
    m0.wait_recv()
    msend[1] = msend[0] + mrecv[0]
    m1.start()
    across(0, 0)
    lax.fori_loop(d // 256, d // 128, weight_part, 0)
    if ring:
        go, own_close = ring_group(n, place, at, gb, tracks[ups + downs :])
        go()
    for k in range(1, nch):
        tokens_part(k)
        if k > 1:
            across(0, k - 1)
    m1.wait_recv()
    row = lax.broadcasted_iota(jnp.int32, (8, d), 0)
    col = lax.broadcasted_iota(jnp.int32, (8, d), 1)
    over_tensor = (row < 6) | ((row == 7) & (col >= 2 * width))
    small = jnp.where(over_tensor, msend[1] + mrecv[1], msend[0])

    def keep(k):
        dtok[rows_of(k), :] = dfirst[rows_of(k), :] + take(0, k)

    if ring:
        msend[2] = small
        mall[place] = small
        msteps = []
        far = n // 2
        for s in range(far):
            a, b = (place - s + n) % n, (place + s) % n
            src = msend.at[2] if s == 0 else mall.at[a]
            pair = [send(src, mall.at[a], mring[0].at[s], mring[1].at[s], fsdp=nxt)]
            if s < far - 1:
                src = msend.at[2] if s == 0 else mall.at[b]
                pair.append(send(src, mall.at[b], mring[2].at[s], mring[3].at[s], fsdp=prv))
            msteps.append(pair)
        def spread(r):
            for i, c in enumerate(msteps[r]):
                if r > 0:
                    msteps[r - 1][i].wait_recv()
                c.start()

        spread(0)
        across(0, nch - 1)
        go()
        odown[...] = down_close()
        todo = [functools.partial(keep, k) for k in range(nch)]
        for r in range(1, far):
            spread(r)
            go()
            if r == 1:
                oup[...] = up_close()
            if todo:
                todo.pop(0)()
        for f_ in todo:
            f_()
        msteps[far - 2][1].wait_recv()
        msteps[far - 1][0].wait_recv()
        total = jnp.sum(mall[...], axis=0)
        gp = d // n
        mine = pltpu.roll(total, (d - f * gp) % d, 1)
        ogain[...] = mine[0:2, :gp]
        oshift[...] = mine[2:4, :gp]
        obias[...] = mine[4:6, :gp]
        k = DH // n
        mine = pltpu.roll(total, (d - f * k) % d, 1)
        ohb[...] = jnp.concatenate([mine[6:7, h * DH : (h + 1) * DH] for h in range(ohb.shape[1])], axis=0).T[:k]
        heads = oqvb.shape[0]
        for h in range(heads):
            for j in range(2):
                c = (j * heads + h) * DH
                oqvb[h, j : j + 1, :] = mine[7:8, c : c + DH][:, :k]
        spot = lax.broadcasted_iota(jnp.int32, (1, d), 1) - d // 2
        pick = lambda j: jnp.sum(jnp.where(spot == j, total[7:8], 0.0), axis=1, keepdims=True)
        count = pick(3)
        col = lax.broadcasted_iota(jnp.int32, (1, 128), 1)
        o = jnp.zeros((1, 128), F32)
        for j in range(3):
            o = jnp.where(col == j, jnp.sqrt(pick(j) / (count * d)), o)
        oroot[...] = o
        x = own_close()
        for j in range(3):
            oattn[j] = x[:, j * width : (j + 1) * width]
        oout[...] = x[:, 3 * width :].T
        for pair in msteps:
            for c in pair:
                c.wait_send()
    else:
        across(0, nch - 1)
        total[...] = small
        for k in range(nch):
            keep(k)

    def finish(k, _):
        end(0, k)
        return 0

    lax.fori_loop(0, nch, finish, 0)
    for c in (m0, m1, ox):
        c.wait_send()


def last(n, ring, qkv, dctx, octx, lse, sq, sk, live_row, wg, full, gown, gsend, dfirst, sums, gup, gdown):
    vm = pl.BlockSpec(memory_space=pltpu.VMEM)
    rows, d = dfirst.shape
    width, total = qkv.shape[2], qkv.shape[1]
    heads = width // DH
    nch = rows // ROWS
    s = jax.ShapeDtypeStruct
    V = pltpu.VMEM
    ops = (qkv, dctx, octx, lse, sq, sk, live_row, wg, full, gown, gsend, dfirst, sums)
    outs = [s((rows, d), F32)]
    gp = d // n
    k = DH // n
    if ring:
        ops += (gup, gdown)
        outs += [s((3, gp, width), F32), s((width, gp), F32), s((gp, gup.shape[1]), F32), s((gp, gdown.shape[1]), F32)] + [s((2, gp), F32)] * 3
        outs += [s((k, d // DH), F32), s((heads, 2, k), F32), s((1, 128), F32)]
    else:
        outs += [s((d, d), BF), s((8, d), F32)]
    scratch = [V((total, 3 * width), BF), V((d, width), BF)]
    scratch += [V((width, total), BF)] * 3 + [V((heads, total, DH), BF)] * 4
    scratch += [V((width, total), F32), V((heads, total), F32)] + [V((heads, BK, DH), F32)] * 2
    scratch += [DMA((1,))] * 2
    scratch += [V((nch, 2, ROWS, d), F32)]
    scratch += [V((nch, 2, ROWS, d), BF)] * 2 + [V((nch, ROWS, d), BF)] * 2
    scratch += [DMA((1, nch))] * 4
    scratch += [V((3, 8, d), F32), V((2, 8, d), F32)] + [DMA((1,))] * 4
    if ring:
        scratch += [V((d, d), BF), V((n, 8, d), F32)] + [DMA((n // 2,))] * 4
        scratch += ring_scratch(n, gp, (128,) * ((gup.shape[1] + gdown.shape[1] + d) // 128))
    return pl.pallas_call(
        functools.partial(last_kernel, n, ring),
        in_specs=[vm] * len(ops),
        out_specs=[vm] * len(outs),
        out_shape=outs,
        scratch_shapes=scratch,
        compiler_params=pltpu.CompilerParams(
            collective_id=3, has_side_effects=True, vmem_limit_bytes=30 << 20
        ),
        name="last",
    )(*ops)


def deliver_kernel(*refs):
    m = (len(refs) - 3) // 2
    src, roots, dst, three, sem = refs[:m], refs[m], refs[m + 1 : -2], refs[-2], refs[-1]
    for j in range(m):
        pltpu.make_async_copy(src[j], dst[j], sem.at[j]).start()
    for j in range(three.shape[0]):
        three[j] = jnp.sum(roots[0:1, j : j + 1])
    for j in range(m):
        pltpu.make_async_copy(src[j], dst[j], sem.at[j]).wait()


def deliver(arrays, roots):
    vm = pl.BlockSpec(memory_space=pltpu.VMEM)
    return pl.pallas_call(
        deliver_kernel,
        in_specs=[vm] * (len(arrays) + 1),
        out_specs=[pl.BlockSpec(memory_space=pl.ANY)] * len(arrays) + [pl.BlockSpec(memory_space=pltpu.SMEM)],
        out_shape=[jax.ShapeDtypeStruct(x.shape, x.dtype) for x in arrays] + [jax.ShapeDtypeStruct((3,), F32)],
        scratch_shapes=[DMA((len(arrays),))],
        compiler_params=pltpu.CompilerParams(vmem_limit_bytes=1 << 20),
        name="deliver",
    )(*arrays, roots)


def split_up(value, dim, devices):
    before, after = (value.shape[:dim], value.shape[dim + 1 :])
    return jnp.moveaxis(value.reshape(*before, devices, -1, *after), dim, 0)


def summed_on_arrival(value, axis, dim):
    blocks = split_up(value, dim, lax.axis_size(axis))
    arrived = lax.all_to_all(blocks, axis, split_axis=0, concat_axis=0, tiled=True)
    return arrived.astype(F32).sum(axis=0)


def shards(
    tokens,
    attn_weight,
    query_value_bias,
    out_weight,
    hidden_weight,
    hidden_bias,
    down_weight,
    norm_gains,
    norm_biases,
    output_biases,
    segment_ids,
    padding,
    cotangent,
):
    n = lax.axis_size("fsdp")
    f = lax.axis_index("fsdp")
    t = lax.axis_index("tensor")
    rows, d = tokens.shape
    gp = d // n
    width = attn_weight.shape[2]
    heads = width // DH
    ff = hidden_weight.shape[1]
    ring = gp % 16 == 0 and n % 2 == 0 and n >= 4
    if ring:
        raw = (
            attn_weight,
            out_weight,
            norm_gains,
            norm_biases,
            output_biases,
            hidden_bias.T,
            query_value_bias.transpose(1, 0, 2),
        )
        wh, wd, wg, wf = hidden_weight, down_weight.T, None, None
    else:
        gather = lambda x, dim: lax.all_gather(x, "fsdp", axis=dim, tiled=True)
        w = gather(attn_weight, 1).transpose(1, 0, 2).reshape(d, 3 * width)
        wo = gather(out_weight, 1).T
        b = gather(query_value_bias, 2).reshape(2, width)
        b = jnp.concatenate([b[0], jnp.zeros((width,), BF), b[1], jnp.zeros((width,), BF)])
        misc = jnp.concatenate(
            [
                gather(norm_gains, 1),
                gather(norm_biases, 1),
                gather(output_biases, 1),
                gather(hidden_bias, 1).reshape(1, ff),
                b[None],
                jnp.zeros((MISC - 8, d), BF),
            ]
        )
        wg = jnp.concatenate([jnp.concatenate([w, wo], axis=1), misc])[None]
        wf = jnp.concatenate([gather(hidden_weight, 0), gather(down_weight, 1).T], axis=1)[None]
        wh = wd = raw = None
    got = list(
        middle(n, tokens, cotangent, width, segment_ids, padding, raw, wh, wd, wg, wf)
    )
    full, qkv, seg_row, seg_keys, pad_row, bounds = got[:6]
    if ring:
        wg = got.pop(6)
    layer_out, d_first, d_ctx, ctx_t, lse, g_own, g_send, g_hidden, g_down, sums = got[6:]
    done = last(
        n, ring, qkv, d_ctx, ctx_t, lse, seg_row, seg_keys, pad_row,
        wg, full, g_own, g_send, d_first, sums, g_hidden, g_down,
    )
    if ring:
        done = deliver((layer_out,) + tuple(done[:-1]), done[-1])
        layer_out, d_tokens, g_attn, g_proj, g_hidden, g_down, g_gain, g_shift, g_bias, g_hb, g_qvb, roots = done
        g_down = g_down.T
        g_hb = g_hb.T
        g_qvb = g_qvb.transpose(1, 0, 2)
    else:
        d_tokens, g, total = done
        total = lax.psum(total, "fsdp")
        g_attn = g[:, : 3 * width].reshape(d, 3, width).transpose(1, 0, 2)
        g_attn = summed_on_arrival(g_attn, "fsdp", 1)
        g_proj = summed_on_arrival(g[:, 3 * width :].T, "fsdp", 1)
        g_hidden = summed_on_arrival(g_hidden, "fsdp", 0)
        g_down = summed_on_arrival(g_down.T, "fsdp", 1)
        vectors = lax.dynamic_slice(total, (0, f * gp), (6, gp))
        g_gain, g_shift, g_bias = vectors[0:2], vectors[2:4], vectors[4:6]
        k = DH // n
        g_hb = lax.dynamic_slice(total[6].reshape(ff // DH, DH), (0, f * k), (ff // DH, k))
        g_qvb = lax.dynamic_slice(
            total[7, : 2 * width].reshape(2 * heads, DH), (0, f * k), (2 * heads, k)
        ).reshape(2, heads, k)
        squares = total[7, d // 2 : d // 2 + 4]
        roots = jnp.sqrt(squares[:3] / (squares[3] * d))
    return (
        layer_out,
        d_tokens,
        g_attn,
        g_qvb,
        g_proj,
        g_hidden,
        g_hb,
        g_down,
        g_gain,
        g_shift,
        g_bias,
        roots,
    )


def solution(mesh):
    placed = (
        P(("fsdp", "tensor"), None),
        P(None, "fsdp", "tensor"),
        P(None, "tensor", "fsdp"),
        P("tensor", "fsdp"),
        P("fsdp", "tensor"),
        P("tensor", "fsdp"),
        P("tensor", "fsdp"),
        P(None, "fsdp"),
        P(None, "fsdp"),
        P(None, "fsdp"),
        P("fsdp"),
        P("fsdp"),
        P(("fsdp", "tensor"), None),
    )
    return jax.shard_map(
        shards,
        mesh=mesh,
        in_specs=placed,
        out_specs=(
            P(("fsdp", "tensor"), None),
            P(("fsdp", "tensor"), None),
            P(None, "fsdp", "tensor"),
            P(None, "tensor", "fsdp"),
            P("tensor", "fsdp"),
            P("fsdp", "tensor"),
            P("tensor", "fsdp"),
            P("tensor", "fsdp"),
            P(None, "fsdp"),
            P(None, "fsdp"),
            P(None, "fsdp"),
            P(),
        ),
        check_vma=False,
    )
```

```python
import functools

import jax
import jax.numpy as jnp
from jax import lax
from jax.experimental import pallas as pl
from jax.experimental.pallas import tpu as pltpu
from jax.sharding import PartitionSpec as P

DH = 64
EPSILON = 1e-12
BQ = 256
BK = 256
F32 = jnp.float32
BF = jnp.bfloat16
MESH = pl.DeviceIdType.MESH
DMA = pltpu.SemaphoreType.DMA
ROWS = 128
MISC = 16
MOST = 768


def places(n):
    t = lax.axis_index("tensor")
    f = lax.axis_index("fsdp")
    c, x = t % 2, t // 2
    core, cross, diag = 2 * x + 1 - c, 2 * (1 - x) + c, 2 * (1 - x) + 1 - c
    y, z = f % 2, f // 2
    place = z + y * (n - 1 - 2 * z)

    def at(p):
        y = p // max(n // 2, 1)
        return 2 * (p + y * (n - 1 - 2 * p)) + y

    return t, f, core, cross, diag, place, at


def send(src, dst, ss, rs, **axes):
    return pltpu.make_async_remote_copy(
        src_ref=src, dst_ref=dst, send_sem=ss, recv_sem=rs, device_id=axes, device_id_type=MESH
    )


def meet(core, cross, ring, *more):
    gate = pltpu.get_barrier_semaphore()
    for where in (core, cross) + more:
        pl.semaphore_signal(gate, inc=1, device_id={"tensor": where}, device_id_type=MESH)
    for where in ring:
        pl.semaphore_signal(gate, inc=1, device_id={"fsdp": where}, device_id_type=MESH)
    pl.semaphore_wait(gate, 2 + len(ring) + len(more))


def both_ways(n, place, at, local, held, sems):
    rs, rr, ls, lr = sems
    nxt, prv = at((place + 1) % n), at((place + n - 1) % n)
    far = n // 2
    half = local.shape[0] // 2
    steps = []
    for s in range(far):
        a, b = at((place - s + n) % n), at((place + s) % n)
        up = local if s == 0 else held.at[a]
        down = local if s == 0 else held.at[b]
        row = []
        for k in (0, 1):
            part = pl.ds(k * half, half)
            if s < far - 1 or k == 0:
                row.append(send(up.at[part], held.at[a, part], rs.at[s, k], rr.at[s, k], fsdp=nxt))
            if s < far - 1 or k == 1:
                row.append(send(down.at[part], held.at[b, part], ls.at[s, k], lr.at[s, k], fsdp=prv))
        steps.append(row)
    return steps


def ring_on(steps, s):
    for i, c in enumerate(steps[s]):
        if s < len(steps) - 1:
            steps[s - 1][i].wait_recv()
            c.start()
    if s == len(steps) - 1:
        steps[s - 1][0].wait_recv()
        steps[s][0].start()
        steps[s - 1][1].wait_recv()
        steps[s - 1][2].wait_recv()
        steps[s - 1][3].wait_recv()
        steps[s][1].start()


def ring_end(steps):
    for c in steps[-1]:
        c.wait_recv()
    for row in steps:
        for c in row:
            c.wait_send()


def mm(a, b, ca=1, cb=0):
    return lax.dot_general(a, b, (((ca,), (cb,)), ((), ())), preferred_element_type=F32)


def some(ref, rows, c0, c1, j, count):
    g = ref.shape[0]
    if g % count:
        size = rows // count
        return ref[0, j * size : (j + 1) * size, c0:c1]
    g //= count
    return ref[j * g : (j + 1) * g, :rows, c0:c1].reshape(g * rows, c1 - c0)


def whole(ref, rows, c0, c1):
    g = ref.shape[0]
    return ref[:, :rows, c0:c1].reshape(g * rows, c1 - c0)


def fold_max(s):
    return jnp.max(s.reshape(s.shape[0] // 8, 8, s.shape[1]), axis=0)


def fold_sum(s):
    return jnp.sum(s.reshape(s.shape[0] // 8, 8, s.shape[1]), axis=0)


def col_sum(s):
    return jnp.sum(fold_sum(s), axis=0, keepdims=True)


def project_part(n, ring, tok, far, outs, wg, mine, near, nsem, sems, gsems, lead, follow, ready):
    full, qkv, misc, sq, sk, live, lives, bounds = outs
    if ring:
        for j in range(len(far)):
            pltpu.make_async_copy(far[j], near[j], nsem.at[j]).start()
    else:
        seg, alive = far
    lsem, xs, xr, cs, cr, fs, fr = sems
    t, f, core, cross, diag, place, at = places(n)
    rows, d = tok.shape
    part = wg.shape[1] - MISC
    head = qkv.shape[2]
    if ring:
        for j in range(len(far)):
            pltpu.make_async_copy(far[j], near[j], nsem.at[j]).wait()
        seg, alive, aw, ow, gains, shifts, biases, hb, qvb = near
        mine[:part] = jnp.concatenate([aw[0], aw[1], aw[2], ow[...].astype(F32).T.astype(BF)], axis=1)
        col = lax.broadcasted_iota(jnp.int32, (part, d), 1)
        row = lax.broadcasted_iota(jnp.int32, (part, d), 0)
        spread = (col == f * part + row).astype(BF)
        wide = [mm(r[...], spread) for r in (gains, shifts, biases)]
        k = hb.shape[0]
        col = lax.broadcasted_iota(jnp.int32, (k, d), 1)
        row = lax.broadcasted_iota(jnp.int32, (k, d), 0)
        spread = (col % DH == f * k + row).astype(BF)
        h = mm(hb[...].astype(F32).T.astype(BF), spread)
        col = lax.broadcasted_iota(jnp.int32, h.shape, 1) // DH
        row = lax.broadcasted_iota(jnp.int32, h.shape, 0)
        h = jnp.sum(jnp.where(col == row, h, 0.0), axis=0, keepdims=True)
        b = jnp.zeros((1, d), F32)
        col = lax.broadcasted_iota(jnp.int32, (1, d), 1) // DH
        heads = qvb.shape[0]
        for j in range(heads):
            x = mm(qvb[j], spread)
            b = jnp.where(col == j, x[0:1], jnp.where(col == 2 * heads + j, x[1:2], b))
        mine[part:] = jnp.concatenate(wide + [h, b, jnp.zeros((8, d), F32)], axis=0).astype(BF)
        steps = both_ways(n, place, at, mine, wg, gsems)
        lead()
        meet(core, cross, (at((place + 1) % n), at((place + n - 1) % n)), diag)
    else:
        meet(core, cross, (), diag)
    R = range(rows // ROWS)
    cut = lambda i: pl.ds(i * ROWS, ROWS)
    xc = [send(tok.at[cut(i)], full.at[t, cut(i)], xs.at[i], xr.at[i], tensor=cross) for i in R]
    cc = [send(tok.at[cut(i)], full.at[t, cut(i)], cs.at[i], cr.at[i], tensor=core) for i in R]
    fc = [send(full.at[cross, cut(i)], full.at[cross, cut(i)], fs.at[i], fr.at[i], tensor=core) for i in R]
    own = [pltpu.make_async_copy(tok, full.at[t], lsem.at[0])]
    if ring:
        own.append(pltpu.make_async_copy(mine, wg.at[f], lsem.at[1]))
        for c in steps[0]:
            c.start()
    for c in xc + cc + own:
        c.start()

    groups = seg.shape[0]
    ids = seg[...].astype(F32)
    on = alive[...]
    keys = jnp.where(on == 1, ids, -1.0)
    onf = on.astype(F32)
    for g in range(groups):
        c = slice(g * 128, (g + 1) * 128)
        sq[:, c] = ids[g : g + 1]
        live[:, c] = onf[g : g + 1]
        sk[c, :] = jnp.broadcast_to(keys[g : g + 1], (128, 128)).T
        lives[c, :] = jnp.broadcast_to(onf[g : g + 1], (128, 128)).T
    per = BQ // 128
    for i in range(groups // per):
        under = jnp.sum((ids < ids[i * per : i * per + 1, 0:1]).astype(F32))
        upto = jnp.sum((ids <= ids[(i + 1) * per - 1 : (i + 1) * per, 127:128]).astype(F32))
        bounds[2 * i] = under.astype(jnp.int32) // BK
        bounds[2 * i + 1] = (upto.astype(jnp.int32) + BK - 1) // BK

    if ring:
        for s in range(1, len(steps)):
            ring_on(steps, s)
        follow()
    for i in R:
        xc[i].wait_recv()
        fc[i].start()
    for c in own:
        c.wait()
    for c in cc:
        c.wait_recv()
    if ring:
        ring_end(steps)
    ready()
    misc[...] = jnp.sum(wg[:, part:, :].astype(F32), axis=0)
    w = 3 * head

    def block(i):
        p = mm(full[i], whole(wg, part, 0, w)) + misc[7:8, :w]
        for j in range(3):
            qkv[j, pl.ds(i * rows, rows), :] = p[:, j * head : (j + 1) * head].astype(BF)

    def three(j, _):
        block(lax.select(j == 0, t, lax.select(j == 1, core, cross)))
        return 0

    lax.fori_loop(0, 3, three, 0)
    for c in fc:
        c.wait_recv()
    block(diag)
    for c in xc + cc + fc:
        c.wait_send()


def moments(h):
    mean = jnp.mean(h, axis=-1, keepdims=True)
    c = h - mean
    r = lax.rsqrt(jnp.mean(c * c, axis=-1, keepdims=True) + EPSILON)
    return c * r, r


def norm_back(dy, g, xhat, r):
    dx = dy * g
    return r * (
        dx
        - jnp.mean(dx, axis=-1, keepdims=True)
        - xhat * jnp.mean(dx * xhat, axis=-1, keepdims=True)
    )


def scatter_tools(core, cross, part, cs, cr, xs, xr, sems):
    ccs, ccr, xxs, xxr = sems
    a = lambda i, k: send(cs.at[k], cr.at[k], ccs.at[i, k], ccr.at[i, k], tensor=core)
    b = lambda i, k: send(xs.at[k], xr.at[k], xxs.at[i, k], xxr.at[i, k], tensor=cross)

    def put(i, k, tile, count):
        if i > 0:
            a(i - 1, k).wait_send()
        width = part.shape[-1] // count
        for j in range(count):
            p = tile(j)
            m = p.shape[0] // 4
            c = slice(j * width, (j + 1) * width)
            cs[k, 0, :, c] = p[m : 2 * m].astype(BF)
            cs[k, 1, :, c] = p[3 * m :].astype(BF)
            part[k, 0, :, c] = p[:m]
            part[k, 1, :, c] = p[2 * m : 3 * m]
        a(i, k).start()

    def put_half(i, k, b, tile, count):
        if i > 0 and b == 0:
            a(i - 1, k).wait_send()
        width = part.shape[-1] // count
        for j in range(count):
            p = tile(j)
            m = p.shape[0] // 2
            c = slice(j * width, (j + 1) * width)
            part[k, b, :, c] = p[:m]
            cs[k, b, :, c] = p[m:].astype(BF)
        if b == 1:
            a(i, k).start()

    def across(i, k):
        a(i, k).wait_recv()
        if i > 0:
            b(i - 1, k).wait_send()
        xs[k] = (part[k, 1] + cr[k, 1].astype(F32)).astype(BF)
        b(i, k).start()
        part[k, 0] = part[k, 0] + cr[k, 0].astype(F32)

    def take(i, k):
        b(i, k).wait_recv()
        return part[k, 0] + xr[k].astype(F32)

    def end(i, k):
        a(i, k).wait_send()
        b(i, k).wait_send()

    return put, put_half, across, take, end


def block_rows(ref, device, c0, c1, n):
    size = ref.shape[0] // n
    return ref.at[pl.ds(pl.multiple_of(device * size, size), size), pl.ds(c0, c1 - c0)]


class RingSum:
    def __init__(self, n, place, at, local, c0, c1, buf, ss, rs, longer):
        nxt, prv = at((place + 1) % n), at((place + n - 1) % n)
        right = n // 2 if longer else n - 1 - n // 2
        self.buf, self.local = buf, lambda p: block_rows(local, at((p + n) % n), c0, c1, n)
        self.place = place
        self.chains = (
            (0, right, lambda s: place + right - s, nxt),
            (right, n - 1 - right, lambda s: place - (n - 1 - right) + s, prv),
        )
        self.ss, self.rs = ss, rs

    def copy(self, chain, s):
        base, _, owner, target = chain
        src = self.local(owner(0)) if s == 0 else self.buf.at[base + s - 1]
        j = base + s
        return send(src, self.buf.at[j], self.ss.at[j], self.rs.at[j], fsdp=target)

    def go(self, s):
        for chain in self.chains:
            base, hops, owner, _ = chain
            if s >= hops:
                continue
            if s > 0:
                self.copy(chain, s - 1).wait_recv()
                j = base + s - 1
                self.buf[j] = (self.buf[j].astype(F32) + self.local(owner(s))[...].astype(F32)).astype(BF)
            self.copy(chain, s).start()

    def close(self):
        total = self.local(self.place)[...].astype(F32)
        for chain in self.chains:
            self.copy(chain, chain[1] - 1).wait_recv()
            total = total + self.buf[chain[0] + chain[1] - 1].astype(F32)
        return total

    def sent(self):
        for chain in self.chains:
            for s in range(chain[1]):
                self.copy(chain, s).wait_send()


def ring_group(n, place, at, local, tracks):
    m = len(tracks)
    q = [RingSum(n, place, at, local, j * 128, j * 128 + 128, *tracks[j], j % 2) for j in range(m)]
    left = list(range(n // 2))

    def go():
        if left:
            s = left.pop(0)
            for r in q:
                r.go(s)

    def close():
        while left:
            go()
        x = jnp.concatenate([r.close() for r in q], axis=1)
        for r in q:
            r.sent()
        return x

    return go, close


def ring_scratch(n, rows, widths):
    out = []
    for w in widths:
        out += [pltpu.VMEM((n - 1, rows, w), BF)]
        out += [DMA((n - 1,)), DMA((n - 1,))]
    return out


def attend_block(i, lo, hi, heads, sq_ref, sk_ref, pad_ref, qt, kh, vt, sc, ctx_ref, octx_ref, lse_ref):
    q0 = pl.multiple_of(i * BQ, BQ)
    sq = sq_ref[0:1, pl.ds(q0, BQ)]
    qpos = q0 + lax.broadcasted_iota(jnp.int32, (BK, BQ), 1)
    part = sc.shape[1] // BK
    spot = lambda h, j: (sc.shape[0] // heads * h + j // part, pl.ds(pl.multiple_of(j % part * BK, BK), BK), slice(None))

    def first(j, c):
        k0 = pl.multiple_of(j * BK, BK)
        sk = jnp.concatenate([sk_ref[pl.ds(k0, BK), :]] * (BQ // 128), axis=1)
        kpos = k0 + lax.broadcasted_iota(jnp.int32, (BK, BQ), 0)
        ok = (sk == sq) | (kpos == qpos)
        out = []
        for h in range(heads):
            s = jnp.where(ok, mm(kh(h, j)[...], qt(h, i)[...]), -1e30)
            sc[spot(h, j)] = s
            out.append(jnp.maximum(c[h], fold_max(s)))
        return tuple(out)

    m = lax.fori_loop(lo, hi, first, (jnp.full((8, BQ), -3e38, F32),) * heads)
    m = [jnp.max(x, axis=0, keepdims=True) for x in m]

    def second(j, c):
        out = []
        for h in range(heads):
            l, acc = c[2 * h : 2 * h + 2]
            p = jnp.exp(sc[spot(h, j)] - m[h])
            out += [l + fold_sum(p), acc + mm(vt(h, j)[...], p.astype(BF))]
        return tuple(out)

    c = lax.fori_loop(lo, hi, second, (jnp.zeros((8, BQ), F32), jnp.zeros((DH, BQ), F32)) * heads)
    o = []
    for h in range(heads):
        l, acc = c[2 * h : 2 * h + 2]
        l = jnp.sum(l, axis=0, keepdims=True)
        lse_ref[h : h + 1, pl.ds(q0, BQ)] = m[h] + jnp.log(l)
        o.append(acc / l)
    ot = jnp.concatenate(o, axis=0) * pad_ref[0:1, pl.ds(q0, BQ)]
    octx_ref[:, pl.ds(q0, BQ)] = ot
    ctx_ref[pl.ds(q0, BQ), :] = ot.T.astype(BF)


def middle_kernel(n, ring, *refs):
    refs = list(refs)
    pop = lambda m: [refs.pop(0) for _ in range(m)]
    tok, cot_hbm = pop(2)
    raw = pop(9 if ring else 2)
    if ring:
        wh, wd = pop(2)
    else:
        wg, wf = pop(2)
    full, qkv, sq, sk, live_row, bounds = pop(6)
    if ring:
        (wg,) = pop(1)
    out, dfirst, dctx, octx, lse, gown, gsend, gup, gdown, sums = pop(10)
    misc, pad = pop(2)
    mine = near = nsem = psems = None
    if ring:
        mine = pop(1)[0]
        near = pop(len(raw))
        nsem = pop(1)[0]
    tsems = pop(7)
    if ring:
        psems = pop(4)
    if ring:
        (wf,) = pop(1)
    ctx, call, slab, wo, dsend = pop(5)
    (norm, dff, acted, dgelu, pre, dpre, first, xhat, r1, part, csem, lsem) = pop(12)
    cs, cr, xs, xr = pop(4)
    ocs, ocr = pop(2)
    rsem = pop(4)
    gsem = pop(6)
    osem = pop(2)
    ssem = pop(6)
    asem = pop(6)
    dsem = pop(6)
    ff = wf.shape[2] // 2
    if ring:
        wsem = pop(4)
    t, f, core, cross, diag, place, at = places(n)
    rows, d = out.shape
    fetch = pltpu.make_async_copy(cot_hbm, out, csem.at[0])
    fetch.start()
    nch = rows // ROWS
    wpart = wg.shape[1] - MISC
    fpart = wf.shape[1]
    width = ctx.shape[1]
    heads = width // DH
    where = (t, core, cross, diag)
    put, put_half, across, take, end = scatter_tools(core, cross, part, cs, cr, xs, xr, rsem)
    gs = {}
    for i, buf in enumerate((norm, dff)):
        gs[i] = (
            lambda k, buf=buf, i=i: send(buf.at[k, 0], buf.at[k, 2], gsem[0].at[i, k], gsem[1].at[i, k], tensor=cross),
            lambda k, buf=buf, i=i: send(buf.at[k, 0], buf.at[k, 1], gsem[2].at[i, k], gsem[3].at[i, k], tensor=core),
            lambda k, buf=buf, i=i: send(buf.at[k, 2], buf.at[k, 3], gsem[4].at[i, k], gsem[5].at[i, k], tensor=core),
        )

    def share(i, k):
        gs[i][0](k).start()
        gs[i][1](k).start()

    def shared(i, k):
        gs[i][0](k).wait_recv()
        gs[i][2](k).start()
        gs[i][1](k).wait_recv()
        gs[i][2](k).wait_recv()

    lane0 = d - slab.shape[-1]
    slab0 = wg.at[:, pl.ds(0, wpart), pl.ds(lane0, slab.shape[-1])]
    slabs = (
        send(slab0, slab.at[1], ssem[0].at[0], ssem[1].at[0], tensor=cross),
        send(slab0, slab.at[0], ssem[2].at[0], ssem[3].at[0], tensor=core),
        send(slab.at[1], slab.at[2], ssem[4].at[0], ssem[5].at[0], tensor=core),
    )

    def rows_at(w, k):
        return pl.ds(pl.multiple_of(w * rows + k * ROWS, ROWS), ROWS)

    def give(j, k):
        return send(ctx.at[rows_at(where[j], k), :], call.at[k, j], asem[2 * j - 2].at[k], asem[2 * j - 1].at[k], tensor=where[j])

    def back(j, k):
        return send(dsend.at[k, j - 1], dctx.at[rows_at(t, k), :], dsem[2 * j - 2].at[k], dsem[2 * j - 1].at[k], tensor=where[j])

    load = []
    steps = []
    if ring:
        load = [
            pltpu.make_async_copy(wh, wf.at[f, :, pl.ds(0, ff)], lsem.at[0]),
            pltpu.make_async_copy(wd, wf.at[f, :, pl.ds(ff, ff)], lsem.at[1]),
        ]
        steps = both_ways(n, place, at, wf.at[f], wf, wsem)

    def lead():
        for c in load:
            c.start()

    def follow():
        for c in load:
            c.wait()
        for c in steps[0]:
            c.start()

    def ready():
        slabs[0].start()
        slabs[1].start()

    outs = (full, qkv, misc, sq, sk, live_row, pad, bounds)
    project_part(n, ring, tok, raw, outs, wg, mine, near, nsem, tsems, psems, lead, follow, ready)
    sums[...] = jnp.zeros_like(sums)

    blocks = 4 * rows // BQ
    across_lanes = d // BQ

    def turned(top):
        def tile(h, i):
            lanes = pl.ds(pl.multiple_of(i % across_lanes * BQ, BQ), BQ)
            return dff.at[h, i // across_lanes, pl.ds(top, DH), lanes]

        return tile

    qt, vt = turned(0), turned(DH)
    stack = 4 * ROWS // BK

    def kh(h, j):
        lanes = pl.ds(pl.multiple_of(j // stack * 128, 128), DH)
        return acted.at[h, pl.ds(pl.multiple_of(j % stack * BK, BK), BK), lanes]

    def prepare(i, _):
        r = pl.ds(pl.multiple_of(i * BQ, BQ), BQ)
        qs = (qkv[0, r, :].astype(F32) * 0.125).T.astype(BF)
        vs = qkv[2, r, :].astype(F32).T.astype(BF)
        ks = qkv[1, r, :]
        for h in range(heads):
            c = slice(h * DH, (h + 1) * DH)
            qt(h, i)[...] = qs[c]
            vt(h, i)[...] = vs[c]
            kh(h, i)[...] = ks[:, c]
        return 0

    lax.fori_loop(0, blocks, prepare, 0)
    reach = (MOST - 2 + BK) // BK

    def attend(base, stride, count):
        def body(i, _):
            b = base + i * stride
            lo = jnp.maximum(b - reach, 0)
            hi = jnp.minimum(b + reach + 1, blocks)
            attend_block(b, lo, hi, heads, sq, sk, live_row, qt, kh, vt, dgelu, ctx, octx, lse)
            return 0

        lax.fori_loop(0, count, body, 0)

    def give_when(sent):
        for w in range(4):
            ks = [k for k in range(nch) if k in sent[w]]
            for j in (3, 2, 1):

                @pl.when(where[j] == w)
                def _(j=j, ks=ks):
                    for k in ks:
                        give(j, k).start()

    def rows_of(k):
        return pl.ds(pl.multiple_of(k * ROWS, ROWS), ROWS)

    def pad_rows(k):
        return pad[rows_at(t, k), 0:1]

    def live(k, x):
        s = jnp.sum(x * x, axis=-1, keepdims=True) * pad_rows(k)
        return jnp.sum(s, axis=0, keepdims=True)

    lane = lax.broadcasted_iota(jnp.int32, (1, d), 1)

    def note(j, v):
        sums[7:8, :] += jnp.where(lane == d // 2 + j, v, 0.0)

    def norm_one(k):
        for j in (1, 2, 3):
            give(j, k).wait_recv()
        call[k, 0] = ctx[rows_at(t, k), :]
        x = full[t, rows_of(k), :].astype(F32)
        branch = misc[4:5, :]
        for j in range(4):
            branch = branch + mm(call[k, j], wo[j], 1, 1)
        xh, r = moments(x + branch)
        y = xh * misc[0:1, :] + misc[2:3, :]
        first[k] = y
        xhat[k] = xh
        r1[k] = r
        norm[k, 0] = y.astype(BF)
        share(0, k)
        note(0, live(k, x))
        note(1, live(k, branch))
        note(3, jnp.sum(pad_rows(k), axis=0, keepdims=True))

    def loop(fn):
        def body(k, _):
            fn(k)
            return 0

        lax.fori_loop(0, nch, body, 0)

    done, whole_rows = set(), [set() for _ in range(4)]

    def ran(ids):
        done.update(r for b in ids for r in range(b * BQ // ROWS, (b + 1) * BQ // ROWS))
        fresh = [
            {k for k in range(nch) if w * nch + k in done and k not in whole_rows[w]} for w in range(4)
        ]
        for w in range(4):
            whole_rows[w] |= fresh[w]
        give_when(fresh)

    attend(0, 1, 2)
    ran((0, 1))
    if ring:
        ring_on(steps, 1)
    attend(3, 1, 2)
    ran((3, 4))
    slabs[0].wait_recv()
    slabs[2].start()
    if ring:
        ring_on(steps, 2)
    attend(2, 1, 1)
    slabs[1].wait_recv()
    slabs[2].wait_recv()
    wo[0] = whole(wg, wpart, lane0, d)[:, -width:]
    for j in range(3):
        wo[j + 1] = slab[j].reshape(d, slab.shape[-1])[:, -width:]
    norm_one(0)
    attend(5, 1, 1)
    ran((2, 5))
    if ring:
        for s in range(3, len(steps)):
            ring_on(steps, s)
    for k in range(1, nch):
        norm_one(k)
    if ring:
        ring_end(steps)
    inv = 0.7071067811865476
    thirds = ff // BQ

    def far_rows(i, k):
        gs[i][0](k).wait_recv()
        gs[i][2](k).start()
        if isinstance(k, int):
            if k > 0:
                across(i, k - 1)
        else:
            pl.when(k > 0)(lambda: across(i, k - 1))
        gs[i][2](k).wait_recv()

    def feed(k, b):
        x = norm[k, 2 * b : 2 * b + 2].reshape(2 * ROWS, d)
        for c in range(0, ff, 256):
            pre[:, c : c + 256] = mm(x, whole(wf, fpart, c, c + 256)) + misc[6:7, c : c + 256]

        def act(i, _):
            u = pre[pl.ds(pl.multiple_of(i * 64, 64), 64), :]
            s = pl.ds(pl.multiple_of(b * 2 * ROWS + i * 64, 64), 64)
            cdf = 0.5 + 0.5 * lax.erf(u * inv)
            acted[k, s, :] = (u * cdf).astype(BF)
            slope = cdf + u * (jnp.exp(-0.5 * u * u) * 0.3989422804014327)
            for c in range(thirds):
                dgelu[k * thirds + c, s, :] = slope[:, c * BQ : (c + 1) * BQ]
            return 0

        lax.fori_loop(0, 2 * ROWS // 64, act, 0)
        y = acted[k, 2 * b * ROWS : 2 * (b + 1) * ROWS, :]
        put_half(0, k, b, lambda j: mm(y, some(wf, fpart, ff, 2 * ff, j, 2), 1, 1), 2)

    def feed_near(k):
        gs[0][1](k).wait_recv()
        feed(k, 0)

    def feed_far(k):
        far_rows(0, k)
        feed(k, 1)

    def feed_all(k):
        feed_near(k)
        feed_far(k)

    loop(feed_all)
    across(0, nch - 1)
    fetch.wait()

    def norm_two(k):
        branch = take(0, k) + misc[5:6, :]
        xh, r = moments(first[k] + branch)
        dy = out[rows_of(k), :].astype(F32)
        out[rows_of(k), :] = (xh * misc[1:2, :] + misc[3:4, :]).astype(BF)
        ds = norm_back(dy, misc[1:2, :], xh, r)
        first[k] = ds
        low = ds.astype(BF)
        dff[k, 0] = low
        share(1, k)
        note(2, live(k, branch))
        sums[1:2, :] += col_sum(dy * xh)
        sums[3:4, :] += col_sum(dy)
        sums[5:6, :] += col_sum(low.astype(F32))

    loop(norm_two)

    def feed_back(k, b):
        g = dff[k, 2 * b : 2 * b + 2].reshape(2 * ROWS, d)
        for c in range(0, ff, 256):
            pre[:, c : c + 256] = mm(g, whole(wf, fpart, ff + c, ff + c + 256))

        def act(i, _):
            r = pl.ds(pl.multiple_of(i * 64, 64), 64)
            s = pl.ds(pl.multiple_of(b * 2 * ROWS + i * 64, 64), 64)
            slope = jnp.concatenate([dgelu[k * thirds + c, s, :] for c in range(thirds)], axis=1)
            low = (pre[r, :] * slope).astype(BF)
            dpre[k, s, :] = low
            sums[6:7, :] += col_sum(low.astype(F32))
            return 0

        lax.fori_loop(0, 2 * ROWS // 64, act, 0)
        y = dpre[k, 2 * b * ROWS : 2 * (b + 1) * ROWS, :]
        put_half(1, k, b, lambda j: mm(y, some(wf, fpart, 0, ff, j, 2), 1, 1), 2)

    def back_near(k):
        gs[1][1](k).wait_recv()
        feed_back(k, 0)

    def back_far(k):
        far_rows(1, k)
        feed_back(k, 1)

    def weight_part(left, right, to):
        def cols(i, _):
            c = pl.ds(pl.multiple_of(i * 128, 128), 128)
            g = 0.0
            for k in range(nch):
                g = g + mm(left[k, :, :, c].reshape(4 * ROWS, 128), right[k], 0, 0)
            to[c, :] = g.astype(BF)
            return 0

        lax.fori_loop(0, d // 128, cols, 0)

    def norm_one_back(k):
        dy = first[k] + take(1, k)
        xh = xhat[k]
        ds = norm_back(dy, misc[0:1, :], xh, r1[k])
        dfirst[rows_of(k), :] = ds
        low = ds.astype(BF)
        for c in gs[1][:2]:
            c(k).wait_send()
        dff[k, 0] = low
        for j in (3, 2, 1):
            dsend[k, j - 1] = mm(low, wo[j]).astype(BF)
            back(j, k).start()
        dctx[rows_at(t, k), :] = mm(low, wo[0]).astype(BF)
        sums[0:1, :] += col_sum(dy * xh)
        sums[2:3, :] += col_sum(dy)
        sums[4:5, :] += col_sum(low.astype(F32))

    oc = send(ocs, ocr, osem[0].at[0], osem[1].at[0], tensor=core)

    def out_part():
        x = dff[:, 0].reshape(rows, d)
        for slot, j in ((0, 1), (1, 3)):
            ocs[slot] = mm(x, call[:, j].reshape(rows, width), 0, 0).astype(BF)
        oc.start()

    def out_take():
        x = dff[:, 0].reshape(rows, d)
        for slot, j, to in ((1, 2, gsend), (0, 0, gown)):
            p = mm(x, call[:, j].reshape(rows, width), 0, 0)
            if slot:
                oc.wait_recv()
            to[...] = (p + ocr[slot].astype(F32)).astype(BF)

    for k in range(2):
        back_near(k)
    back_far(0)
    for k in range(2, nch):
        back_near(k)
    for k in range(1, nch):
        back_far(k)
    across(1, nch - 1)
    weight_part(dff, acted, gdown)
    for k in range(nch - 1):
        norm_one_back(k)
    weight_part(norm, dpre, gup)
    norm_one_back(nch - 1)
    out_part()
    out_take()

    def finish(k, _):
        end(1, k)
        for j in (1, 2, 3):
            back(j, k).wait_recv()
            back(j, k).wait_send()
            give(j, k).wait_send()
        for c in gs[0] + gs[1][2:]:
            c(k).wait_send()
        return 0

    lax.fori_loop(0, nch, finish, 0)
    for c in slabs + (oc,):
        c.wait_send()


def middle(n, tok, cot, head, seg, alive, raw, wh, wd, wg, wf):
    ring = wf is None
    vm = pl.BlockSpec(memory_space=pltpu.VMEM)
    far = pl.BlockSpec(memory_space=pltpu.HBM)
    pin = lambda x: pltpu.with_memory_space_constraint(x, pltpu.HBM)
    rows, d = cot.shape
    width = head
    heads = width // DH
    total = 4 * rows
    nch = rows // ROWS
    s = jax.ShapeDtypeStruct
    V = pltpu.VMEM
    ff = wh.shape[1] if ring else wf.shape[2] // 2
    tables = (seg.reshape(-1, 128), alive.reshape(-1, 128))
    if ring:
        ops = tuple(pin(x) for x in (tok, cot) + tables + raw + (wh, wd))
        specs = [far] * len(ops)
    else:
        ops = (tok, pin(cot)) + tables + (wg, wf)
        specs = [vm, far] + [vm] * 4
    outs = [
        s((4, rows, d), BF),
        s((3, total, width), BF),
        s((1, total), F32),
        s((total, 128), F32),
        s((1, total), F32),
        s((2 * total // BQ,), jnp.int32),
    ]
    ospecs = [vm] * 5 + [pl.BlockSpec(memory_space=pltpu.SMEM)]
    if ring:
        outs.append(s((n, d // n + MISC, d), BF))
    outs += [
        s((rows, d), BF),
        s((rows, d), F32),
        s((total, width), BF),
        s((width, total), F32),
        s((heads, total), F32),
        s((d, width), BF),
        s((d, width), BF),
        s((d, ff), BF),
        s((d, ff), BF),
        s((8, d), F32),
    ]
    ospecs += [vm] * (len(outs) - len(ospecs))
    g, gr = (n, d // n) if ring else (wg.shape[0], wg.shape[1] - MISC)
    wide = -(-width // 128) * 128
    scratch = [V((MISC, d), F32), V((total, 128), F32)]
    if ring:
        held = tables + raw
        scratch += [V((d // n + MISC, d), BF)] + [V(x.shape, x.dtype) for x in held] + [DMA((len(held),))]
    scratch += [DMA((2,))] + [DMA((nch,))] * 6
    if ring:
        scratch += [DMA((n // 2, 2))] * 4
        scratch += [V((n, d // n, 2 * ff), BF)]
    scratch += [V((total, width), BF), V((nch, 4, ROWS, width), BF), V((3, g, gr, wide), BF), V((4, d, width), BF)]
    scratch += [V((nch, 3, ROWS, width), BF)]
    scratch += [V((nch, 4, ROWS, d), BF)] * 2
    scratch += [V((nch, 4 * ROWS, ff), BF), V((nch * (ff // BQ), 4 * ROWS, BQ), F32), V((2 * ROWS, ff), F32), V((nch, 4 * ROWS, ff), BF)]
    scratch += [V((nch, ROWS, d), F32)] * 2 + [V((nch, ROWS, 1), F32)]
    scratch += [V((nch, 2, ROWS, d), F32), DMA((1,)), DMA((2,))]
    scratch += [V((nch, 2, ROWS, d), BF)] * 2 + [V((nch, ROWS, d), BF)] * 2
    scratch += [V((2, d, width), BF)] * 2
    scratch += [DMA((2, nch))] * 10 + [DMA((1,))] * 8 + [DMA((nch,))] * 12
    if ring:
        scratch += [DMA((n // 2, 2))] * 4
    return pl.pallas_call(
        functools.partial(middle_kernel, n, ring),
        in_specs=specs,
        out_specs=ospecs,
        out_shape=outs,
        scratch_shapes=scratch,
        compiler_params=pltpu.CompilerParams(
            collective_id=2, has_side_effects=True, vmem_limit_bytes=38 << 20
        ),
        name="middle",
    )(*ops)


def attend_back_part(heads, reach, hook, qkv_ref, dc_ref, oct_ref, lse_ref, sq_ref, sk_ref, pad_ref, dqkv_ref, scratch):
    qt, dt, kt, kh, vh, qh, dh, dqt, dsum, dka, dva = scratch
    S=qkv_ref.shape[1]; W=heads*DH
    qs=(qkv_ref[0].astype(F32)*0.125)
    qsb=qs.astype(BF); qt[...]=qs.T.astype(BF)
    kk=qkv_ref[1]; vv=qkv_ref[2]
    kt[...]=kk.astype(F32).T.astype(BF)
    dct=dc_ref[...].astype(F32).T*pad_ref[0:1,:]
    dt[...]=dct.astype(BF)
    dcn=dct.T.astype(BF)
    prod=dct*oct_ref[...]
    for h in range(heads):
        c=slice(h*DH,(h+1)*DH)
        kh[h]=kk[:,c]; vh[h]=vv[:,c]; qh[h]=qsb[:,c]; dh[h]=dcn[:,c]
        dsum[h:h+1,:]=jnp.sum(prod[h*DH:(h+1)*DH],axis=0,keepdims=True)
    dqt[...]=jnp.zeros_like(dqt)
    def kblock(j):
        k0=j*BK
        lo=max(j-reach,0); hi=min(j+reach+1,S//BQ)
        sk=jnp.concatenate([sk_ref[pl.ds(k0,BK),:]]*(BQ//128),axis=1)
        kpos=k0+lax.broadcasted_iota(jnp.int32,(BK,BQ),0)
        dka[...]=jnp.zeros_like(dka); dva[...]=jnp.zeros_like(dva)
        def body(i,_):
            q0=pl.multiple_of(i*BQ,BQ)
            sq=sq_ref[0:1,pl.ds(q0,BQ)]
            qpos=q0+lax.broadcasted_iota(jnp.int32,(BK,BQ),1)
            ok=(sk==sq)|(kpos==qpos)
            for h in range(heads):
                r=slice(h*DH,(h+1)*DH)
                s=jnp.where(ok,mm(kh[h,pl.ds(k0,BK),:],qt[r,pl.ds(q0,BQ)]),-1e30)
                p=jnp.exp(s-lse_ref[h:h+1,pl.ds(q0,BQ)])
                dp=mm(vh[h,pl.ds(k0,BK),:],dt[r,pl.ds(q0,BQ)])
                ds=(p*(dp-dsum[h:h+1,pl.ds(q0,BQ)])).astype(BF)
                dva[h]+=mm(p.astype(BF),dh[h,pl.ds(q0,BQ),:])
                dka[h]+=mm(ds,qh[h,pl.ds(q0,BQ),:])
                dqt[r,pl.ds(q0,BQ)]+=mm(kt[r,pl.ds(k0,BK)],ds)
            return 0
        lax.fori_loop(lo,hi,body,0)
        dqkv_ref[pl.ds(k0,BK),W:]=jnp.concatenate([dka[h] for h in range(heads)]+[dva[h] for h in range(heads)],axis=1).astype(BF)
    for j in range(S//BK):
        kblock(j)
        hook(j)
    dqkv_ref[:,:W]=(dqt[...]*0.125).T.astype(BF)


def last_kernel(n, ring, *refs):
    refs = list(refs)
    pop = lambda m: [refs.pop(0) for _ in range(m)]
    qkv, dctx, octx, lse, sq, sk, live_row = pop(7)
    wg, full, gown, gsend, dfirst, sums = pop(6)
    if ring:
        gup, gdown = pop(2)
        dtok, oattn, oout, oup, odown, ogain, oshift, obias, ohb, oqvb, oroot = pop(11)
    else:
        dtok, gb, total = pop(3)
    dqkv, gfar = pop(2)
    bscratch = pop(11)
    osem = pop(2)
    part, cs, cr, xs, xr = pop(5)
    rsem = pop(4)
    msend, mrecv = pop(2)
    msem = pop(4)
    if ring:
        gb, mall = pop(2)
        mring = pop(4)
        tracks = [refs[i : i + 3] for i in range(0, len(refs), 3)]
    t, f, core, cross, diag, place, at = places(n)
    rows, d = dtok.shape
    nch = rows // ROWS
    wpart = wg.shape[1] - MISC
    width = qkv.shape[2]
    w3 = 3 * width
    where = (t, core, cross, diag)
    put, put_half, across, take, end = scatter_tools(core, cross, part, cs, cr, xs, xr, rsem)
    nxt, prv = at((place + 1) % n), at((place + n - 1) % n)

    def rows_of(k):
        return pl.ds(pl.multiple_of(k * ROWS, ROWS), ROWS)

    meet(core, cross, (nxt, prv) if ring else ())
    ox = send(gsend, gfar, osem[0].at[0], osem[1].at[0], tensor=cross)
    ox.start()
    hooks = []
    if ring:
        ups, downs = gup.shape[1] // 128, gdown.shape[1] // 128
        down, down_close = ring_group(n, place, at, gdown, tracks[:downs])
        up, up_close = ring_group(n, place, at, gup, tracks[downs : downs + ups])
        down()
        up()
        hooks = [down, up] * (n // 2)

    def hook(j):
        if j < len(hooks):
            hooks[j]()

    reach = (MOST - 2 + BK) // BK
    attend_back_part(width // DH, reach, hook, qkv, dctx, octx, lse, sq, sk, live_row, dqkv, bscratch)

    b = col_sum(dqkv[...].astype(F32))
    b = jnp.concatenate([b[:, :width], b[:, 2 * width :], jnp.zeros((1, d - 2 * width), F32)], axis=1)
    msend[0] = sums[...]
    msend[0, 7:8, :] = sums[7:8, :] + b
    m0 = send(msend.at[0], mrecv.at[0], msem[0].at[0], msem[1].at[0], tensor=core)
    m1 = send(msend.at[1], mrecv.at[1], msem[2].at[0], msem[3].at[0], tensor=cross)
    m0.start()
    ox.wait_recv()

    def weight_part(i, _):
        c = pl.ds(pl.multiple_of(i * 128, 128), 128)
        g = 0.0
        for j in range(4):
            g = g + mm(full[j, :, c], dqkv[j * rows : (j + 1) * rows, :], 0, 0)
        o = gown[c, :].astype(F32) + gfar[c, :].astype(F32)
        gb[c, :] = jnp.concatenate([g, o], axis=1).astype(BF)
        return 0

    def tokens_part(k):
        x = jnp.concatenate([dqkv[pl.ds(w * rows + k * ROWS, ROWS), :] for w in where], axis=0)
        put(0, k, lambda j: mm(x, some(wg, wpart, 0, w3, j, 2), 1, 1), 2)

    tokens_part(0)
    lax.fori_loop(0, d // 256, weight_part, 0)
    m0.wait_recv()
    msend[1] = msend[0] + mrecv[0]
    m1.start()
    across(0, 0)
    lax.fori_loop(d // 256, d // 128, weight_part, 0)
    if ring:
        go, own_close = ring_group(n, place, at, gb, tracks[ups + downs :])
        go()
    for k in range(1, nch):
        tokens_part(k)
        if k > 1:
            across(0, k - 1)
    m1.wait_recv()
    row = lax.broadcasted_iota(jnp.int32, (8, d), 0)
    col = lax.broadcasted_iota(jnp.int32, (8, d), 1)
    over_tensor = (row < 6) | ((row == 7) & (col >= 2 * width))
    small = jnp.where(over_tensor, msend[1] + mrecv[1], msend[0])

    def keep(k):
        dtok[rows_of(k), :] = dfirst[rows_of(k), :] + take(0, k)

    if ring:
        msend[2] = small
        mall[place] = small
        msteps = []
        far = n // 2
        for s in range(far):
            a, b = (place - s + n) % n, (place + s) % n
            src = msend.at[2] if s == 0 else mall.at[a]
            pair = [send(src, mall.at[a], mring[0].at[s], mring[1].at[s], fsdp=nxt)]
            if s < far - 1:
                src = msend.at[2] if s == 0 else mall.at[b]
                pair.append(send(src, mall.at[b], mring[2].at[s], mring[3].at[s], fsdp=prv))
            msteps.append(pair)
        def spread(r):
            for i, c in enumerate(msteps[r]):
                if r > 0:
                    msteps[r - 1][i].wait_recv()
                c.start()

        spread(0)
        across(0, nch - 1)
        go()
        odown[...] = down_close()
        todo = [functools.partial(keep, k) for k in range(nch)]
        for r in range(1, far):
            spread(r)
            go()
            if r == 1:
                oup[...] = up_close()
            if todo:
                todo.pop(0)()
        for f_ in todo:
            f_()
        msteps[far - 2][1].wait_recv()
        msteps[far - 1][0].wait_recv()
        total = jnp.sum(mall[...], axis=0)
        gp = d // n
        mine = pltpu.roll(total, (d - f * gp) % d, 1)
        ogain[...] = mine[0:2, :gp]
        oshift[...] = mine[2:4, :gp]
        obias[...] = mine[4:6, :gp]
        k = DH // n
        mine = pltpu.roll(total, (d - f * k) % d, 1)
        ohb[...] = jnp.concatenate([mine[6:7, h * DH : (h + 1) * DH] for h in range(ohb.shape[1])], axis=0).T[:k]
        heads = oqvb.shape[0]
        for h in range(heads):
            for j in range(2):
                c = (j * heads + h) * DH
                oqvb[h, j : j + 1, :] = mine[7:8, c : c + DH][:, :k]
        spot = lax.broadcasted_iota(jnp.int32, (1, d), 1) - d // 2
        pick = lambda j: jnp.sum(jnp.where(spot == j, total[7:8], 0.0), axis=1, keepdims=True)
        count = pick(3)
        col = lax.broadcasted_iota(jnp.int32, (1, 128), 1)
        o = jnp.zeros((1, 128), F32)
        for j in range(3):
            o = jnp.where(col == j, jnp.sqrt(pick(j) / (count * d)), o)
        oroot[...] = o
        x = own_close()
        for j in range(3):
            oattn[j] = x[:, j * width : (j + 1) * width]
        oout[...] = x[:, 3 * width :].T
        for pair in msteps:
            for c in pair:
                c.wait_send()
    else:
        across(0, nch - 1)
        total[...] = small
        for k in range(nch):
            keep(k)

    def finish(k, _):
        end(0, k)
        return 0

    lax.fori_loop(0, nch, finish, 0)
    for c in (m0, m1, ox):
        c.wait_send()


def last(n, ring, qkv, dctx, octx, lse, sq, sk, live_row, wg, full, gown, gsend, dfirst, sums, gup, gdown):
    vm = pl.BlockSpec(memory_space=pltpu.VMEM)
    rows, d = dfirst.shape
    width, total = qkv.shape[2], qkv.shape[1]
    heads = width // DH
    nch = rows // ROWS
    s = jax.ShapeDtypeStruct
    V = pltpu.VMEM
    ops = (qkv, dctx, octx, lse, sq, sk, live_row, wg, full, gown, gsend, dfirst, sums)
    outs = [s((rows, d), F32)]
    gp = d // n
    k = DH // n
    if ring:
        ops += (gup, gdown)
        outs += [s((3, gp, width), F32), s((width, gp), F32), s((gp, gup.shape[1]), F32), s((gp, gdown.shape[1]), F32)] + [s((2, gp), F32)] * 3
        outs += [s((k, d // DH), F32), s((heads, 2, k), F32), s((1, 128), F32)]
    else:
        outs += [s((d, d), BF), s((8, d), F32)]
    scratch = [V((total, 3 * width), BF), V((d, width), BF)]
    scratch += [V((width, total), BF)] * 3 + [V((heads, total, DH), BF)] * 4
    scratch += [V((width, total), F32), V((heads, total), F32)] + [V((heads, BK, DH), F32)] * 2
    scratch += [DMA((1,))] * 2
    scratch += [V((nch, 2, ROWS, d), F32)]
    scratch += [V((nch, 2, ROWS, d), BF)] * 2 + [V((nch, ROWS, d), BF)] * 2
    scratch += [DMA((1, nch))] * 4
    scratch += [V((3, 8, d), F32), V((2, 8, d), F32)] + [DMA((1,))] * 4
    if ring:
        scratch += [V((d, d), BF), V((n, 8, d), F32)] + [DMA((n // 2,))] * 4
        scratch += ring_scratch(n, gp, (128,) * ((gup.shape[1] + gdown.shape[1] + d) // 128))
    return pl.pallas_call(
        functools.partial(last_kernel, n, ring),
        in_specs=[vm] * len(ops),
        out_specs=[vm] * len(outs),
        out_shape=outs,
        scratch_shapes=scratch,
        compiler_params=pltpu.CompilerParams(
            collective_id=3, has_side_effects=True, vmem_limit_bytes=30 << 20
        ),
        name="last",
    )(*ops)


def deliver_kernel(*refs):
    m = (len(refs) - 3) // 2
    src, roots, dst, three, sem = refs[:m], refs[m], refs[m + 1 : -2], refs[-2], refs[-1]
    for j in range(m):
        pltpu.make_async_copy(src[j], dst[j], sem.at[j]).start()
    for j in range(three.shape[0]):
        three[j] = jnp.sum(roots[0:1, j : j + 1])
    for j in range(m):
        pltpu.make_async_copy(src[j], dst[j], sem.at[j]).wait()


def deliver(arrays, roots):
    vm = pl.BlockSpec(memory_space=pltpu.VMEM)
    return pl.pallas_call(
        deliver_kernel,
        in_specs=[vm] * (len(arrays) + 1),
        out_specs=[pl.BlockSpec(memory_space=pl.ANY)] * len(arrays) + [pl.BlockSpec(memory_space=pltpu.SMEM)],
        out_shape=[jax.ShapeDtypeStruct(x.shape, x.dtype) for x in arrays] + [jax.ShapeDtypeStruct((3,), F32)],
        scratch_shapes=[DMA((len(arrays),))],
        compiler_params=pltpu.CompilerParams(vmem_limit_bytes=1 << 20),
        name="deliver",
    )(*arrays, roots)


def split_up(value, dim, devices):
    before, after = (value.shape[:dim], value.shape[dim + 1 :])
    return jnp.moveaxis(value.reshape(*before, devices, -1, *after), dim, 0)


def summed_on_arrival(value, axis, dim):
    blocks = split_up(value, dim, lax.axis_size(axis))
    arrived = lax.all_to_all(blocks, axis, split_axis=0, concat_axis=0, tiled=True)
    return arrived.astype(F32).sum(axis=0)


def shards(
    tokens,
    attn_weight,
    query_value_bias,
    out_weight,
    hidden_weight,
    hidden_bias,
    down_weight,
    norm_gains,
    norm_biases,
    output_biases,
    segment_ids,
    padding,
    cotangent,
):
    n = lax.axis_size("fsdp")
    f = lax.axis_index("fsdp")
    t = lax.axis_index("tensor")
    rows, d = tokens.shape
    gp = d // n
    width = attn_weight.shape[2]
    heads = width // DH
    ff = hidden_weight.shape[1]
    ring = gp % 16 == 0 and n % 2 == 0 and n >= 4
    if ring:
        raw = (
            attn_weight,
            out_weight,
            norm_gains,
            norm_biases,
            output_biases,
            hidden_bias.T,
            query_value_bias.transpose(1, 0, 2),
        )
        wh, wd, wg, wf = hidden_weight, down_weight.T, None, None
    else:
        gather = lambda x, dim: lax.all_gather(x, "fsdp", axis=dim, tiled=True)
        w = gather(attn_weight, 1).transpose(1, 0, 2).reshape(d, 3 * width)
        wo = gather(out_weight, 1).T
        b = gather(query_value_bias, 2).reshape(2, width)
        b = jnp.concatenate([b[0], jnp.zeros((width,), BF), b[1], jnp.zeros((width,), BF)])
        misc = jnp.concatenate(
            [
                gather(norm_gains, 1),
                gather(norm_biases, 1),
                gather(output_biases, 1),
                gather(hidden_bias, 1).reshape(1, ff),
                b[None],
                jnp.zeros((MISC - 8, d), BF),
            ]
        )
        wg = jnp.concatenate([jnp.concatenate([w, wo], axis=1), misc])[None]
        wf = jnp.concatenate([gather(hidden_weight, 0), gather(down_weight, 1).T], axis=1)[None]
        wh = wd = raw = None
    got = list(
        middle(n, tokens, cotangent, width, segment_ids, padding, raw, wh, wd, wg, wf)
    )
    full, qkv, seg_row, seg_keys, pad_row, bounds = got[:6]
    if ring:
        wg = got.pop(6)
    layer_out, d_first, d_ctx, ctx_t, lse, g_own, g_send, g_hidden, g_down, sums = got[6:]
    done = last(
        n, ring, qkv, d_ctx, ctx_t, lse, seg_row, seg_keys, pad_row,
        wg, full, g_own, g_send, d_first, sums, g_hidden, g_down,
    )
    if ring:
        done = deliver((layer_out,) + tuple(done[:-1]), done[-1])
        layer_out, d_tokens, g_attn, g_proj, g_hidden, g_down, g_gain, g_shift, g_bias, g_hb, g_qvb, roots = done
        g_down = g_down.T
        g_hb = g_hb.T
        g_qvb = g_qvb.transpose(1, 0, 2)
    else:
        d_tokens, g, total = done
        total = lax.psum(total, "fsdp")
        g_attn = g[:, : 3 * width].reshape(d, 3, width).transpose(1, 0, 2)
        g_attn = summed_on_arrival(g_attn, "fsdp", 1)
        g_proj = summed_on_arrival(g[:, 3 * width :].T, "fsdp", 1)
        g_hidden = summed_on_arrival(g_hidden, "fsdp", 0)
        g_down = summed_on_arrival(g_down.T, "fsdp", 1)
        vectors = lax.dynamic_slice(total, (0, f * gp), (6, gp))
        g_gain, g_shift, g_bias = vectors[0:2], vectors[2:4], vectors[4:6]
        k = DH // n
        g_hb = lax.dynamic_slice(total[6].reshape(ff // DH, DH), (0, f * k), (ff // DH, k))
        g_qvb = lax.dynamic_slice(
            total[7, : 2 * width].reshape(2 * heads, DH), (0, f * k), (2 * heads, k)
        ).reshape(2, heads, k)
        squares = total[7, d // 2 : d // 2 + 4]
        roots = jnp.sqrt(squares[:3] / (squares[3] * d))
    return (
        layer_out,
        d_tokens,
        g_attn,
        g_qvb,
        g_proj,
        g_hidden,
        g_hb,
        g_down,
        g_gain,
        g_shift,
        g_bias,
        roots,
    )


def solution(mesh):
    placed = (
        P(("fsdp", "tensor"), None),
        P(None, "fsdp", "tensor"),
        P(None, "tensor", "fsdp"),
        P("tensor", "fsdp"),
        P("fsdp", "tensor"),
        P("tensor", "fsdp"),
        P("tensor", "fsdp"),
        P(None, "fsdp"),
        P(None, "fsdp"),
        P(None, "fsdp"),
        P("fsdp"),
        P("fsdp"),
        P(("fsdp", "tensor"), None),
    )
    return jax.shard_map(
        shards,
        mesh=mesh,
        in_specs=placed,
        out_specs=(
            P(("fsdp", "tensor"), None),
            P(("fsdp", "tensor"), None),
            P(None, "fsdp", "tensor"),
            P(None, "tensor", "fsdp"),
            P("tensor", "fsdp"),
            P("fsdp", "tensor"),
            P("tensor", "fsdp"),
            P("tensor", "fsdp"),
            P(None, "fsdp"),
            P(None, "fsdp"),
            P(None, "fsdp"),
            P(),
        ),
        check_vma=False,
    )
```
